32 devices in a mesh: mesh: 4 (over y, x), sub: 8 (over z, core).
Axes of the slice: x: 2, y: 2, z: 4, core: 2. Of those that a mesh axis runs over, the one named last changes fastest.
Arguments:
- displacement: float32 [3, 2, 32, 1024], P(None, None, 'mesh', 'sub'), may hold values from -4 to 4
- velocity: float32 [3, 2, 32, 1024], P(None, None, 'mesh', 'sub'), may hold values from -6 to 6
- node_mass: float32 [2, 32, 1024], P(None, 'mesh', 'sub'), may hold values from 0.5 to 2
- moduli: float32 [2, 32, 1024], P(None, 'mesh', 'sub'), may hold values from 0.5 to 2
- stiffness: float32 [24, 24], replicated, may hold values from -0.45 to 12, as said below
- surface_ref: float32 [3, 32, 1024], P(None, 'mesh', 'sub'), may hold values from -6 to 6
- facets: float32 [4, 8, 6, 1024], P('mesh', 'sub'), may hold values from -6 to 6
- penalty: float32 [4, 8, 1024], P('mesh', 'sub'), may hold values from 0.5 to 4
- owners: int32 [2, 4, 8, 8, 1], P(None, 'mesh', 'sub'), may hold values from 0 to 3; in each aligned block of 8 rows (0 to 7, 8 to 15, ..., all dimensions but the last counted through in order) at most 4 rows name the same one
- facet_pairs: int32 [2, 32, 1024], P(None, 'mesh', 'sub'), may hold values from 0 to 1023
Outputs:
- final_displacement: float32 [3, 2, 32, 1024], P(None, None, 'mesh', 'sub')
- final_velocity: float32 [3, 2, 32, 1024], P(None, None, 'mesh', 'sub')
The draws below stay inside these ranges and needn't reach their ends.
Inputs may be any that keep to these rules, and one draw needn't show every extreme that they name: `owners`: in every step no device sends more than 4 of its blocks to one owner, and some device sends exactly 4 to one owner. `stiffness`: Symmetric.
All inputs are finite; a program needn't handle non-finite values.
Results may differ from the reference program's by a relative error of at most 0.0001.
Values sent between devices are 32-bit elements; how exact they have to be, the bound alone decides.
A program may use at most 64 MiB of HBM per device.

```python
import math
import jax
import jax.numpy as jnp
import numpy as np
from jax import lax

NZ = 2
BLOCK = 128
TF = 1024
STEPS = 2
OWNERS = 4
SUBPARTS = 8
SB = 8
CAP = 4
NX = 32
NY = 1024
N_MESH = 4


def draw_stiffness(key, part):
    key_off = jax.random.fold_in(key, 11)
    key_diag = jax.random.fold_in(key, 12)
    sampled = jax.random.truncated_normal(key_off, -3.0, 3.0, (24, 24), jnp.float32) * 0.15
    symmetric = (sampled + sampled.T) * 0.5
    off_diagonal = symmetric * (1.0 - jnp.eye(24, dtype=jnp.float32))
    surplus = jax.random.uniform(key_diag, (24,), jnp.float32, 0.5, 1.5)
    return off_diagonal + jnp.diag(jnp.sum(jnp.abs(off_diagonal), axis=1) + surplus)


def touch_ends(entries, own_key, least, high):
    shape = entries.shape
    index_at = [jax.random.randint(jax.random.fold_in(own_key, axis), (), 0, shape[axis]) for axis in range(len(shape))]
    entries = entries.at[tuple(index_at)].set(least)
    longest = shape.index(max(shape))
    index_at[longest] = (index_at[longest] + 1) % shape[longest]
    return entries.at[tuple(index_at)].set(high)


def steps_of(rng, dims, cuts, least, high):
    def one(position, shards_of):
        draws = jax.random.uniform(jax.random.fold_in(jax.random.fold_in(rng, 6), position), (shards_of,), jnp.float32, least / len(cuts), high / len(cuts))
        return jnp.repeat(jnp.exp(draws), dims[position] // shards_of).reshape((-1,) + (1,) * (len(dims) - position - 1))

    gain = one(*cuts[0])
    for cut in cuts[1:]:
        gain = gain * one(*cut)
    return gain


def assign_block(stream_key, own, number, rows, number_of, top, reach, slope):
    order = jax.random.permutation(stream_key, number_of)
    heavy_load, usual = shares(number_of, rows * top, reach, slope, True), shares(number_of, rows * top, reach, slope, False)
    places = jnp.arange(number_of)

    def named(tallies, offset_by):
        used = int((tallies > 0).sum())
        fixed = max(1, used // 4)
        moved = fixed + (places - fixed + offset_by * (used - fixed)) % max(1, number_of - fixed)
        return jnp.zeros((number_of,), jnp.int32).at[order[jnp.where(places < fixed, places, moved)]].set(jnp.asarray(tallies, jnp.int32))

    tallies = jnp.where(number % 4 == 0, named(heavy_load, number // 4), named(usual, number - number // 4 - 1))
    mixed = jax.random.permutation(jax.random.fold_in(own, 3), number_of)
    source_of, taker = mixed[0:number_of // 2 * 2:2], mixed[1:number_of // 2 * 2:2]
    margin = jnp.minimum(tallies[source_of] - 1, reach - tallies[taker]) // 2
    margin = jnp.where((source_of == order[0]) | (taker == order[0]) | (tallies[taker] == 0), 0, jnp.maximum(margin, 0))
    moved = jax.random.randint(jax.random.fold_in(own, 4), (number_of // 2,), 0, 1 << 20) % (margin + 1)
    tallies = tallies.at[source_of].add(-moved).at[taker].add(moved)
    labels = jnp.searchsorted(jnp.cumsum(tallies), jnp.arange(rows * top), side="right").astype(jnp.int32)
    listing = labels.reshape(top, rows).T
    listing = listing[jax.random.permutation(jax.random.fold_in(own, 1), rows)]
    offset_by = jax.random.randint(jax.random.fold_in(own, 2), (rows, 1), 0, top)
    return jnp.take_along_axis(listing, (jnp.arange(top)[None, :] + offset_by) % top, axis=1)


def shares(amount, total, reach, lean, full):
    portions = [(1 << 20) // math.isqrt(rank ** lean) + 1 for rank in range(1, amount + 1)]
    largest = reach if full else min(reach, max(-(-total // amount), total * portions[0] // sum(portions)))
    least = 1 if total - largest >= amount - 1 else 0
    given, spare = [largest] + [least] * (amount - 1), total - largest - least * (amount - 1)
    while spare > 0:
        free = [i for i in range(1, amount) if given[i] < largest] or [i for i in range(1, amount) if given[i] < reach]
        whole, remaining = sum([portions[i] for i in free]), spare
        for i in free:
            more = min(reach - given[i], max(1, remaining * portions[i] // whole), spare)
            given[i] = given[i] + more
            spare = spare - more
    return np.array(given)


def bell_draw(rng, shape, width, bound, cuts=(), held_as=jnp.bfloat16):
    array = width * jax.random.normal(rng, shape, jnp.float32)
    if cuts:
        array = array * steps_of(rng, shape, cuts, -0.22, 0.18)
    return jnp.clip(array, -bound, bound).astype(held_as)


def setup_inputs(seed: int = 0) -> dict:
    arg_keys = jax.random.split(jax.random.key(seed), 11)
    displacement = bell_draw(arg_keys[0], (3, NZ, NX, NY), 0.3, 4.0, ((2, 4), (3, 8)), jnp.float32)
    velocity = bell_draw(arg_keys[1], (3, NZ, NX, NY), 1.0, 6.0, ((2, 4), (3, 8)), jnp.float32)
    node_mass = jnp.clip(jnp.exp(math.log(2.0) - 1.3862944 * jax.random.uniform(arg_keys[2], (NZ, NX, NY), jnp.float32) ** steps_of(arg_keys[2], (NZ, NX, NY), ((1, 4), (2, 8)), -0.2, 0.2)), 0.5, 2.0)
    moduli = jnp.clip(jnp.exp(math.log(2.0) - 1.3862944 * jax.random.uniform(arg_keys[3], (NZ, NX, NY), jnp.float32) ** steps_of(arg_keys[3], (NZ, NX, NY), ((1, 4), (2, 8)), -0.2, 0.2)), 0.5, 2.0)
    stiffness = draw_stiffness(jax.random.fold_in(arg_keys[10], 71), 0)
    surface_ref = bell_draw(arg_keys[5], (3, NX, NY), 1.0, 6.0, ((1, 4), (2, 8)), jnp.float32)
    facets = bell_draw(arg_keys[6], (OWNERS, SUBPARTS, 6, TF), 1.0, 6.0, ((0, 4), (1, 8)), jnp.float32)
    penalty = jnp.clip(jnp.exp(math.log(4.0) - 2.0794415 * jax.random.uniform(arg_keys[7], (OWNERS, SUBPARTS, TF), jnp.float32) ** steps_of(arg_keys[7], (OWNERS, SUBPARTS, TF), ((0, 4), (1, 8)), -0.2, 0.2)), 0.5, 4.0)
    owners_keys = jax.random.split(jax.random.fold_in(arg_keys[8], 1), STEPS * OWNERS * SUBPARTS * SB // SB)
    owners_turns = jax.random.permutation(jax.random.fold_in(arg_keys[8], 3), STEPS * OWNERS * SUBPARTS * SB // SB)
    owners = jax.vmap(lambda own, number: assign_block(jax.random.fold_in(arg_keys[8], 2), own, number, SB, OWNERS, 1, CAP, 2))(owners_keys, owners_turns).reshape((STEPS, OWNERS, SUBPARTS, SB, 1))
    facet_pairs = touch_ends(jax.random.randint(arg_keys[9], (STEPS, NX, NY), 0, TF), jax.random.fold_in(arg_keys[9], 1), 0, TF - 1).astype(jnp.int32)
    return dict(displacement=displacement, velocity=velocity, node_mass=node_mass, moduli=moduli, stiffness=stiffness, surface_ref=surface_ref, facets=facets, penalty=penalty, owners=owners, facet_pairs=facet_pairs)


TIME_STEP = 0.1
CORNER_SHIFTS = ((0, 0, 0), (0, 0, 1), (0, 1, 0), (0, 1, 1), (1, 0, 0), (1, 0, 1), (1, 1, 0), (1, 1, 1))


def node_forces(node_patch, patch_moduli, stiffness):
    layers = node_patch.shape[1]
    row_count = node_patch.shape[2] - 2
    col_count = node_patch.shape[3] - 2
    element_scale = jnp.zeros((layers - 1, row_count + 1, col_count + 1), jnp.float32)
    corners = []
    for shift_z, shift_x, shift_y in CORNER_SHIFTS:
        element_scale = element_scale + patch_moduli[shift_z:shift_z + layers - 1, shift_x:shift_x + row_count + 1, shift_y:shift_y + col_count + 1]
        corners.append(node_patch[:, shift_z:shift_z + layers - 1, shift_x:shift_x + row_count + 1, shift_y:shift_y + col_count + 1])
    element_scale = element_scale * 0.125
    stacked = jnp.concatenate(corners, axis=0).reshape(24, -1)
    forces = jnp.dot(stiffness, stacked, precision=lax.Precision.HIGHEST).reshape(24, layers - 1, row_count + 1, col_count + 1) * element_scale[None]
    summed = jnp.zeros((3, layers, row_count, col_count), jnp.float32)
    for corner, (shift_z, shift_x, shift_y) in enumerate(CORNER_SHIFTS):
        contribution = forces[3 * corner:3 * corner + 3, :, 1 - shift_x:1 - shift_x + row_count, 1 - shift_y:1 - shift_y + col_count]
        summed = summed.at[:, shift_z:shift_z + layers - 1].add(contribution)
    return summed


def contact_push(points, facet_rows, stiffness_row):
    normal_gap = jnp.sum(facet_rows[3:6] * (points - facet_rows[0:3]), axis=0)
    return facet_rows[3:6] * (stiffness_row * jnp.maximum(-normal_gap, 0.0))[None]


def internal_forces(displacement, moduli, stiffness):
    padded = jnp.pad(displacement, ((0, 0), (0, 0), (1, 1), (1, 1)), mode="wrap")
    padded_moduli = jnp.pad(moduli, ((0, 0), (1, 1), (1, 1)), mode="wrap")
    row_count = displacement.shape[2] // N_MESH

    def one_block(block_index):
        row_start = block_index * row_count
        node_patch = lax.dynamic_slice_in_dim(padded, row_start, row_count + 2, 2)
        patch_moduli = lax.dynamic_slice_in_dim(padded_moduli, row_start, row_count + 2, 1)
        return node_forces(node_patch, patch_moduli, stiffness)

    pieces = lax.map(one_block, jnp.arange(N_MESH, dtype=jnp.int32))
    return pieces.transpose(1, 2, 0, 3, 4).reshape(displacement.shape)


def contact_forces(positions, owner_step, pair_step, facets, penalty):
    groups = facets.shape[0]
    sub_count = facets.shape[1]
    table_width = facets.shape[3]
    row_count = positions.shape[1] // groups
    col_count = positions.shape[2] // sub_count
    points = positions.reshape(3, groups, row_count, sub_count, col_count).transpose(0, 1, 3, 2, 4).reshape(3, -1)
    pair_rows = pair_step.reshape(groups, row_count, sub_count, col_count).transpose(0, 2, 1, 3).reshape(groups, sub_count, -1)
    per_point = jnp.repeat(owner_step[..., 0], BLOCK, axis=2)
    sub_index = jnp.arange(sub_count, dtype=jnp.int32)[None, :, None]
    flat_index = ((per_point * sub_count + sub_index) * table_width + pair_rows).reshape(-1).astype(jnp.int32)
    whole_table = facets.transpose(2, 0, 1, 3).reshape(6, -1)
    facet_rows = jnp.take(whole_table, flat_index, axis=1)
    pushed = contact_push(points, facet_rows, jnp.take(penalty.reshape(-1), flat_index))
    return pushed.reshape(3, groups, sub_count, row_count, col_count).transpose(0, 1, 3, 2, 4).reshape(positions.shape)


def reference(displacement, velocity, node_mass, moduli, stiffness, surface_ref, facets, penalty, owners, facet_pairs):
    for step_index in range(STEPS):
        internal = internal_forces(displacement, moduli, stiffness)
        pushed = contact_forces(surface_ref + displacement[:, 0], owners[step_index], facet_pairs[step_index], facets, penalty)
        net_force = (-internal).at[:, 0].add(pushed)
        velocity = velocity + TIME_STEP * net_force / node_mass[None]
        displacement = displacement + TIME_STEP * velocity
    return displacement, velocity
```

```python
import functools

import jax
import jax.numpy as jnp
from jax import lax
from jax.experimental import pallas as pl
from jax.experimental.pallas import tpu as pltpu
from jax.sharding import PartitionSpec as P

TIME_STEP = 0.1
MESH = pl.DeviceIdType.MESH
ROWS = 8
LANES = 128
GROUP = 8
GROUPS = LANES // GROUP
F32 = jnp.float32
BF16 = jnp.bfloat16
BLOCKS = 9 * 8
DEPTH = BLOCKS + 8
NEAR = [(dq, ds) for dq in (-1, 0, 1) for ds in (-1, 0, 1) if dq or ds]


def roll(x, shift):
    shift %= LANES
    return pltpu.roll(x, shift, 1) if shift else x


def iota(shape, axis):
    return lax.broadcasted_iota(jnp.int32, shape, axis)


def one_hot(condition):
    return jnp.where(condition, 1.0, 0.0).astype(BF16)


def coefficients(stiff):
    high = stiff.astype(BF16)
    low = (stiff - high.astype(F32)).astype(BF16)
    row = iota((32, 24), 0)
    o, b, e = row & 7, row >> 4, (row >> 3) & 1
    wanted = 3 * (4 * (o & 1) + 2 * b + e) + (o >> 1)
    pick = one_hot((wanted == iota((32, 24), 1)) & (o < 6))
    high = jnp.dot(pick, high, preferred_element_type=F32).astype(BF16)
    low = jnp.dot(pick, low, preferred_element_type=F32).astype(BF16)

    def columns(shape):
        col = iota(shape, 1)
        third = jnp.where(col >= DEPTH, 1, 0) + jnp.where(col >= 2 * DEPTH, 1, 0) + jnp.where(col >= 3 * DEPTH, 1, 0)
        rest = col - DEPTH * third
        off, p = rest >> 3, rest & 7
        di = jnp.where(off >= 3, 1, 0) + jnp.where(off >= 6, 1, 0) - 1
        dj = off - 3 * (di + 1) - 1
        return third, di, dj, p, off < 9

    def inside(b2, e2):
        return (b2 >= 0) & (b2 <= 1) & (e2 >= 0) & (e2 <= 1)

    third, di, dj, p, used = columns((24, 256))
    force = None
    for group in range(4):
        b2, e2 = di + (group >> 1), dj + (group & 1)
        wanted = 3 * (4 * (p & 1) + 2 * b2 + e2) + (p >> 1)
        place = used & inside(b2, e2) & (p < 6) & (wanted == iota((24, 256), 0))
        term = jnp.dot(high, one_hot(place & (third < 2)), preferred_element_type=F32)
        term = term + jnp.dot(low, one_hot(place & (third == 2)), preferred_element_type=F32)
        force = term if force is None else jnp.where((iota((32, 256), 0) >> 3) == group, term, force)
    third, di, dj, p, used = columns((32, 256))
    row = iota((32, 256), 0)
    counted = used & inside(di + (row >> 4), dj + ((row >> 3) & 1)) & (p >= 6) & (third < 2)
    return jnp.concatenate([force, jnp.where(counted, 0.125, 0.0)], axis=0).astype(BF16)


def stacked(blocks):
    x = jnp.concatenate(blocks + [jnp.zeros_like(blocks[0])], axis=0)
    high = x.astype(BF16)
    low = (x - high.astype(F32)).astype(BF16)
    return jnp.concatenate([high, low, high, jnp.zeros((256 - 3 * DEPTH, x.shape[1]), BF16)], axis=0)


def kernel(
    n_mesh,
    n_sub,
    width,
    stiff_hbm,
    owners_hbm,
    disp_hbm,
    vel_hbm,
    mass_hbm,
    moduli_hbm,
    surf_hbm,
    facets_hbm,
    penalty_hbm,
    pairs_hbm,
    out_disp,
    out_vel,
    stiff,
    owners,
    own,
    vel,
    mass,
    inverse,
    base,
    pairs,
    raw,
    tables,
    distant,
    edge,
    border,
    edges,
    borders,
    local_sem,
    table_send,
    table_recv,
    edge_send,
    edge_recv,
    border_send,
    border_recv,
):
    q, s = lax.axis_index("mesh"), lax.axis_index("sub")
    chunks = width // LANES
    half = chunks // 2
    bits = width.bit_length() - 1

    def at(dq, ds):
        return (lax.rem(q + dq + n_mesh, n_mesh), lax.rem(s + ds + n_sub, n_sub))

    copies = [
        pltpu.make_async_copy(src, dst, local_sem.at[i])
        for i, (src, dst) in enumerate(
            [
                (disp_hbm, own.at[pl.ds(0, 48)]),
                (moduli_hbm, own.at[pl.ds(48, 16)]),
                (owners_hbm, owners),
                (pairs_hbm, pairs),
                (vel_hbm, vel.at[pl.ds(0, 48)]),
                (mass_hbm, mass),
            ]
            + [(surf_hbm.at[pl.ds(8 * m, 8)], base.at[pl.ds(16 * m, 8)]) for m in range(3)]
            + [
                (facets_hbm, raw.at[pl.ds(0, 6 * chunks)]),
                (penalty_hbm, raw.at[pl.ds(6 * chunks, chunks)]),
                (stiff_hbm, stiff),
            ]
        )
    ]
    for copy in copies:
        copy.start()
    barrier = pltpu.get_barrier_semaphore()
    partners = [(dq, ds) for ds in (0, -1, 1) for dq in range(n_mesh) if dq or ds]
    for device in partners:
        pl.semaphore_signal(barrier, inc=1, device_id=at(*device), device_id_type=MESH)

    lane = iota((8, LANES), 1)
    plane = iota((8, LANES), 0)
    group = lane >> 3
    place_in = lane & 7
    entry = plane < 6
    surface = entry & ((plane & 1) == 0)
    flat = jnp.zeros((8, LANES), F32)
    for p in (1, 3, 5):
        base[pl.ds(8 * p, 8), :] = flat
    base[pl.ds(48, 8), :] = flat - 1.0

    for copy in copies[:9]:
        copy.wait()

    for a in range(2):
        slowness = TIME_STEP / mass[pl.ds(8 * a, 8), :]
        for p in range(a, 8, 2):
            inverse[pl.ds(8 * p, 8), :] = slowness
    holder = jnp.zeros((8, LANES), jnp.int32)
    for b in range(ROWS):
        holder = jnp.where(plane == b, owners[0, b], holder)
    base[pl.ds(56, 8), :] = ((holder << bits) + pairs[pl.ds(0, 8), :]).astype(F32)

    def of_row(ref, i):
        return ref[pl.ds(i, 8, stride=8), :]

    here = {i: of_row(own, i) for i in range(ROWS)}
    gain = {i: of_row(inverse, i) for i in range(ROWS)}
    speed = {i: jnp.where(entry, of_row(vel, i), gain[i]) for i in range(ROWS)}
    point = {i: of_row(base, i) for i in range(ROWS)}
    point = {i: jnp.where(surface, point[i] + here[i], point[i]) for i in range(ROWS)}

    sent = flat
    for g, i in [(i, i) for i in range(ROWS)] + [(8, 0), (9, 1), (14, 6), (15, 7)]:
        deep = roll(here[i], GROUP * g + 4)
        deep = jnp.where(place_in < 2, roll(point[i], GROUP * g + 1), deep)
        deep = jnp.where(place_in > 5, roll(speed[i], GROUP * g + 7), deep)
        sent = jnp.where(group == g, deep, sent)
    edge[...] = sent
    for k, ids in enumerate(((6, 7, 7, 7), (0, 1, 0, 0))):
        for j, (what, i) in enumerate(zip((here, here, speed, point), ids)):
            border[k, pl.ds(8 * j, 8), :] = what[i]

    copies[9].wait()
    copies[10].wait()
    parts = [raw[pl.ds(chunks * c, chunks), :] for c in range(7)]
    root = jnp.sqrt(parts[6])
    normal = [root * parts[3 + m] for m in range(3)]
    offset = normal[0] * parts[0] + normal[1] * parts[1] + normal[2] * parts[2]
    for c, values in enumerate(normal + [offset]):
        for h in range(2):
            tables[q, pl.ds(2 * c + h, half, stride=8), :] = values[half * h : half * (h + 1)]

    pl.semaphore_wait(barrier, len(partners))

    edge_copies = {}
    for i, (dq, ds) in enumerate(NEAR):
        edge_copies[dq, ds] = pltpu.make_async_remote_copy(
            src_ref=edge,
            dst_ref=edges.at[i],
            send_sem=edge_send.at[i],
            recv_sem=edge_recv.at[i],
            device_id=at(-dq, -ds),
            device_id_type=MESH,
        )
    border_copies = [
        pltpu.make_async_remote_copy(
            src_ref=border.at[k],
            dst_ref=borders.at[k],
            send_sem=border_send.at[k],
            recv_sem=border_recv.at[k],
            device_id=at(dq, 0),
            device_id_type=MESH,
        )
        for k, dq in enumerate((1, -1))
    ]
    table_copies = {}
    for i, (dq, ds) in enumerate(partners):
        table_copies[dq, ds] = pltpu.make_async_remote_copy(
            src_ref=tables.at[q],
            dst_ref={0: tables.at[q], 1: distant.at[q], -1: distant.at[n_mesh + q]}[ds],
            send_sem=table_send.at[i],
            recv_sem=table_recv.at[i],
            device_id=at(dq, ds),
            device_id_type=MESH,
        )
    for copy in edge_copies.values():
        copy.start()
    for copy in border_copies:
        copy.start()
    for copy in table_copies.values():
        copy.start()

    copies[11].wait()
    weights = coefficients(stiff[...])

    def elastic(first, second):
        blocks = [jnp.concatenate([a, b], axis=1) for a, b in zip(first, second)]
        got = jnp.dot(weights, stacked(blocks), preferred_element_type=F32)
        terms = [got[8 * g : 8 * g + 8] * got[32 + 8 * g : 40 + 8 * g] for g in range(4)]
        force = (terms[0] + terms[1]) + (terms[2] + terms[3])
        return force[:, :LANES], force[:, LANES:]

    def around(rows, i):
        return [x for di in (-1, 0, 1) for x in rows[i + di]]

    def turned(x):
        return (roll(x, 1), x, roll(x, -1))

    def narrowed(total, second):
        return jnp.where(second, pltpu.roll(total, 7, 0), total)

    def facet_of(step, i):
        index = jnp.broadcast_to(pairs[pl.ds(step * ROWS + i, 1), :], (8, LANES))
        chunk, place = index >> 7, index & (LANES - 1)
        second = chunk >= half
        chunk = jnp.where(second, chunk - half, chunk)
        owner = owners[step, i]
        total = flat
        for k in range(half):
            picked = jnp.take_along_axis(tables[owner, pl.ds(8 * k, 8), :], place, axis=1, mode="promise_in_bounds")
            total = jnp.where(chunk == k, picked, total)
        return narrowed(total, second)

    def facet_by(code, sides, choice):
        code = code.astype(jnp.int32)
        owner, index = code >> bits, code & (width - 1)
        chunk, place = index >> 7, index & (LANES - 1)
        second = chunk >= half
        chunk = jnp.where(second, chunk - half, chunk) + half * owner
        if choice is not None:
            chunk = chunk + choice * (half * n_mesh)
        total = flat
        for side in sides:
            for o in range(n_mesh):
                for k in range(half):
                    ref, at_slot = (distant, (side - 1) * n_mesh + o) if side else (tables, o)
                    rows = ref[at_slot, pl.ds(8 * k, 8), :]
                    picked = jnp.take_along_axis(rows, place, axis=1, mode="promise_in_bounds")
                    total = jnp.where(chunk == (side * n_mesh + o) * half + k, picked, total)
        return narrowed(total, second)

    def push_of(facet, at_point):
        product = jnp.where(surface | (plane == 6), facet * at_point, 0.0)
        product = product + pltpu.roll(product, 4, 0)
        product = product + pltpu.roll(product, 2, 0)
        return jnp.where(surface, facet * jnp.maximum(-product, 0.0), 0.0)

    def ring_step(values, moving, net):
        slow = jnp.where(
            (plane & 1) == 0, jnp.broadcast_to(moving[6:7], (8, LANES)), jnp.broadcast_to(moving[7:8], (8, LANES))
        )
        faster = moving + slow * net
        return jnp.where(entry, values + TIME_STEP * faster, values)

    rows = {i: turned(here[i]) for i in range(ROWS)}
    force = {}
    for i in (1, 3, 5):
        force[i], force[i + 1] = elastic(around(rows, i), around(rows, i + 1))
    for copy in border_copies:
        copy.wait_recv()
    for i, (k, j) in {-2: (0, 0), -1: (0, 1), 8: (1, 0), 9: (1, 1)}.items():
        here[i] = borders[k, pl.ds(8 * j, 8), :]
        rows[i] = turned(here[i])
    force[0], force[7] = elastic(around(rows, 0), around(rows, 7))
    force[-1], force[8] = elastic(around(rows, -1), around(rows, 8))
    for device, copy in table_copies.items():
        if device[1] == 0:
            copy.wait_recv()
    later = {}
    after, fast = {}, {}
    for i in range(ROWS):
        net = push_of(facet_of(0, i), point[i]) - force[i]
        later[i] = facet_of(1, i)
        fast[i] = speed[i] + gain[i] * net
        after[i] = jnp.where(entry, here[i] + TIME_STEP * fast[i], here[i])
    for i, k in ((-1, 0), (8, 1)):
        moving, at_point = borders[k, pl.ds(16, 8), :], borders[k, pl.ds(24, 8), :]
        facet = facet_by(jnp.broadcast_to(at_point[7:8], (8, LANES)), (0,), None)
        after[i] = ring_step(here[i], moving, push_of(facet, at_point) - force[i])
    shifted = {i: (roll(after[i], 1), roll(after[i], -1)) for i in range(-1, 9)}

    for copy in edge_copies.values():
        copy.wait_recv()

    def column(ds):
        middle = sent if ds == 0 else edges[NEAR.index((0, ds))]
        beyond = jnp.where(group < 12, edges[NEAR.index((1, ds))], edges[NEAR.index((-1, ds))])
        return jnp.where(group < 8, middle, beyond)

    left, centre, right = column(-1), column(0), column(1)
    from_before = (place_in == 0) | (place_in == 2) | (place_in == 3) | (place_in == 6)
    strips = [jnp.where(from_before, left, centre), jnp.where(from_before, centre, right)]
    strip_force = elastic(
        *([roll(x, -(GROUP * di + dj)) for di in (-1, 0, 1) for dj in (-1, 0, 1)] for x in strips)
    )
    strip_speed = [roll(x, -3) for x in strips]
    strip_point = [roll(x, 3) for x in strips]
    for device, copy in table_copies.items():
        if device[1] != 0:
            copy.wait_recv()
    strip_after = []
    for k in range(2):
        outer = place_in == (3, 4)[k]
        facet = facet_by(
            jnp.broadcast_to(strip_point[k][7:8], (8, LANES)), (0, 1 + k), jnp.where(outer, 1 + k, 0)
        )
        net = push_of(facet, strip_point[k]) - strip_force[k]
        strip_after.append(ring_step(strips[k], strip_speed[k], net))
    corner = jnp.where(place_in == 4, strip_after[0], strip_after[1])

    rows = {}
    for i in range(-1, 9):
        start = GROUP * (i % GROUPS) + 3
        mid = jnp.where((lane == 0) | (lane == LANES - 1), roll(corner, -(start + 1)), after[i])
        before = jnp.where(lane < 2, roll(strip_after[0], -start), shifted[i][0])
        behind = jnp.where(lane >= LANES - 2, roll(strip_after[1], LANES - 2 - start), shifted[i][1])
        rows[i] = (before, mid, behind)
    for i in range(0, ROWS, 2):
        force[i], force[i + 1] = elastic(around(rows, i), around(rows, i + 1))
    side = (lane == 0) | (lane == LANES - 1)
    for i in range(ROWS):
        mid = rows[i][1]
        at_point = of_row(base, i)
        at_point = jnp.where(surface, at_point + mid, at_point)
        net = push_of(later[i], at_point) - force[i]
        past = jnp.where(side, (mid - here[i]) * (1.0 / TIME_STEP), fast[i])
        past = past + gain[i] * net
        out_vel[pl.ds(i, 6, stride=8), :] = past[0:6]
        out_disp[pl.ds(i, 6, stride=8), :] = (mid + TIME_STEP * past)[0:6]

    for copy in list(edge_copies.values()) + border_copies + list(table_copies.values()):
        copy.wait_send()


def flush(moved, speed, out_moved, out_speed, sem):
    copies = [
        pltpu.make_async_copy(src, dst, sem.at[i])
        for i, (src, dst) in enumerate(((moved, out_moved), (speed, out_speed)))
    ]
    for copy in copies:
        copy.start()
    for copy in copies:
        copy.wait()


def shards(
    displacement,
    velocity,
    node_mass,
    moduli,
    stiffness,
    surface_ref,
    facets,
    penalty,
    owners,
    facet_pairs,
):
    steps = owners.shape[0]
    width = facets.shape[3]
    n_mesh, n_sub = lax.axis_size("mesh"), lax.axis_size("sub")
    assert displacement.shape == (3, 2, ROWS, LANES) and steps == 2
    assert width == 1 << (width.bit_length() - 1) and width >= 2 * LANES
    out = pltpu.VMEM((6 * ROWS, LANES), F32)
    anywhere = pl.BlockSpec(memory_space=pl.ANY)
    vmem = pl.BlockSpec(memory_space=pltpu.VMEM)
    dma = pltpu.SemaphoreType.DMA
    moved, speed = pl.pallas_call(
        functools.partial(kernel, n_mesh, n_sub, width),
        out_shape=(out, out),
        in_specs=[anywhere] * 10,
        out_specs=(vmem, vmem),
        scratch_shapes=[
            pltpu.VMEM((24, 24), F32),
            pltpu.SMEM((steps, ROWS), jnp.int32),
            pltpu.VMEM((8 * ROWS, LANES), F32),
            pltpu.VMEM((8 * ROWS, LANES), F32),
            pltpu.VMEM((2 * ROWS, LANES), F32),
            pltpu.VMEM((8 * ROWS, LANES), F32),
            pltpu.VMEM((8 * ROWS, LANES), F32),
            pltpu.VMEM((steps * ROWS, LANES), jnp.int32),
            pltpu.VMEM((7 * width // LANES, LANES), F32),
            pltpu.VMEM((n_mesh, 4 * width // LANES, LANES), F32),
            pltpu.VMEM((2 * n_mesh, 4 * width // LANES, LANES), F32),
            pltpu.VMEM((8, LANES), F32),
            pltpu.VMEM((2, 32, LANES), F32),
            pltpu.VMEM((8, 8, LANES), F32),
            pltpu.VMEM((2, 32, LANES), F32),
            dma((12,)),
            dma((3 * n_mesh - 1,)),
            dma((3 * n_mesh - 1,)),
            dma((8,)),
            dma((8,)),
            dma((2,)),
            dma((2,)),
        ],
        compiler_params=pltpu.CompilerParams(collective_id=0, has_side_effects=True),
    )(
        stiffness,
        owners.reshape(steps, ROWS),
        displacement.reshape(6 * ROWS, LANES),
        velocity.reshape(6 * ROWS, LANES),
        node_mass.reshape(2 * ROWS, LANES),
        moduli.reshape(2 * ROWS, LANES),
        surface_ref.reshape(3 * ROWS, LANES),
        facets.transpose(0, 2, 1, 3).reshape(6 * width // LANES, LANES),
        penalty.reshape(width // LANES, LANES),
        facet_pairs.reshape(steps * ROWS, LANES),
    )
    moved, speed = pl.pallas_call(
        flush,
        out_shape=[jax.ShapeDtypeStruct((6 * ROWS, LANES), F32)] * 2,
        in_specs=[anywhere, anywhere],
        out_specs=[anywhere, anywhere],
        scratch_shapes=[dma((2,))],
        compiler_params=pltpu.CompilerParams(vmem_limit_bytes=1 << 20),
    )(pltpu.with_memory_space_constraint(moved, pltpu.VMEM), pltpu.with_memory_space_constraint(speed, pltpu.VMEM))
    return moved.reshape(displacement.shape), speed.reshape(velocity.shape)


def solution(mesh):
    in_specs = (
        P(None, None, "mesh", "sub"),
        P(None, None, "mesh", "sub"),
        P(None, "mesh", "sub"),
        P(None, "mesh", "sub"),
        P(),
        P(None, "mesh", "sub"),
        P("mesh", "sub", None, None),
        P("mesh", "sub", None),
        P(None, "mesh", "sub", None, None),
        P(None, "mesh", "sub"),
    )
    out_specs = (P(None, None, "mesh", "sub"), P(None, None, "mesh", "sub"))
    return jax.shard_map(shards, mesh=mesh, in_specs=in_specs, out_specs=out_specs, check_vma=False)
```

```python
import functools

import jax
import jax.numpy as jnp
from jax import lax
from jax.experimental import pallas as pl
from jax.experimental.pallas import tpu as pltpu
from jax.sharding import PartitionSpec as P

TIME_STEP = 0.1
MESH = pl.DeviceIdType.MESH
ROWS = 8
LANES = 128
GROUP = 8
GROUPS = LANES // GROUP
F32 = jnp.float32
BF16 = jnp.bfloat16
BLOCKS = 9 * 8
DEPTH = BLOCKS + 8
NEAR = [(dq, ds) for dq in (-1, 0, 1) for ds in (-1, 0, 1) if dq or ds]


def roll(x, shift):
    shift %= LANES
    return pltpu.roll(x, shift, 1) if shift else x


def iota(shape, axis):
    return lax.broadcasted_iota(jnp.int32, shape, axis)


def one_hot(condition):
    return jnp.where(condition, 1.0, 0.0).astype(BF16)


def coefficients(stiff):
    high = stiff.astype(BF16)
    low = (stiff - high.astype(F32)).astype(BF16)
    row = iota((32, 24), 0)
    o, b, e = row & 7, row >> 4, (row >> 3) & 1
    wanted = 3 * (4 * (o & 1) + 2 * b + e) + (o >> 1)
    pick = one_hot((wanted == iota((32, 24), 1)) & (o < 6))
    high = jnp.dot(pick, high, preferred_element_type=F32).astype(BF16)
    low = jnp.dot(pick, low, preferred_element_type=F32).astype(BF16)

    def columns(shape):
        col = iota(shape, 1)
        third = jnp.where(col >= DEPTH, 1, 0) + jnp.where(col >= 2 * DEPTH, 1, 0) + jnp.where(col >= 3 * DEPTH, 1, 0)
        rest = col - DEPTH * third
        off, p = rest >> 3, rest & 7
        di = jnp.where(off >= 3, 1, 0) + jnp.where(off >= 6, 1, 0) - 1
        dj = off - 3 * (di + 1) - 1
        return third, di, dj, p, off < 9

    def inside(b2, e2):
        return (b2 >= 0) & (b2 <= 1) & (e2 >= 0) & (e2 <= 1)

    third, di, dj, p, used = columns((24, 256))
    force = None
    for group in range(4):
        b2, e2 = di + (group >> 1), dj + (group & 1)
        wanted = 3 * (4 * (p & 1) + 2 * b2 + e2) + (p >> 1)
        place = used & inside(b2, e2) & (p < 6) & (wanted == iota((24, 256), 0))
        term = jnp.dot(high, one_hot(place & (third < 2)), preferred_element_type=F32)
        term = term + jnp.dot(low, one_hot(place & (third == 2)), preferred_element_type=F32)
        force = term if force is None else jnp.where((iota((32, 256), 0) >> 3) == group, term, force)
    third, di, dj, p, used = columns((32, 256))
    row = iota((32, 256), 0)
    counted = used & inside(di + (row >> 4), dj + ((row >> 3) & 1)) & (p >= 6) & (third < 2)
    return jnp.concatenate([force, jnp.where(counted, 0.125, 0.0)], axis=0).astype(BF16)


def stacked(blocks):
    x = jnp.concatenate(blocks + [jnp.zeros_like(blocks[0])], axis=0)
    high = x.astype(BF16)
    low = (x - high.astype(F32)).astype(BF16)
    return jnp.concatenate([high, low, high, jnp.zeros((256 - 3 * DEPTH, x.shape[1]), BF16)], axis=0)


def kernel(
    n_mesh,
    n_sub,
    width,
    stiff_hbm,
    owners_hbm,
    disp_hbm,
    vel_hbm,
    mass_hbm,
    moduli_hbm,
    surf_hbm,
    facets_hbm,
    penalty_hbm,
    pairs_hbm,
    out_disp,
    out_vel,
    stiff,
    owners,
    inbox,
    inverse,
    pairs,
    raw,
    tables,
    distant,
    edge,
    border,
    edges,
    borders,
    sems,
    ready,
):
    q, s = lax.axis_index("mesh"), lax.axis_index("sub")
    own, vel = inbox.at[pl.ds(0, 64)], inbox.at[pl.ds(64, 64)]
    mass, base = inbox.at[pl.ds(112, 16)], inbox.at[pl.ds(128, 64)]
    chunks = width // LANES
    half = chunks // 2
    bits = width.bit_length() - 1

    def at(dq, ds):
        return (lax.rem(q + dq + n_mesh, n_mesh), lax.rem(s + ds + n_sub, n_sub))

    def landed(ref, i):
        return pltpu.make_async_copy(ref, ref, sems.at[i])

    copies = [
        pltpu.make_async_copy(src, dst, sems.at[i])
        for src, dst, i in [
            (disp_hbm, own.at[pl.ds(0, 48)], 0),
            (moduli_hbm, own.at[pl.ds(48, 16)], 0),
            (owners_hbm, owners, 2),
            (pairs_hbm, pairs, 1),
            (vel_hbm, vel.at[pl.ds(0, 48)], 0),
            (mass_hbm, mass, 0),
        ]
        + [(surf_hbm.at[pl.ds(8 * m, 8)], base.at[pl.ds(16 * m, 8)], 0) for m in range(3)]
        + [
            (facets_hbm, raw.at[pl.ds(0, 6 * chunks)], 3),
            (penalty_hbm, raw.at[pl.ds(6 * chunks, chunks)], 3),
            (stiff_hbm, stiff, 4),
        ]
    ]
    for copy in copies:
        copy.start()
    first, last = s == 0, s == n_sub - 1
    partners = [(dq, ds) for ds in (0, 1, -1) for dq in range(n_mesh) if dq or ds]
    barrier = pltpu.get_barrier_semaphore()
    for device in partners:
        if device[1] != 1:
            pl.semaphore_signal(barrier, inc=1, device_id=at(*device), device_id_type=MESH)

    @pl.when(jnp.logical_not(last))
    def _():
        for device in partners:
            if device[1] == 1:
                pl.semaphore_signal(barrier, inc=1, device_id=at(*device), device_id_type=MESH)

    lane = iota((8, LANES), 1)
    plane = iota((8, LANES), 0)
    group = lane >> 3
    place_in = lane & 7
    entry = plane < 6
    surface = entry & ((plane & 1) == 0)
    flat = jnp.zeros((8, LANES), F32)
    for p in (1, 3, 5):
        base[pl.ds(8 * p, 8), :] = flat
    base[pl.ds(48, 8), :] = flat - 1.0

    landed(inbox.at[pl.ds(0, 152)], 0).wait()
    copies[2].wait()
    copies[3].wait()

    for a in range(2):
        slowness = TIME_STEP / mass[pl.ds(8 * a, 8), :]
        for p in range(a, 8, 2):
            inverse[pl.ds(8 * p, 8), :] = slowness
    holder = jnp.zeros((8, LANES), jnp.int32)
    for b in range(ROWS):
        holder = jnp.where(plane == b, owners[0, b], holder)
    base[pl.ds(56, 8), :] = ((holder << bits) + pairs[pl.ds(0, 8), :]).astype(F32)

    def of_row(ref, i):
        return ref[pl.ds(i, 8, stride=8), :]

    here = {i: of_row(own, i) for i in range(ROWS)}
    gain = {i: of_row(inverse, i) for i in range(ROWS)}
    speed = {i: jnp.where(entry, of_row(vel, i), gain[i]) for i in range(ROWS)}
    point = {i: of_row(base, i) for i in range(ROWS)}
    point = {i: jnp.where(surface, point[i] + here[i], point[i]) for i in range(ROWS)}

    sent = flat
    for g, i in [(i, i) for i in range(ROWS)] + [(8, 0), (9, 1), (14, 6), (15, 7)]:
        deep = roll(here[i], GROUP * g + 4)
        deep = jnp.where(place_in < 2, roll(point[i], GROUP * g + 1), deep)
        deep = jnp.where(place_in > 5, roll(speed[i], GROUP * g + 7), deep)
        sent = jnp.where(group == g, deep, sent)
    edge[...] = sent
    for k, ids in enumerate(((6, 7, 7, 7), (0, 1, 0, 0))):
        for j, (what, i) in enumerate(zip((here, here, speed, point), ids)):
            border[k, pl.ds(8 * j, 8), :] = what[i]

    landed(raw, 3).wait()
    parts = [raw[pl.ds(chunks * c, chunks), :] for c in range(7)]
    root = jnp.sqrt(parts[6])
    normal = [root * parts[3 + m] for m in range(3)]
    offset = normal[0] * parts[0] + normal[1] * parts[1] + normal[2] * parts[2]
    for c, values in enumerate(normal + [offset]):
        for h in range(2):
            tables[q, pl.ds(2 * c + h, half, stride=8), :] = values[half * h : half * (h + 1)]

    pl.semaphore_wait(barrier, jnp.where(first, 2 * n_mesh - 1, 3 * n_mesh - 1))

    def send(source, target, device, going, coming):
        return pltpu.make_async_remote_copy(
            src_ref=source,
            dst_ref=target,
            send_sem=sems.at[going],
            recv_sem=sems.at[coming],
            device_id=at(*device),
            device_id_type=MESH,
        )

    edge_copies, table_copies = {}, {}
    for i, (dq, ds) in enumerate(NEAR):
        edge_copies[-dq, -ds] = send(edge, edges.at[i], (-dq, -ds), 5, 9)
    border_copies = [send(border.at[k], borders.at[k], (dq, 0), 6, 10) for k, dq in enumerate((1, -1))]
    for dq, ds in partners:
        target = {0: tables.at[q], 1: distant.at[q], -1: distant.at[n_mesh + q]}[ds]
        table_copies[dq, ds] = send(tables.at[q], target, (dq, ds), 7 if ds == 0 else 8, 11 if ds == 0 else 12)

    def start(side):
        for copies_of in (edge_copies, table_copies):
            for device, copy in copies_of.items():
                if device[1] == side:
                    copy.start()

    @pl.when(last)
    def _():
        start(1)
        for dq in range(n_mesh):
            pl.semaphore_signal(ready, inc=1, device_id=at(dq, 1), device_id_type=MESH)

    for copy in border_copies:
        copy.start()
    start(0)

    @pl.when(jnp.logical_not(last))
    def _():
        start(1)

    @pl.when(first)
    def _():
        pl.semaphore_wait(ready, n_mesh)

    start(-1)

    landed(stiff, 4).wait()
    weights = coefficients(stiff[...])

    def elastic(first, second):
        blocks = [jnp.concatenate([a, b], axis=1) for a, b in zip(first, second)]
        got = jnp.dot(weights, stacked(blocks), preferred_element_type=F32)
        terms = [got[8 * g : 8 * g + 8] * got[32 + 8 * g : 40 + 8 * g] for g in range(4)]
        force = (terms[0] + terms[1]) + (terms[2] + terms[3])
        return force[:, :LANES], force[:, LANES:]

    def around(rows, i):
        return [x for di in (-1, 0, 1) for x in rows[i + di]]

    def turned(x):
        return (roll(x, 1), x, roll(x, -1))

    def narrowed(total, second):
        return jnp.where(second, pltpu.roll(total, 7, 0), total)

    def facet_of(step, i):
        index = jnp.broadcast_to(pairs[pl.ds(step * ROWS + i, 1), :], (8, LANES))
        chunk, place = index >> 7, index & (LANES - 1)
        second = chunk >= half
        chunk = jnp.where(second, chunk - half, chunk)
        owner = owners[step, i]
        total = flat
        for k in range(half):
            picked = jnp.take_along_axis(tables[owner, pl.ds(8 * k, 8), :], place, axis=1, mode="promise_in_bounds")
            total = jnp.where(chunk == k, picked, total)
        return narrowed(total, second)

    def facet_by(code, sides, choice):
        code = code.astype(jnp.int32)
        owner, index = code >> bits, code & (width - 1)
        chunk, place = index >> 7, index & (LANES - 1)
        second = chunk >= half
        chunk = jnp.where(second, chunk - half, chunk) + half * owner
        if choice is not None:
            chunk = chunk + choice * (half * n_mesh)
        total = flat
        for side in sides:
            for o in range(n_mesh):
                for k in range(half):
                    ref, at_slot = (distant, (side - 1) * n_mesh + o) if side else (tables, o)
                    rows = ref[at_slot, pl.ds(8 * k, 8), :]
                    picked = jnp.take_along_axis(rows, place, axis=1, mode="promise_in_bounds")
                    total = jnp.where(chunk == (side * n_mesh + o) * half + k, picked, total)
        return narrowed(total, second)

    def push_of(facet, at_point):
        product = jnp.where(surface | (plane == 6), facet * at_point, 0.0)
        product = product + pltpu.roll(product, 4, 0)
        product = product + pltpu.roll(product, 2, 0)
        return jnp.where(surface, facet * jnp.maximum(-product, 0.0), 0.0)

    def ring_step(values, moving, net):
        slow = jnp.where(
            (plane & 1) == 0, jnp.broadcast_to(moving[6:7], (8, LANES)), jnp.broadcast_to(moving[7:8], (8, LANES))
        )
        faster = moving + slow * net
        return jnp.where(entry, values + TIME_STEP * faster, values)

    rows = {i: turned(here[i]) for i in range(ROWS)}
    force = {}
    for i in (1, 3, 5):
        force[i], force[i + 1] = elastic(around(rows, i), around(rows, i + 1))
    landed(borders, 10).wait()
    for i, (k, j) in {-2: (0, 0), -1: (0, 1), 8: (1, 0), 9: (1, 1)}.items():
        here[i] = borders[k, pl.ds(8 * j, 8), :]
        rows[i] = turned(here[i])
    force[0], force[7] = elastic(around(rows, 0), around(rows, 7))
    force[-1], force[8] = elastic(around(rows, -1), around(rows, 8))
    landed(tables.at[pl.ds(0, n_mesh - 1)], 11).wait()
    later = {}
    after, fast = {}, {}
    for i in range(ROWS):
        net = push_of(facet_of(0, i), point[i]) - force[i]
        later[i] = facet_of(1, i)
        fast[i] = speed[i] + gain[i] * net
        after[i] = jnp.where(entry, here[i] + TIME_STEP * fast[i], here[i])
    for i, k in ((-1, 0), (8, 1)):
        moving, at_point = borders[k, pl.ds(16, 8), :], borders[k, pl.ds(24, 8), :]
        facet = facet_by(jnp.broadcast_to(at_point[7:8], (8, LANES)), (0,), None)
        after[i] = ring_step(here[i], moving, push_of(facet, at_point) - force[i])
    shifted = {i: (roll(after[i], 1), roll(after[i], -1)) for i in range(-1, 9)}

    landed(edges, 9).wait()

    def column(ds):
        middle = sent if ds == 0 else edges[NEAR.index((0, ds))]
        beyond = jnp.where(group < 12, edges[NEAR.index((1, ds))], edges[NEAR.index((-1, ds))])
        return jnp.where(group < 8, middle, beyond)

    left, centre, right = column(-1), column(0), column(1)
    from_before = (place_in == 0) | (place_in == 2) | (place_in == 3) | (place_in == 6)
    strips = [jnp.where(from_before, left, centre), jnp.where(from_before, centre, right)]
    strip_force = elastic(
        *([roll(x, -(GROUP * di + dj)) for di in (-1, 0, 1) for dj in (-1, 0, 1)] for x in strips)
    )
    strip_speed = [roll(x, -3) for x in strips]
    strip_point = [roll(x, 3) for x in strips]
    landed(distant, 12).wait()
    strip_after = []
    for k in range(2):
        outer = place_in == (3, 4)[k]
        facet = facet_by(
            jnp.broadcast_to(strip_point[k][7:8], (8, LANES)), (0, 1 + k), jnp.where(outer, 1 + k, 0)
        )
        net = push_of(facet, strip_point[k]) - strip_force[k]
        strip_after.append(ring_step(strips[k], strip_speed[k], net))
    corner = jnp.where(place_in == 4, strip_after[0], strip_after[1])

    rows = {}
    for i in range(-1, 9):
        start = GROUP * (i % GROUPS) + 3
        mid = jnp.where((lane == 0) | (lane == LANES - 1), roll(corner, -(start + 1)), after[i])
        before = jnp.where(lane < 2, roll(strip_after[0], -start), shifted[i][0])
        behind = jnp.where(lane >= LANES - 2, roll(strip_after[1], LANES - 2 - start), shifted[i][1])
        rows[i] = (before, mid, behind)
    for i in range(0, ROWS, 2):
        force[i], force[i + 1] = elastic(around(rows, i), around(rows, i + 1))
    side = (lane == 0) | (lane == LANES - 1)
    for i in range(ROWS):
        mid = rows[i][1]
        at_point = of_row(base, i)
        at_point = jnp.where(surface, at_point + mid, at_point)
        net = push_of(later[i], at_point) - force[i]
        past = jnp.where(side, (mid - here[i]) * (1.0 / TIME_STEP), fast[i])
        past = past + gain[i] * net
        out_vel[pl.ds(i, 6, stride=8), :] = past[0:6]
        out_disp[pl.ds(i, 6, stride=8), :] = (mid + TIME_STEP * past)[0:6]

    for ref, i in ((edges, 5), (border, 6), (tables.at[pl.ds(0, n_mesh - 1)], 7), (distant, 8)):
        landed(ref, i).wait()


def flush(moved, speed, out_moved, out_speed, sem):
    copies = [
        pltpu.make_async_copy(src, dst, sem.at[i])
        for i, (src, dst) in enumerate(((moved, out_moved), (speed, out_speed)))
    ]
    for copy in copies:
        copy.start()
    for copy in copies:
        copy.wait()


def shards(
    displacement,
    velocity,
    node_mass,
    moduli,
    stiffness,
    surface_ref,
    facets,
    penalty,
    owners,
    facet_pairs,
):
    steps = owners.shape[0]
    width = facets.shape[3]
    n_mesh, n_sub = lax.axis_size("mesh"), lax.axis_size("sub")
    assert displacement.shape == (3, 2, ROWS, LANES) and steps == 2
    assert width == 1 << (width.bit_length() - 1) and width >= 2 * LANES
    out = pltpu.VMEM((6 * ROWS, LANES), F32)
    anywhere = pl.BlockSpec(memory_space=pl.ANY)
    vmem = pl.BlockSpec(memory_space=pltpu.VMEM)
    dma = pltpu.SemaphoreType.DMA
    moved, speed = pl.pallas_call(
        functools.partial(kernel, n_mesh, n_sub, width),
        out_shape=(out, out),
        in_specs=[anywhere] * 10,
        out_specs=(vmem, vmem),
        scratch_shapes=[
            pltpu.VMEM((24, 24), F32),
            pltpu.SMEM((steps, ROWS), jnp.int32),
            pltpu.VMEM((24 * ROWS, LANES), F32),
            pltpu.VMEM((8 * ROWS, LANES), F32),
            pltpu.VMEM((steps * ROWS, LANES), jnp.int32),
            pltpu.VMEM((7 * width // LANES, LANES), F32),
            pltpu.VMEM((n_mesh, 4 * width // LANES, LANES), F32),
            pltpu.VMEM((2 * n_mesh, 4 * width // LANES, LANES), F32),
            pltpu.VMEM((8, LANES), F32),
            pltpu.VMEM((2, 32, LANES), F32),
            pltpu.VMEM((8, 8, LANES), F32),
            pltpu.VMEM((2, 32, LANES), F32),
            dma((13,)),
            pltpu.SemaphoreType.REGULAR,
        ],
        compiler_params=pltpu.CompilerParams(collective_id=0, has_side_effects=True),
    )(
        stiffness,
        owners.reshape(steps, ROWS),
        displacement.reshape(6 * ROWS, LANES),
        velocity.reshape(6 * ROWS, LANES),
        node_mass.reshape(2 * ROWS, LANES),
        moduli.reshape(2 * ROWS, LANES),
        surface_ref.reshape(3 * ROWS, LANES),
        facets.transpose(0, 2, 1, 3).reshape(6 * width // LANES, LANES),
        penalty.reshape(width // LANES, LANES),
        facet_pairs.reshape(steps * ROWS, LANES),
    )
    moved, speed = pl.pallas_call(
        flush,
        out_shape=[jax.ShapeDtypeStruct((6 * ROWS, LANES), F32)] * 2,
        in_specs=[anywhere, anywhere],
        out_specs=[anywhere, anywhere],
        scratch_shapes=[dma((2,))],
        compiler_params=pltpu.CompilerParams(vmem_limit_bytes=1 << 20),
    )(pltpu.with_memory_space_constraint(moved, pltpu.VMEM), pltpu.with_memory_space_constraint(speed, pltpu.VMEM))
    return moved.reshape(displacement.shape), speed.reshape(velocity.shape)


def solution(mesh):
    in_specs = (
        P(None, None, "mesh", "sub"),
        P(None, None, "mesh", "sub"),
        P(None, "mesh", "sub"),
        P(None, "mesh", "sub"),
        P(),
        P(None, "mesh", "sub"),
        P("mesh", "sub", None, None),
        P("mesh", "sub", None),
        P(None, "mesh", "sub", None, None),
        P(None, "mesh", "sub"),
    )
    out_specs = (P(None, None, "mesh", "sub"), P(None, None, "mesh", "sub"))
    return jax.shard_map(shards, mesh=mesh, in_specs=in_specs, out_specs=out_specs, check_vma=False)
```

```python
import functools

import jax
import jax.numpy as jnp
from jax import lax
from jax.experimental import pallas as pl
from jax.experimental.pallas import tpu as pltpu
from jax.sharding import PartitionSpec as P

TIME_STEP = 0.1
MESH = pl.DeviceIdType.MESH
ROWS = 8
LANES = 128
GROUP = 8
GROUPS = LANES // GROUP
F32 = jnp.float32
BF16 = jnp.bfloat16
BLOCKS = 9 * 8
DEPTH = BLOCKS + 8


def roll(x, shift):
    shift %= LANES
    return pltpu.roll(x, shift, 1) if shift else x


def iota(shape, axis):
    return lax.broadcasted_iota(jnp.int32, shape, axis)


def one_hot(condition):
    return jnp.where(condition, 1.0, 0.0).astype(BF16)


def coefficients(stiff):
    high = stiff.astype(BF16)
    low = (stiff - high.astype(F32)).astype(BF16)
    row = iota((32, 24), 0)
    o, b, e = row & 7, row >> 4, (row >> 3) & 1
    wanted = 3 * (4 * (o & 1) + 2 * b + e) + (o >> 1)
    pick = one_hot((wanted == iota((32, 24), 1)) & (o < 6))
    high = jnp.dot(pick, high, preferred_element_type=F32).astype(BF16)
    low = jnp.dot(pick, low, preferred_element_type=F32).astype(BF16)

    def columns(shape):
        col = iota(shape, 1)
        third = jnp.where(col >= DEPTH, 1, 0) + jnp.where(col >= 2 * DEPTH, 1, 0) + jnp.where(col >= 3 * DEPTH, 1, 0)
        rest = col - DEPTH * third
        off, p = rest >> 3, rest & 7
        di = jnp.where(off >= 3, 1, 0) + jnp.where(off >= 6, 1, 0) - 1
        dj = off - 3 * (di + 1) - 1
        return third, di, dj, p, off < 9

    def inside(b2, e2):
        return (b2 >= 0) & (b2 <= 1) & (e2 >= 0) & (e2 <= 1)

    third, di, dj, p, used = columns((24, 256))
    force = None
    for group in range(4):
        b2, e2 = di + (group >> 1), dj + (group & 1)
        wanted = 3 * (4 * (p & 1) + 2 * b2 + e2) + (p >> 1)
        place = used & inside(b2, e2) & (p < 6) & (wanted == iota((24, 256), 0))
        term = jnp.dot(high, one_hot(place & (third < 2)), preferred_element_type=F32)
        term = term + jnp.dot(low, one_hot(place & (third == 2)), preferred_element_type=F32)
        force = term if force is None else jnp.where((iota((32, 256), 0) >> 3) == group, term, force)
    third, di, dj, p, used = columns((32, 256))
    row = iota((32, 256), 0)
    counted = used & inside(di + (row >> 4), dj + ((row >> 3) & 1)) & (p >= 6) & (third < 2)
    return jnp.concatenate([force, jnp.where(counted, 0.125, 0.0)], axis=0).astype(BF16)


def stacked(blocks):
    x = jnp.concatenate(blocks + [jnp.zeros_like(blocks[0])], axis=0)
    high = x.astype(BF16)
    low = (x - high.astype(F32)).astype(BF16)
    return jnp.concatenate([high, low, high, jnp.zeros((256 - 3 * DEPTH, x.shape[1]), BF16)], axis=0)


def kernel(
    n_mesh,
    n_sub,
    width,
    stiff_hbm,
    owners_hbm,
    disp_hbm,
    vel_hbm,
    mass_hbm,
    moduli_hbm,
    surf_hbm,
    facets_hbm,
    penalty_hbm,
    pairs_hbm,
    out_disp,
    out_vel,
    stiff,
    owners,
    inbox,
    inverse,
    pairs,
    raw,
    tables,
    distant,
    edge,
    border,
    edges,
    borders,
    note,
    noted,
    sems,
    ready,
):
    q, s = lax.axis_index("mesh"), lax.axis_index("sub")
    own, vel = inbox.at[pl.ds(0, 64)], inbox.at[pl.ds(64, 64)]
    mass, base = inbox.at[pl.ds(112, 16)], inbox.at[pl.ds(128, 64)]
    chunks = width // LANES
    half = chunks // 2
    bits = width.bit_length() - 1

    def at(dq, ds):
        return (lax.rem(q + dq + n_mesh, n_mesh), lax.rem(s + ds + n_sub, n_sub))

    size = 4 * chunks
    planar = 2 * 8 + 2 * 32 + (n_mesh - 1) * size
    direct = 3 * 8 + n_mesh * size

    def landed(rows, i):
        ref = distant.at[pl.ds(0, rows)]
        return pltpu.make_async_copy(ref, ref, sems.at[i])

    copies = [
        pltpu.make_async_copy(src, dst, sems.at[i])
        for src, dst, i in [
            (disp_hbm, own.at[pl.ds(0, 48)], 0),
            (moduli_hbm, own.at[pl.ds(48, 16)], 0),
            (owners_hbm, owners, 2),
            (pairs_hbm, pairs, 1),
            (vel_hbm, vel.at[pl.ds(0, 48)], 0),
            (mass_hbm, mass, 0),
        ]
        + [(surf_hbm.at[pl.ds(8 * m, 8)], base.at[pl.ds(16 * m, 8)], 0) for m in range(3)]
        + [
            (facets_hbm, raw.at[pl.ds(0, 6 * chunks)], 3),
            (penalty_hbm, raw.at[pl.ds(6 * chunks, chunks)], 3),
            (stiff_hbm, stiff, 4),
        ]
    ]
    for copy in copies:
        copy.start()
    first, last, odd = s == 0, s == n_sub - 1, lax.rem(s, 2) == 1
    from_last, from_above = first, odd & (s != n_sub - 1)
    to_below = jnp.logical_not(odd | first)
    barrier = pltpu.get_barrier_semaphore()

    def hello(dq, ds):
        pl.semaphore_signal(barrier, inc=1, device_id=at(dq, ds), device_id_type=MESH)

    for dq in range(1, n_mesh):
        hello(dq, 0)

    @pl.when(first)
    def _():
        hello(0, 1)
        for dq in range(n_mesh):
            hello(dq, -1)

    @pl.when(jnp.logical_not(first))
    def _():
        hello(0, -1)

    @pl.when(from_above)
    def _():
        for dq in range(n_mesh):
            hello(dq, 1)

    @pl.when(to_below)
    def _():
        hello(0, 1)

    lane = iota((8, LANES), 1)
    plane = iota((8, LANES), 0)
    group = lane >> 3
    place_in = lane & 7
    entry = plane < 6
    surface = entry & ((plane & 1) == 0)
    flat = jnp.zeros((8, LANES), F32)
    for p in (1, 3, 5):
        base[pl.ds(8 * p, 8), :] = flat
    base[pl.ds(48, 8), :] = flat - 1.0

    landed(152, 0).wait()
    copies[2].wait()
    copies[3].wait()

    for a in range(2):
        slowness = TIME_STEP / mass[pl.ds(8 * a, 8), :]
        for p in range(a, 8, 2):
            inverse[pl.ds(8 * p, 8), :] = slowness
    holder = jnp.zeros((8, LANES), jnp.int32)
    for b in range(ROWS):
        holder = jnp.where(plane == b, owners[0, b], holder)
    base[pl.ds(56, 8), :] = ((holder << bits) + pairs[pl.ds(0, 8), :]).astype(F32)

    def of_row(ref, i):
        return ref[pl.ds(i, 8, stride=8), :]

    here = {i: of_row(own, i) for i in range(ROWS)}
    gain = {i: of_row(inverse, i) for i in range(ROWS)}
    speed = {i: jnp.where(entry, of_row(vel, i), gain[i]) for i in range(ROWS)}
    point = {i: of_row(base, i) for i in range(ROWS)}
    point = {i: jnp.where(surface, point[i] + here[i], point[i]) for i in range(ROWS)}

    sent = flat
    for g, i in [(i, i) for i in range(ROWS)] + [(8, 0), (9, 1), (14, 6), (15, 7)]:
        deep = roll(here[i], GROUP * g + 4)
        deep = jnp.where(place_in < 2, roll(point[i], GROUP * g + 1), deep)
        deep = jnp.where(place_in > 5, roll(speed[i], GROUP * g + 7), deep)
        sent = jnp.where(group == g, deep, sent)
    edge[...] = sent
    for k, ids in enumerate(((6, 7, 7, 7), (0, 1, 0, 0))):
        for j, (what, i) in enumerate(zip((here, here, speed, point), ids)):
            border[k, pl.ds(8 * j, 8), :] = what[i]

    landed(7 * chunks, 3).wait()
    parts = [raw[pl.ds(chunks * c, chunks), :] for c in range(7)]
    root = jnp.sqrt(parts[6])
    normal = [root * parts[3 + m] for m in range(3)]
    offset = normal[0] * parts[0] + normal[1] * parts[1] + normal[2] * parts[2]
    for c, values in enumerate(normal + [offset]):
        for h in range(2):
            tables[q, pl.ds(2 * c + h, half, stride=8), :] = values[half * h : half * (h + 1)]

    expected = n_mesh - 1 + jnp.where(first, 1, jnp.where(odd, jnp.where(last, n_mesh + 1, 2), n_mesh + 1))
    pl.semaphore_wait(barrier, expected)

    def send(source, target, device, going, coming):
        return pltpu.make_async_remote_copy(
            src_ref=source,
            dst_ref=target,
            send_sem=sems.at[going],
            recv_sem=sems.at[coming],
            device_id=device,
            device_id_type=MESH,
        )

    def send_direct(ds):
        for dq in (0, 1, -1):
            send(edge, edges.at[2 - dq], at(dq, ds), 6, 13).start()
        for t in range(n_mesh):
            device = (t, lax.rem(s + ds + n_sub, n_sub))
            send(tables.at[q], distant.at[pl.ds(pl.multiple_of(q * size, size), size)], device, 6, 14).start()

    @pl.when(last)
    def _():
        send_direct(1)
        pl.semaphore_signal(ready, inc=1, device_id=at(0, 1), device_id_type=MESH)

    for t in range(n_mesh):
        for k, dq in enumerate((1, -1)):

            @pl.when(lax.rem(q + dq + n_mesh, n_mesh) == t)
            def _():
                send(border.at[k], borders.at[k], (t, s), 5, 9).start()
                send(edge, edges.at[4 * k], (t, s), 5, 9).start()

        @pl.when(q != t)
        def _():
            send(tables.at[q], tables.at[q], (t, s), 5, 10).start()

    @pl.when(to_below)
    def _():
        send_direct(-1)

    copies[11].wait()
    weights = coefficients(stiff[...])

    def elastic(first, second):
        blocks = [jnp.concatenate([a, b], axis=1) for a, b in zip(first, second)]
        got = jnp.dot(weights, stacked(blocks), preferred_element_type=F32)
        terms = [got[8 * g : 8 * g + 8] * got[32 + 8 * g : 40 + 8 * g] for g in range(4)]
        force = (terms[0] + terms[1]) + (terms[2] + terms[3])
        return force[:, :LANES], force[:, LANES:]

    def around(rows, i):
        return [x for di in (-1, 0, 1) for x in rows[i + di]]

    def turned(x):
        return (roll(x, 1), x, roll(x, -1))

    def narrowed(total, second):
        return jnp.where(second, pltpu.roll(total, 7, 0), total)

    def facet_of(step, i):
        index = jnp.broadcast_to(pairs[pl.ds(step * ROWS + i, 1), :], (8, LANES))
        chunk, place = index >> 7, index & (LANES - 1)
        second = chunk >= half
        chunk = jnp.where(second, chunk - half, chunk)
        owner = owners[step, i]
        total = flat
        for k in range(half):
            picked = jnp.take_along_axis(tables[owner, pl.ds(8 * k, 8), :], place, axis=1, mode="promise_in_bounds")
            total = jnp.where(chunk == k, picked, total)
        return narrowed(total, second)

    def facet_by(at_point, ref):
        code = jnp.broadcast_to(at_point[7:8], (8, LANES)).astype(jnp.int32)
        owner, index = code >> bits, code & (width - 1)
        chunk, place = index >> 7, index & (LANES - 1)
        second = chunk >= half
        chunk = jnp.where(second, chunk - half, chunk) + half * owner
        total = flat
        for k in range(half * n_mesh):
            rows = ref(k)
            picked = jnp.take_along_axis(rows, place, axis=1, mode="promise_in_bounds")
            total = jnp.where(chunk == k, picked, total)
        return narrowed(total, second)

    def of_plane(k):
        return tables[k // half, pl.ds(8 * (k % half), 8), :]

    def of_side(k):
        return distant[pl.ds(8 * k, 8), :]

    def push_of(facet, at_point):
        product = jnp.where(surface | (plane == 6), facet * at_point, 0.0)
        product = product + pltpu.roll(product, 4, 0)
        product = product + pltpu.roll(product, 2, 0)
        return jnp.where(surface, facet * jnp.maximum(-product, 0.0), 0.0)

    def ring_step(values, moving, net):
        slow = jnp.where(
            (plane & 1) == 0, jnp.broadcast_to(moving[6:7], (8, LANES)), jnp.broadcast_to(moving[7:8], (8, LANES))
        )
        faster = moving + slow * net
        return jnp.where(entry, values + TIME_STEP * faster, values)

    rows = {i: turned(here[i]) for i in range(ROWS)}
    force = {}
    for i in (1, 3, 5):
        force[i], force[i + 1] = elastic(around(rows, i), around(rows, i + 1))
    landed(2 * 8 + 2 * 32, 9).wait()
    for i, (k, j) in {-2: (0, 0), -1: (0, 1), 8: (1, 0), 9: (1, 1)}.items():
        here[i] = borders[k, pl.ds(8 * j, 8), :]
        rows[i] = turned(here[i])
    force[0], force[7] = elastic(around(rows, 0), around(rows, 7))
    force[-1], force[8] = elastic(around(rows, -1), around(rows, 8))

    def column(middle, before, behind):
        return jnp.where(group < 8, middle, jnp.where(group < 12, behind, before))

    centre = column(sent, edges[0], edges[4])
    landed((n_mesh - 1) * size, 10).wait()
    own_point = roll(centre, 3)
    own_push = push_of(facet_by(own_point, of_plane), own_point)

    note[0] = centre
    note[1] = own_push

    @pl.when(jnp.logical_not(last))
    def _():
        send(note, noted.at[0], at(0, 1), 7, 11).start()

    @pl.when(odd)
    def _():
        send(note, noted.at[1], at(0, -1), 8, 12).start()

    @pl.when(first)
    def _():
        pl.semaphore_wait(ready, 1)
        send(note, noted.at[1], at(0, -1), 8, 12).start()

    later = {}
    after, fast = {}, {}
    for i in range(ROWS):
        net = push_of(facet_of(0, i), point[i]) - force[i]
        later[i] = facet_of(1, i)
        fast[i] = speed[i] + gain[i] * net
        after[i] = jnp.where(entry, here[i] + TIME_STEP * fast[i], here[i])
    for i, k in ((-1, 0), (8, 1)):
        moving, at_point = borders[k, pl.ds(16, 8), :], borders[k, pl.ds(24, 8), :]
        facet = facet_by(at_point, of_plane)
        after[i] = ring_step(here[i], moving, push_of(facet, at_point) - force[i])
    shifted = {i: (roll(after[i], 1), roll(after[i], -1)) for i in range(-1, 9)}

    has_direct = from_last | from_above

    @pl.when(jnp.logical_not(from_above))
    def _():
        landed(2 * 8, 12).wait()

    @pl.when(jnp.logical_not(first))
    def _():
        landed(2 * 8, 11).wait()

    @pl.when(has_direct)
    def _():
        landed(3 * 8, 13).wait()

    far = column(edges[2], edges[1], edges[3])
    left, right = jnp.where(from_last, far, noted[0, 0]), jnp.where(from_above, far, noted[1, 0])
    from_before = (place_in == 0) | (place_in == 2) | (place_in == 3) | (place_in == 6)
    strips = [jnp.where(from_before, left, centre), jnp.where(from_before, centre, right)]
    strip_force = elastic(
        *([roll(x, -(GROUP * di + dj)) for di in (-1, 0, 1) for dj in (-1, 0, 1)] for x in strips)
    )
    strip_speed = [roll(x, -3) for x in strips]
    far_point = roll(far, 3)

    @pl.when(has_direct)
    def _():
        landed(n_mesh * size, 14).wait()

    far_push = push_of(facet_by(far_point, of_side), far_point)
    strip_after = []
    for k, by_far in enumerate((from_last, from_above)):
        push = jnp.where(by_far, far_push, noted[k, 1])
        push = jnp.where(place_in == (3, 4)[k], push, own_push)
        strip_after.append(ring_step(strips[k], strip_speed[k], push - strip_force[k]))
    corner = jnp.where(place_in == 4, strip_after[0], strip_after[1])

    rows = {}
    for i in range(-1, 9):
        start = GROUP * (i % GROUPS) + 3
        mid = jnp.where((lane == 0) | (lane == LANES - 1), roll(corner, -(start + 1)), after[i])
        before = jnp.where(lane < 2, roll(strip_after[0], -start), shifted[i][0])
        behind = jnp.where(lane >= LANES - 2, roll(strip_after[1], LANES - 2 - start), shifted[i][1])
        rows[i] = (before, mid, behind)
    for i in range(0, ROWS, 2):
        force[i], force[i + 1] = elastic(around(rows, i), around(rows, i + 1))
    side = (lane == 0) | (lane == LANES - 1)
    for i in range(ROWS):
        mid = rows[i][1]
        at_point = of_row(base, i)
        at_point = jnp.where(surface, at_point + mid, at_point)
        net = push_of(later[i], at_point) - force[i]
        past = jnp.where(side, (mid - here[i]) * (1.0 / TIME_STEP), fast[i])
        past = past + gain[i] * net
        out_vel[pl.ds(i, 6, stride=8), :] = past[0:6]
        out_disp[pl.ds(i, 6, stride=8), :] = (mid + TIME_STEP * past)[0:6]

    landed(planar, 5).wait()

    @pl.when(to_below | last)
    def _():
        landed(direct, 6).wait()

    @pl.when(jnp.logical_not(last))
    def _():
        landed(2 * 8, 7).wait()

    @pl.when(odd | first)
    def _():
        landed(2 * 8, 8).wait()


def flush(moved, speed, out_moved, out_speed, sem):
    copies = [
        pltpu.make_async_copy(src, dst, sem.at[i])
        for i, (src, dst) in enumerate(((moved, out_moved), (speed, out_speed)))
    ]
    for copy in copies:
        copy.start()
    for copy in copies:
        copy.wait()


def shards(
    displacement,
    velocity,
    node_mass,
    moduli,
    stiffness,
    surface_ref,
    facets,
    penalty,
    owners,
    facet_pairs,
):
    steps = owners.shape[0]
    width = facets.shape[3]
    n_mesh, n_sub = lax.axis_size("mesh"), lax.axis_size("sub")
    assert displacement.shape == (3, 2, ROWS, LANES) and steps == 2 and n_sub % 2 == 0
    assert width == 1 << (width.bit_length() - 1) and width >= 2 * LANES
    out = pltpu.VMEM((6 * ROWS, LANES), F32)
    anywhere = pl.BlockSpec(memory_space=pl.ANY)
    vmem = pl.BlockSpec(memory_space=pltpu.VMEM)
    dma = pltpu.SemaphoreType.DMA
    moved, speed = pl.pallas_call(
        functools.partial(kernel, n_mesh, n_sub, width),
        out_shape=(out, out),
        in_specs=[anywhere] * 10,
        out_specs=(vmem, vmem),
        scratch_shapes=[
            pltpu.VMEM((24, 24), F32),
            pltpu.SMEM((steps, ROWS), jnp.int32),
            pltpu.VMEM((24 * ROWS, LANES), F32),
            pltpu.VMEM((8 * ROWS, LANES), F32),
            pltpu.VMEM((steps * ROWS, LANES), jnp.int32),
            pltpu.VMEM((7 * width // LANES, LANES), F32),
            pltpu.VMEM((n_mesh, 4 * width // LANES, LANES), F32),
            pltpu.VMEM((n_mesh * 4 * width // LANES + 128, LANES), F32),
            pltpu.VMEM((8, LANES), F32),
            pltpu.VMEM((2, 32, LANES), F32),
            pltpu.VMEM((5, 8, LANES), F32),
            pltpu.VMEM((2, 32, LANES), F32),
            pltpu.VMEM((2, 8, LANES), F32),
            pltpu.VMEM((2, 2, 8, LANES), F32),
            dma((15,)),
            pltpu.SemaphoreType.REGULAR,
        ],
        compiler_params=pltpu.CompilerParams(collective_id=0, has_side_effects=True),
    )(
        stiffness,
        owners.reshape(steps, ROWS),
        displacement.reshape(6 * ROWS, LANES),
        velocity.reshape(6 * ROWS, LANES),
        node_mass.reshape(2 * ROWS, LANES),
        moduli.reshape(2 * ROWS, LANES),
        surface_ref.reshape(3 * ROWS, LANES),
        facets.transpose(0, 2, 1, 3).reshape(6 * width // LANES, LANES),
        penalty.reshape(width // LANES, LANES),
        facet_pairs.reshape(steps * ROWS, LANES),
    )
    moved, speed = pl.pallas_call(
        flush,
        out_shape=[jax.ShapeDtypeStruct((6 * ROWS, LANES), F32)] * 2,
        in_specs=[anywhere, anywhere],
        out_specs=[anywhere, anywhere],
        scratch_shapes=[dma((2,))],
        compiler_params=pltpu.CompilerParams(vmem_limit_bytes=1 << 20),
    )(pltpu.with_memory_space_constraint(moved, pltpu.VMEM), pltpu.with_memory_space_constraint(speed, pltpu.VMEM))
    return moved.reshape(displacement.shape), speed.reshape(velocity.shape)


def solution(mesh):
    in_specs = (
        P(None, None, "mesh", "sub"),
        P(None, None, "mesh", "sub"),
        P(None, "mesh", "sub"),
        P(None, "mesh", "sub"),
        P(),
        P(None, "mesh", "sub"),
        P("mesh", "sub", None, None),
        P("mesh", "sub", None),
        P(None, "mesh", "sub", None, None),
        P(None, "mesh", "sub"),
    )
    out_specs = (P(None, None, "mesh", "sub"), P(None, None, "mesh", "sub"))
    return jax.shard_map(shards, mesh=mesh, in_specs=in_specs, out_specs=out_specs, check_vma=False)
```

```python
import functools

import jax
import jax.numpy as jnp
from jax import lax
from jax.experimental import pallas as pl
from jax.experimental.pallas import tpu as pltpu
from jax.sharding import PartitionSpec as P

TIME_STEP = 0.1
MESH = pl.DeviceIdType.MESH
ROWS = 8
LANES = 128
GROUP = 8
GROUPS = LANES // GROUP
F32 = jnp.float32
BF16 = jnp.bfloat16
BLOCKS = 9 * 8
DEPTH = BLOCKS + 8


def roll(x, shift):
    shift %= LANES
    return pltpu.roll(x, shift, 1) if shift else x


def iota(shape, axis):
    return lax.broadcasted_iota(jnp.int32, shape, axis)


def one_hot(condition):
    return jnp.where(condition, 1.0, 0.0).astype(BF16)


def coefficients(stiff):
    high = stiff.astype(BF16)
    low = (stiff - high.astype(F32)).astype(BF16)
    row = iota((32, 24), 0)
    o, b, e = row & 7, row >> 4, (row >> 3) & 1
    wanted = 3 * (4 * (o & 1) + 2 * b + e) + (o >> 1)
    pick = one_hot((wanted == iota((32, 24), 1)) & (o < 6))
    high = jnp.dot(pick, high, preferred_element_type=F32).astype(BF16)
    low = jnp.dot(pick, low, preferred_element_type=F32).astype(BF16)

    def columns(shape):
        col = iota(shape, 1)
        third = jnp.where(col >= DEPTH, 1, 0) + jnp.where(col >= 2 * DEPTH, 1, 0) + jnp.where(col >= 3 * DEPTH, 1, 0)
        rest = col - DEPTH * third
        off, p = rest >> 3, rest & 7
        di = jnp.where(off >= 3, 1, 0) + jnp.where(off >= 6, 1, 0) - 1
        dj = off - 3 * (di + 1) - 1
        return third, di, dj, p, off < 9

    def inside(b2, e2):
        return (b2 >= 0) & (b2 <= 1) & (e2 >= 0) & (e2 <= 1)

    third, di, dj, p, used = columns((24, 256))
    force = None
    for group in range(4):
        b2, e2 = di + (group >> 1), dj + (group & 1)
        wanted = 3 * (4 * (p & 1) + 2 * b2 + e2) + (p >> 1)
        place = used & inside(b2, e2) & (p < 6) & (wanted == iota((24, 256), 0))
        term = jnp.dot(high, one_hot(place & (third < 2)), preferred_element_type=F32)
        term = term + jnp.dot(low, one_hot(place & (third == 2)), preferred_element_type=F32)
        force = term if force is None else jnp.where((iota((32, 256), 0) >> 3) == group, term, force)
    third, di, dj, p, used = columns((32, 256))
    row = iota((32, 256), 0)
    counted = used & inside(di + (row >> 4), dj + ((row >> 3) & 1)) & (p >= 6) & (third < 2)
    return jnp.concatenate([force, jnp.where(counted, 0.125, 0.0)], axis=0).astype(BF16)


def stacked(blocks):
    x = jnp.concatenate(blocks + [jnp.zeros_like(blocks[0])], axis=0)
    high = x.astype(BF16)
    low = (x - high.astype(F32)).astype(BF16)
    return jnp.concatenate([high, low, high, jnp.zeros((256 - 3 * DEPTH, x.shape[1]), BF16)], axis=0)


def kernel(
    n_mesh,
    n_sub,
    width,
    stiff_hbm,
    owners_hbm,
    disp_hbm,
    vel_hbm,
    mass_hbm,
    moduli_hbm,
    surf_hbm,
    facets_hbm,
    penalty_hbm,
    pairs_hbm,
    out_disp,
    out_vel,
    stiff,
    owners,
    inbox,
    inverse,
    pairs,
    raw,
    tables,
    distant,
    edge,
    border,
    edges,
    borders,
    note,
    noted,
    sems,
    ready,
):
    q, s = lax.axis_index("mesh"), lax.axis_index("sub")
    own, vel = inbox.at[pl.ds(0, 64)], inbox.at[pl.ds(64, 64)]
    mass, base = inbox.at[pl.ds(112, 16)], inbox.at[pl.ds(128, 64)]
    chunks = width // LANES
    half = chunks // 2
    bits = width.bit_length() - 1

    def at(dq, ds):
        return (lax.rem(q + dq + n_mesh, n_mesh), lax.rem(s + ds + n_sub, n_sub))

    size = 4 * chunks
    planar = 2 * 8 + 2 * 32 + (n_mesh - 1) * size
    direct = 3 * 8 + n_mesh * size

    def landed(rows, i):
        ref = distant.at[pl.ds(0, rows)]
        return pltpu.make_async_copy(ref, ref, sems.at[i])

    copies = [
        pltpu.make_async_copy(src, dst, sems.at[i])
        for src, dst, i in [
            (disp_hbm, own.at[pl.ds(0, 48)], 0),
            (moduli_hbm, own.at[pl.ds(48, 16)], 0),
            (owners_hbm, owners, 1),
            (pairs_hbm, pairs, 0),
            (vel_hbm, vel.at[pl.ds(0, 48)], 0),
            (mass_hbm, mass, 0),
        ]
        + [(surf_hbm.at[pl.ds(8 * m, 8)], base.at[pl.ds(16 * m, 8)], 0) for m in range(3)]
        + [
            (facets_hbm, raw.at[pl.ds(0, 6 * chunks)], 2),
            (penalty_hbm, raw.at[pl.ds(6 * chunks, chunks)], 2),
            (stiff_hbm, stiff, 3),
        ]
    ]
    for copy in copies:
        copy.start()
    first, last, odd = s == 0, s == n_sub - 1, lax.rem(s, 2) == 1
    from_last, from_above = first, odd & (s != n_sub - 1)
    to_below = jnp.logical_not(odd | first)
    barrier = pltpu.get_barrier_semaphore()

    def hello(dq, ds):
        pl.semaphore_signal(barrier, inc=1, device_id=at(dq, ds), device_id_type=MESH)

    for dq in range(1, n_mesh):
        hello(dq, 0)

    @pl.when(first)
    def _():
        hello(0, 1)
        for dq in range(n_mesh):
            hello(dq, -1)

    @pl.when(jnp.logical_not(first))
    def _():
        hello(0, -1)

    @pl.when(from_above)
    def _():
        for dq in range(n_mesh):
            hello(dq, 1)

    @pl.when(to_below)
    def _():
        hello(0, 1)

    lane = iota((8, LANES), 1)
    plane = iota((8, LANES), 0)
    group = lane >> 3
    place_in = lane & 7
    entry = plane < 6
    surface = entry & ((plane & 1) == 0)
    flat = jnp.zeros((8, LANES), F32)
    for p in (1, 3, 5):
        base[pl.ds(8 * p, 8), :] = flat
    base[pl.ds(48, 8), :] = flat - 1.0

    landed(152 + 16, 0).wait()
    copies[2].wait()

    for a in range(2):
        slowness = TIME_STEP / mass[pl.ds(8 * a, 8), :]
        for p in range(a, 8, 2):
            inverse[pl.ds(8 * p, 8), :] = slowness
    holder = jnp.zeros((8, LANES), jnp.int32)
    for b in range(ROWS):
        holder = jnp.where(plane == b, owners[0, b], holder)
    base[pl.ds(56, 8), :] = ((holder << bits) + pairs[pl.ds(0, 8), :]).astype(F32)

    def of_row(ref, i):
        return ref[pl.ds(i, 8, stride=8), :]

    here = {i: of_row(own, i) for i in range(ROWS)}
    gain = {i: of_row(inverse, i) for i in range(ROWS)}
    speed = {i: jnp.where(entry, of_row(vel, i), gain[i]) for i in range(ROWS)}
    point = {i: of_row(base, i) for i in range(ROWS)}
    point = {i: jnp.where(surface, point[i] + here[i], point[i]) for i in range(ROWS)}

    sent = flat
    for g, i in [(i, i) for i in range(ROWS)] + [(8, 0), (9, 1), (14, 6), (15, 7)]:
        deep = roll(here[i], GROUP * g + 4)
        deep = jnp.where(place_in < 2, roll(point[i], GROUP * g + 1), deep)
        deep = jnp.where(place_in > 5, roll(speed[i], GROUP * g + 7), deep)
        sent = jnp.where(group == g, deep, sent)
    edge[...] = sent
    for k, ids in enumerate(((6, 7, 7, 7), (0, 1, 0, 0))):
        for j, (what, i) in enumerate(zip((here, here, speed, point), ids)):
            border[k, pl.ds(8 * j, 8), :] = what[i]

    landed(7 * chunks, 2).wait()
    parts = [raw[pl.ds(chunks * c, chunks), :] for c in range(7)]
    root = jnp.sqrt(parts[6])
    normal = [root * parts[3 + m] for m in range(3)]
    offset = normal[0] * parts[0] + normal[1] * parts[1] + normal[2] * parts[2]
    for c, values in enumerate(normal + [offset]):
        for h in range(2):
            tables[q, pl.ds(2 * c + h, half, stride=8), :] = values[half * h : half * (h + 1)]

    expected = n_mesh - 1 + jnp.where(first, 1, jnp.where(odd, jnp.where(last, n_mesh + 1, 2), n_mesh + 1))
    pl.semaphore_wait(barrier, expected)

    def send(source, target, device, going, coming):
        return pltpu.make_async_remote_copy(
            src_ref=source,
            dst_ref=target,
            send_sem=sems.at[going],
            recv_sem=sems.at[coming],
            device_id=device,
            device_id_type=MESH,
        )

    def send_direct(ds):
        place = pl.multiple_of(q * size, size)

        def to(t):
            device = (t, lax.rem(s + ds + n_sub, n_sub))
            send(tables.at[q], distant.at[pl.ds(place, size)], device, 1, 8).start()

        def edge_to(dq):
            send(edge, edges.at[2 - dq], at(dq, ds), 1, 7).start()

        for dq in (0, 1, -1):

            @pl.when(at(dq, 0)[0] == 0)
            def _():
                edge_to(dq)

        to(0)
        for dq in (0, 1, -1):

            @pl.when(at(dq, 0)[0] != 0)
            def _():
                edge_to(dq)

        for t in range(1, n_mesh):
            to(t)

    @pl.when(last)
    def _():
        send_direct(1)
        pl.semaphore_signal(ready, inc=1, device_id=at(0, 1), device_id_type=MESH)

    for t in range(n_mesh):
        for k, dq in enumerate((1, -1)):

            @pl.when(lax.rem(q + dq + n_mesh, n_mesh) == t)
            def _():
                send(border.at[k], borders.at[k], (t, s), 0, 4).start()
                send(edge, edges.at[4 * k], (t, s), 0, 4).start()

        @pl.when(q != t)
        def _():
            send(tables.at[q], tables.at[q], (t, s), 0, 5).start()

    @pl.when(to_below)
    def _():
        send_direct(-1)

    copies[11].wait()
    weights = coefficients(stiff[...])

    def elastic(first, second):
        blocks = [jnp.concatenate([a, b], axis=1) for a, b in zip(first, second)]
        got = jnp.dot(weights, stacked(blocks), preferred_element_type=F32)
        terms = [got[8 * g : 8 * g + 8] * got[32 + 8 * g : 40 + 8 * g] for g in range(4)]
        force = (terms[0] + terms[1]) + (terms[2] + terms[3])
        return force[:, :LANES], force[:, LANES:]

    def around(rows, i):
        return [x for di in (-1, 0, 1) for x in rows[i + di]]

    def turned(x):
        return (roll(x, 1), x, roll(x, -1))

    def narrowed(total, second):
        return jnp.where(second, pltpu.roll(total, 7, 0), total)

    def facet_of(step, i):
        index = jnp.broadcast_to(pairs[pl.ds(step * ROWS + i, 1), :], (8, LANES))
        chunk, place = index >> 7, index & (LANES - 1)
        second = chunk >= half
        chunk = jnp.where(second, chunk - half, chunk)
        owner = owners[step, i]
        total = flat
        for k in range(half):
            picked = jnp.take_along_axis(tables[owner, pl.ds(8 * k, 8), :], place, axis=1, mode="promise_in_bounds")
            total = jnp.where(chunk == k, picked, total)
        return narrowed(total, second)

    def facet_by(at_point, ref):
        code = jnp.broadcast_to(at_point[7:8], (8, LANES)).astype(jnp.int32)
        owner, index = code >> bits, code & (width - 1)
        chunk, place = index >> 7, index & (LANES - 1)
        second = chunk >= half
        chunk = jnp.where(second, chunk - half, chunk) + half * owner
        total = flat
        for k in range(half * n_mesh):
            rows = ref(k)
            picked = jnp.take_along_axis(rows, place, axis=1, mode="promise_in_bounds")
            total = jnp.where(chunk == k, picked, total)
        return narrowed(total, second)

    def of_plane(k):
        return tables[k // half, pl.ds(8 * (k % half), 8), :]

    def of_side(k):
        return distant[pl.ds(8 * k, 8), :]

    def push_of(facet, at_point):
        product = jnp.where(surface | (plane == 6), facet * at_point, 0.0)
        product = product + pltpu.roll(product, 4, 0)
        product = product + pltpu.roll(product, 2, 0)
        return jnp.where(surface, facet * jnp.maximum(-product, 0.0), 0.0)

    def ring_step(values, moving, net):
        slow = jnp.where(
            (plane & 1) == 0, jnp.broadcast_to(moving[6:7], (8, LANES)), jnp.broadcast_to(moving[7:8], (8, LANES))
        )
        faster = moving + slow * net
        return jnp.where(entry, values + TIME_STEP * faster, values)

    rows = {i: turned(here[i]) for i in range(ROWS)}
    force = {}
    for i in (1, 3, 5):
        force[i], force[i + 1] = elastic(around(rows, i), around(rows, i + 1))
    landed(2 * 8 + 2 * 32, 4).wait()
    for i, (k, j) in {-2: (0, 0), -1: (0, 1), 8: (1, 0), 9: (1, 1)}.items():
        here[i] = borders[k, pl.ds(8 * j, 8), :]
        rows[i] = turned(here[i])
    force[0], force[7] = elastic(around(rows, 0), around(rows, 7))
    force[-1], force[8] = elastic(around(rows, -1), around(rows, 8))

    def column(middle, before, behind):
        return jnp.where(group < 8, middle, jnp.where(group < 12, behind, before))

    centre = column(sent, edges[0], edges[4])
    landed((n_mesh - 1) * size, 5).wait()
    own_point = roll(centre, 3)
    own_push = push_of(facet_by(own_point, of_plane), own_point)

    note[0] = centre
    note[1] = own_push

    @pl.when(jnp.logical_not(last))
    def _():
        send(note, noted.at[0], at(0, 1), 2, 6).start()

    @pl.when(odd)
    def _():
        send(note, noted.at[1], at(0, -1), 3, 6).start()

    @pl.when(first)
    def _():
        pl.semaphore_wait(ready, 1)
        send(note, noted.at[1], at(0, -1), 3, 6).start()

    later = {}
    after, fast = {}, {}
    for i in range(ROWS):
        net = push_of(facet_of(0, i), point[i]) - force[i]
        later[i] = facet_of(1, i)
        fast[i] = speed[i] + gain[i] * net
        after[i] = jnp.where(entry, here[i] + TIME_STEP * fast[i], here[i])
    for i, k in ((-1, 0), (8, 1)):
        moving, at_point = borders[k, pl.ds(16, 8), :], borders[k, pl.ds(24, 8), :]
        facet = facet_by(at_point, of_plane)
        after[i] = ring_step(here[i], moving, push_of(facet, at_point) - force[i])
    shifted = {i: (roll(after[i], 1), roll(after[i], -1)) for i in range(-1, 9)}

    has_direct = from_last | from_above

    @pl.when(jnp.logical_not(has_direct))
    def _():
        landed(2 * 2 * 8, 6).wait()

    @pl.when(has_direct)
    def _():
        landed(2 * 8, 6).wait()
        landed(3 * 8, 7).wait()

    far = column(edges[2], edges[1], edges[3])
    left, right = jnp.where(from_last, far, noted[0, 0]), jnp.where(from_above, far, noted[1, 0])
    from_before = (place_in == 0) | (place_in == 2) | (place_in == 3) | (place_in == 6)
    strips = [jnp.where(from_before, left, centre), jnp.where(from_before, centre, right)]
    strip_force = elastic(
        *([roll(x, -(GROUP * di + dj)) for di in (-1, 0, 1) for dj in (-1, 0, 1)] for x in strips)
    )
    strip_speed = [roll(x, -3) for x in strips]
    far_point = roll(far, 3)

    @pl.when(has_direct)
    def _():
        landed(n_mesh * size, 8).wait()

    far_push = push_of(facet_by(far_point, of_side), far_point)
    strip_after = []
    for k, by_far in enumerate((from_last, from_above)):
        push = jnp.where(by_far, far_push, noted[k, 1])
        push = jnp.where(place_in == (3, 4)[k], push, own_push)
        strip_after.append(ring_step(strips[k], strip_speed[k], push - strip_force[k]))
    corner = jnp.where(place_in == 4, strip_after[0], strip_after[1])

    rows = {}
    for i in range(-1, 9):
        start = GROUP * (i % GROUPS) + 3
        mid = jnp.where((lane == 0) | (lane == LANES - 1), roll(corner, -(start + 1)), after[i])
        before = jnp.where(lane < 2, roll(strip_after[0], -start), shifted[i][0])
        behind = jnp.where(lane >= LANES - 2, roll(strip_after[1], LANES - 2 - start), shifted[i][1])
        rows[i] = (before, mid, behind)
    for i in range(0, ROWS, 2):
        force[i], force[i + 1] = elastic(around(rows, i), around(rows, i + 1))
    side = (lane == 0) | (lane == LANES - 1)
    for i in range(ROWS):
        mid = rows[i][1]
        at_point = of_row(base, i)
        at_point = jnp.where(surface, at_point + mid, at_point)
        net = push_of(later[i], at_point) - force[i]
        past = jnp.where(side, (mid - here[i]) * (1.0 / TIME_STEP), fast[i])
        past = past + gain[i] * net
        out_vel[pl.ds(i, 6, stride=8), :] = past[0:6]
        out_disp[pl.ds(i, 6, stride=8), :] = (mid + TIME_STEP * past)[0:6]

    landed(planar, 0).wait()

    @pl.when(to_below | last)
    def _():
        landed(direct, 1).wait()

    @pl.when(jnp.logical_not(last))
    def _():
        landed(2 * 8, 2).wait()

    @pl.when(odd | first)
    def _():
        landed(2 * 8, 3).wait()


def flush(moved, speed, out_moved, out_speed, sem):
    copies = [
        pltpu.make_async_copy(src, dst, sem.at[i])
        for i, (src, dst) in enumerate(((moved, out_moved), (speed, out_speed)))
    ]
    for copy in copies:
        copy.start()
    for copy in copies:
        copy.wait()


def shards(
    displacement,
    velocity,
    node_mass,
    moduli,
    stiffness,
    surface_ref,
    facets,
    penalty,
    owners,
    facet_pairs,
):
    steps = owners.shape[0]
    width = facets.shape[3]
    n_mesh, n_sub = lax.axis_size("mesh"), lax.axis_size("sub")
    assert displacement.shape == (3, 2, ROWS, LANES) and steps == 2 and n_sub % 2 == 0
    assert width == 1 << (width.bit_length() - 1) and width >= 2 * LANES
    out = pltpu.VMEM((6 * ROWS, LANES), F32)
    anywhere = pl.BlockSpec(memory_space=pl.ANY)
    vmem = pl.BlockSpec(memory_space=pltpu.VMEM)
    dma = pltpu.SemaphoreType.DMA
    moved, speed = pl.pallas_call(
        functools.partial(kernel, n_mesh, n_sub, width),
        out_shape=(out, out),
        in_specs=[anywhere] * 10,
        out_specs=(vmem, vmem),
        scratch_shapes=[
            pltpu.VMEM((24, 24), F32),
            pltpu.SMEM((steps, ROWS), jnp.int32),
            pltpu.VMEM((24 * ROWS, LANES), F32),
            pltpu.VMEM((8 * ROWS, LANES), F32),
            pltpu.VMEM((steps * ROWS, LANES), jnp.int32),
            pltpu.VMEM((7 * width // LANES, LANES), F32),
            pltpu.VMEM((n_mesh, 4 * width // LANES, LANES), F32),
            pltpu.VMEM((n_mesh * 4 * width // LANES + 128, LANES), F32),
            pltpu.VMEM((8, LANES), F32),
            pltpu.VMEM((2, 32, LANES), F32),
            pltpu.VMEM((5, 8, LANES), F32),
            pltpu.VMEM((2, 32, LANES), F32),
            pltpu.VMEM((2, 8, LANES), F32),
            pltpu.VMEM((2, 2, 8, LANES), F32),
            dma((9,)),
            pltpu.SemaphoreType.REGULAR,
        ],
        compiler_params=pltpu.CompilerParams(collective_id=0, has_side_effects=True),
    )(
        stiffness,
        owners.reshape(steps, ROWS),
        displacement.reshape(6 * ROWS, LANES),
        velocity.reshape(6 * ROWS, LANES),
        node_mass.reshape(2 * ROWS, LANES),
        moduli.reshape(2 * ROWS, LANES),
        surface_ref.reshape(3 * ROWS, LANES),
        facets.transpose(0, 2, 1, 3).reshape(6 * width // LANES, LANES),
        penalty.reshape(width // LANES, LANES),
        facet_pairs.reshape(steps * ROWS, LANES),
    )
    moved, speed = pl.pallas_call(
        flush,
        out_shape=[jax.ShapeDtypeStruct((6 * ROWS, LANES), F32)] * 2,
        in_specs=[anywhere, anywhere],
        out_specs=[anywhere, anywhere],
        scratch_shapes=[dma((2,))],
        compiler_params=pltpu.CompilerParams(vmem_limit_bytes=1 << 20),
    )(pltpu.with_memory_space_constraint(moved, pltpu.VMEM), pltpu.with_memory_space_constraint(speed, pltpu.VMEM))
    return moved.reshape(displacement.shape), speed.reshape(velocity.shape)


def solution(mesh):
    in_specs = (
        P(None, None, "mesh", "sub"),
        P(None, None, "mesh", "sub"),
        P(None, "mesh", "sub"),
        P(None, "mesh", "sub"),
        P(),
        P(None, "mesh", "sub"),
        P("mesh", "sub", None, None),
        P("mesh", "sub", None),
        P(None, "mesh", "sub", None, None),
        P(None, "mesh", "sub"),
    )
    out_specs = (P(None, None, "mesh", "sub"), P(None, None, "mesh", "sub"))
    return jax.shard_map(shards, mesh=mesh, in_specs=in_specs, out_specs=out_specs, check_vma=False)
```

```python
import functools

import jax
import jax.numpy as jnp
from jax import lax
from jax.experimental import pallas as pl
from jax.experimental.pallas import tpu as pltpu
from jax.sharding import PartitionSpec as P

TIME_STEP = 0.1
MESH = pl.DeviceIdType.MESH
ROWS = 8
LANES = 128
GROUP = 8
GROUPS = LANES // GROUP
F32 = jnp.float32
BF16 = jnp.bfloat16
BLOCKS = 9 * 8
DEPTH = BLOCKS + 8


def roll(x, shift):
    shift %= LANES
    return pltpu.roll(x, shift, 1) if shift else x


def iota(shape, axis):
    return lax.broadcasted_iota(jnp.int32, shape, axis)


def one_hot(condition):
    return jnp.where(condition, 1.0, 0.0).astype(BF16)


def coefficients(stiff):
    high = stiff.astype(BF16)
    low = (stiff - high.astype(F32)).astype(BF16)
    row = iota((32, 24), 0)
    o, b, e = row & 7, row >> 4, (row >> 3) & 1
    wanted = 3 * (4 * (o & 1) + 2 * b + e) + (o >> 1)
    pick = one_hot((wanted == iota((32, 24), 1)) & (o < 6))
    high = jnp.dot(pick, high, preferred_element_type=F32).astype(BF16)
    low = jnp.dot(pick, low, preferred_element_type=F32).astype(BF16)

    def columns(shape):
        col = iota(shape, 1)
        third = jnp.where(col >= DEPTH, 1, 0) + jnp.where(col >= 2 * DEPTH, 1, 0) + jnp.where(col >= 3 * DEPTH, 1, 0)
        rest = col - DEPTH * third
        off, p = rest >> 3, rest & 7
        di = jnp.where(off >= 3, 1, 0) + jnp.where(off >= 6, 1, 0) - 1
        dj = off - 3 * (di + 1) - 1
        return third, di, dj, p, off < 9

    def inside(b2, e2):
        return (b2 >= 0) & (b2 <= 1) & (e2 >= 0) & (e2 <= 1)

    third, di, dj, p, used = columns((24, 256))
    force = None
    for group in range(4):
        b2, e2 = di + (group >> 1), dj + (group & 1)
        wanted = 3 * (4 * (p & 1) + 2 * b2 + e2) + (p >> 1)
        place = used & inside(b2, e2) & (p < 6) & (wanted == iota((24, 256), 0))
        term = jnp.dot(high, one_hot(place & (third < 2)), preferred_element_type=F32)
        term = term + jnp.dot(low, one_hot(place & (third == 2)), preferred_element_type=F32)
        force = term if force is None else jnp.where((iota((32, 256), 0) >> 3) == group, term, force)
    third, di, dj, p, used = columns((24, LANES))
    single = None
    for group in range(4):
        b2, e2 = di + (group >> 1), dj + (group & 1)
        wanted = 3 * (4 * (p & 1) + 2 * b2 + e2) + (p >> 1)
        place = used & inside(b2, e2) & (p < 6) & (wanted == iota((24, LANES), 0)) & (third == 0)
        term = jnp.dot(high, one_hot(place), preferred_element_type=F32)
        term = term + jnp.dot(low, one_hot(place), preferred_element_type=F32)
        single = term if single is None else jnp.where((iota((32, LANES), 0) >> 3) == group, term, single)
    third, di, dj, p, used = columns((32, 256))
    row = iota((32, 256), 0)
    counted = used & inside(di + (row >> 4), dj + ((row >> 3) & 1)) & (p >= 6) & (third < 2)
    return jnp.concatenate([force, jnp.where(counted, 0.125, 0.0)], axis=0).astype(BF16), single


TOUCHED = [
    [2 * b + e for b in (0, 1) for e in (0, 1) if 0 <= di + b <= 1 and 0 <= dj + e <= 1]
    for di in (-1, 0, 1)
    for dj in (-1, 0, 1)
]
SPREAD = [(off, p, g) for off in range(9) for p in range(6) for g in TOUCHED[off]]


def stacked(blocks):
    x = jnp.concatenate(blocks + [jnp.zeros_like(blocks[0])], axis=0)
    high = x.astype(BF16)
    low = (x - high.astype(F32)).astype(BF16)
    return jnp.concatenate([high, low, high, jnp.zeros((256 - 3 * DEPTH, x.shape[1]), BF16)], axis=0)


def kernel(
    n_mesh,
    n_sub,
    width,
    stiff_hbm,
    owners_hbm,
    disp_hbm,
    vel_hbm,
    mass_hbm,
    moduli_hbm,
    surf_hbm,
    facets_hbm,
    penalty_hbm,
    pairs_hbm,
    out_disp,
    out_vel,
    stiff,
    owners,
    inbox,
    inverse,
    pairs,
    raw,
    tables,
    distant,
    edge,
    border,
    edges,
    borders,
    note,
    noted,
    spread,
    turns,
    sems,
    ready,
):
    q, s = lax.axis_index("mesh"), lax.axis_index("sub")
    own, vel = inbox.at[pl.ds(0, 64)], inbox.at[pl.ds(64, 64)]
    mass, base = inbox.at[pl.ds(112, 16)], inbox.at[pl.ds(128, 64)]
    chunks = width // LANES
    half = chunks // 2
    bits = width.bit_length() - 1

    def at(dq, ds):
        return (lax.rem(q + dq + n_mesh, n_mesh), lax.rem(s + ds + n_sub, n_sub))

    size = 4 * chunks
    planar = 2 * 8 + 2 * 32 + (n_mesh - 1) * size
    direct = 3 * 8 + n_mesh * size

    def landed(rows, i):
        ref = distant.at[pl.ds(0, rows)]
        return pltpu.make_async_copy(ref, ref, sems.at[i])

    copies = [
        pltpu.make_async_copy(src, dst, sems.at[i])
        for src, dst, i in [
            (disp_hbm, own.at[pl.ds(0, 48)], 0),
            (moduli_hbm, own.at[pl.ds(48, 16)], 0),
            (owners_hbm, owners, 1),
            (pairs_hbm, pairs, 0),
            (vel_hbm, vel.at[pl.ds(0, 48)], 0),
            (mass_hbm, mass, 0),
        ]
        + [(surf_hbm.at[pl.ds(8 * m, 8)], base.at[pl.ds(16 * m, 8)], 0) for m in range(3)]
        + [
            (facets_hbm, raw.at[pl.ds(0, 6 * chunks)], 2),
            (penalty_hbm, raw.at[pl.ds(6 * chunks, chunks)], 2),
            (stiff_hbm, stiff, 3),
        ]
    ]
    for copy in copies:
        copy.start()
    first, last, odd = s == 0, s == n_sub - 1, lax.rem(s, 2) == 1
    from_last, from_above = first, odd & (s != n_sub - 1)
    to_below = jnp.logical_not(odd | first)
    barrier = pltpu.get_barrier_semaphore()

    def hello(dq, ds):
        pl.semaphore_signal(barrier, inc=1, device_id=at(dq, ds), device_id_type=MESH)

    for dq in range(1, n_mesh):
        hello(dq, 0)

    @pl.when(first)
    def _():
        hello(0, 1)
        for dq in range(n_mesh):
            hello(dq, -1)

    @pl.when(jnp.logical_not(first))
    def _():
        hello(0, -1)

    @pl.when(from_above)
    def _():
        for dq in range(n_mesh):
            hello(dq, 1)

    @pl.when(to_below)
    def _():
        hello(0, 1)

    lane = iota((8, LANES), 1)
    plane = iota((8, LANES), 0)
    group = lane >> 3
    place_in = lane & 7
    entry = plane < 6
    surface = entry & ((plane & 1) == 0)
    flat = jnp.zeros((8, LANES), F32)
    for p in (1, 3, 5):
        base[pl.ds(8 * p, 8), :] = flat
    base[pl.ds(48, 8), :] = flat - 1.0

    landed(152 + 16, 0).wait()
    copies[2].wait()

    holder = jnp.zeros((8, LANES), jnp.int32)
    for b in range(ROWS):
        holder = jnp.where(plane == b, owners[0, b], holder)
    base[pl.ds(56, 8), :] = ((holder << bits) + pairs[pl.ds(0, 8), :]).astype(F32)

    def of_row(ref, i):
        return ref[pl.ds(i, 8, stride=8), :]

    here = {i: of_row(own, i) for i in range(ROWS)}
    speed = {i: of_row(vel, i) for i in range(ROWS)}
    point = {i: of_row(base, i) for i in range(ROWS)}
    point = {i: jnp.where(surface, point[i] + here[i], point[i]) for i in range(ROWS)}

    sent = flat
    for g, i in [(i, i) for i in range(ROWS)] + [(8, 0), (9, 1), (14, 6), (15, 7)]:
        deep = roll(here[i], GROUP * g + 4)
        deep = jnp.where(place_in < 2, roll(point[i], GROUP * g + 1), deep)
        deep = jnp.where(place_in > 5, roll(speed[i], GROUP * g + 7), deep)
        sent = jnp.where(group == g, deep, sent)
    edge[...] = sent
    for k, ids in enumerate(((6, 7, 7, 7), (0, 1, 0, 0))):
        for j, (what, i) in enumerate(zip((here, here, speed, point), ids)):
            border[k, pl.ds(8 * j, 8), :] = what[i]

    landed(7 * chunks, 2).wait()
    parts = [raw[pl.ds(chunks * c, chunks), :] for c in range(7)]
    root = jnp.sqrt(parts[6])
    normal = [root * parts[3 + m] for m in range(3)]
    offset = normal[0] * parts[0] + normal[1] * parts[1] + normal[2] * parts[2]
    for c, values in enumerate(normal + [offset]):
        for h in range(2):
            tables[q, pl.ds(2 * c + h, half, stride=8), :] = values[half * h : half * (h + 1)]

    expected = n_mesh - 1 + jnp.where(first, 1, jnp.where(odd, jnp.where(last, n_mesh + 1, 2), n_mesh + 1))
    pl.semaphore_wait(barrier, expected)

    def send(source, target, device, going, coming):
        return pltpu.make_async_remote_copy(
            src_ref=source,
            dst_ref=target,
            send_sem=sems.at[going],
            recv_sem=sems.at[coming],
            device_id=device,
            device_id_type=MESH,
        )

    def send_direct(ds):
        place = pl.multiple_of(q * size, size)

        def to(t):
            device = (t, lax.rem(s + ds + n_sub, n_sub))
            send(tables.at[q], distant.at[pl.ds(place, size)], device, 1, 8).start()

        def edge_to(dq):
            send(edge, edges.at[2 - dq], at(dq, ds), 1, 7).start()

        for dq in (0, 1, -1):

            @pl.when(at(dq, 0)[0] == 0)
            def _():
                edge_to(dq)

        to(0)
        for dq in (0, 1, -1):

            @pl.when(at(dq, 0)[0] != 0)
            def _():
                edge_to(dq)

        for t in range(1, n_mesh):
            to(t)

    @pl.when(last)
    def _():
        send_direct(1)
        pl.semaphore_signal(ready, inc=1, device_id=at(0, 1), device_id_type=MESH)

    for t in range(n_mesh):
        for k, dq in enumerate((1, -1)):

            @pl.when(lax.rem(q + dq + n_mesh, n_mesh) == t)
            def _():
                send(border.at[k], borders.at[k], (t, s), 0, 4).start()
                send(edge, edges.at[4 * k], (t, s), 0, 4).start()

        @pl.when(q != t)
        def _():
            send(tables.at[q], tables.at[q], (t, s), 0, 5).start()

    @pl.when(to_below)
    def _():
        send_direct(-1)

    for a in range(2):
        slowness = TIME_STEP / mass[pl.ds(8 * a, 8), :]
        for p in range(a, 8, 2):
            inverse[pl.ds(8 * p, 8), :] = slowness
    gain = {i: of_row(inverse, i) for i in range(ROWS)}
    copies[11].wait()
    weights, single = coefficients(stiff[...])
    for n, (off, p, g) in enumerate(SPREAD):
        column_of = single[8 * g : 8 * g + 8, 8 * off + p : 8 * off + p + 1]
        spread[pl.ds(8 * n, 8), :] = jnp.broadcast_to(column_of, (8, LANES))

    def elastic(first, second):
        blocks = [jnp.concatenate([a, b], axis=1) for a, b in zip(first, second)]
        got = jnp.dot(weights, stacked(blocks), preferred_element_type=F32)
        terms = [got[8 * g : 8 * g + 8] * got[32 + 8 * g : 40 + 8 * g] for g in range(4)]
        force = (terms[0] + terms[1]) + (terms[2] + terms[3])
        return force[:, :LANES], force[:, LANES:]

    def side_forces(moved):
        for k, blocks in enumerate(moved):
            for off, x in enumerate(blocks):
                turns[pl.ds(72 * k + 8 * off, 8), :] = x

        def plane_of(k, off, p):
            return jnp.broadcast_to(turns[pl.ds(72 * k + 8 * off + p, 1), :], (8, LANES))

        def plus(table, key, term):
            table[key] = table[key] + term if key in table else term

        sums, scales, n = {}, {}, 0
        for off in range(9):
            for k in range(len(moved)):
                both = plane_of(k, off, 6) + plane_of(k, off, 7)
                for g in TOUCHED[off]:
                    plus(scales, (k, g), both)
            for p in range(6):
                values = [plane_of(k, off, p) for k in range(len(moved))]
                for g in TOUCHED[off]:
                    factor = spread[pl.ds(8 * n, 8), :]
                    n += 1
                    for k, value in enumerate(values):
                        plus(sums, (k, g), factor * value)
        terms = {key: sums[key] * (0.125 * scales[key]) for key in sums}
        return [(terms[k, 0] + terms[k, 1]) + (terms[k, 2] + terms[k, 3]) for k in range(len(moved))]

    def around(rows, i):
        return [x for di in (-1, 0, 1) for x in rows[i + di]]

    def turned(x):
        return (roll(x, 1), x, roll(x, -1))

    def narrowed(total, second):
        return jnp.where(second, pltpu.roll(total, 7, 0), total)

    def facet_of(step, i):
        index = jnp.broadcast_to(pairs[pl.ds(step * ROWS + i, 1), :], (8, LANES))
        chunk, place = index >> 7, index & (LANES - 1)
        second = chunk >= half
        chunk = jnp.where(second, chunk - half, chunk)
        owner = owners[step, i]
        total = flat
        for k in range(half):
            picked = jnp.take_along_axis(tables[owner, pl.ds(8 * k, 8), :], place, axis=1, mode="promise_in_bounds")
            total = jnp.where(chunk == k, picked, total)
        return narrowed(total, second)

    def wanted_by(at_point):
        code = jnp.broadcast_to(at_point[7:8], (8, LANES)).astype(jnp.int32)
        owner, index = code >> bits, code & (width - 1)
        chunk, place = index >> 7, index & (LANES - 1)
        second = chunk >= half
        return jnp.where(second, chunk - half, chunk) + half * owner, place, second

    def facet_by(wanted, ref):
        chunk, place, second = wanted
        total = flat
        for k in range(half * n_mesh):
            rows = ref(k)
            picked = jnp.take_along_axis(rows, place, axis=1, mode="promise_in_bounds")
            total = jnp.where(chunk == k, picked, total)
        return narrowed(total, second)

    def of_plane(k):
        return tables[k // half, pl.ds(8 * (k % half), 8), :]

    def of_side(k):
        return distant[pl.ds(8 * k, 8), :]

    def push_of(facet, at_point):
        product = jnp.where(surface | (plane == 6), facet * at_point, 0.0)
        product = product + pltpu.roll(product, 4, 0)
        product = product + pltpu.roll(product, 2, 0)
        return jnp.where(surface, facet * jnp.maximum(-product, 0.0), 0.0)

    def ring_step(values, moving, net):
        weight = jnp.where(
            (plane & 1) == 0, jnp.broadcast_to(moving[6:7], (8, LANES)), jnp.broadcast_to(moving[7:8], (8, LANES))
        )
        slow = TIME_STEP / weight
        faster = moving + slow * net
        return jnp.where(entry, values + TIME_STEP * faster, values), faster

    rows = {i: turned(here[i]) for i in range(ROWS)}
    force = {}
    for i in (1, 3, 5):
        force[i], force[i + 1] = elastic(around(rows, i), around(rows, i + 1))
    landed(2 * 8 + 2 * 32, 4).wait()
    for i, (k, j) in {-2: (0, 0), -1: (0, 1), 8: (1, 0), 9: (1, 1)}.items():
        here[i] = borders[k, pl.ds(8 * j, 8), :]
        rows[i] = turned(here[i])
    force[0], force[7] = elastic(around(rows, 0), around(rows, 7))
    force[-1], force[8] = elastic(around(rows, -1), around(rows, 8))

    def column(middle, before, behind):
        return jnp.where(group < 8, middle, jnp.where(group < 12, behind, before))

    centre = column(sent, edges[0], edges[4])
    landed((n_mesh - 1) * size, 5).wait()
    own_point = roll(centre, 3)
    own_push = push_of(facet_by(wanted_by(own_point), of_plane), own_point)

    note[0] = centre
    note[1] = own_push

    @pl.when(jnp.logical_not(last))
    def _():
        send(note, noted.at[0], at(0, 1), 2, 6).start()

    @pl.when(odd)
    def _():
        send(note, noted.at[1], at(0, -1), 3, 6).start()

    @pl.when(first)
    def _():
        pl.semaphore_wait(ready, 1)
        send(note, noted.at[1], at(0, -1), 3, 6).start()

    later = {}
    after, fast = {}, {}
    for i in range(ROWS):
        net = push_of(facet_of(0, i), point[i]) - force[i]
        later[i] = facet_of(1, i)
        fast[i] = speed[i] + gain[i] * net
        after[i] = jnp.where(entry, here[i] + TIME_STEP * fast[i], here[i])
    for i, k in ((-1, 0), (8, 1)):
        moving, at_point = borders[k, pl.ds(16, 8), :], borders[k, pl.ds(24, 8), :]
        facet = facet_by(wanted_by(at_point), of_plane)
        after[i], _ = ring_step(here[i], moving, push_of(facet, at_point) - force[i])

    rows = {i: turned(after[i]) for i in range(-1, 9)}
    for i in range(0, ROWS, 2):
        force[i], force[i + 1] = elastic(around(rows, i), around(rows, i + 1))
    for i in range(ROWS):
        at_point = of_row(base, i)
        at_point = jnp.where(surface, at_point + after[i], at_point)
        past = fast[i] + gain[i] * (push_of(later[i], at_point) - force[i])
        out_vel[pl.ds(i, 6, stride=8), :] = past[0:6]
        out_disp[pl.ds(i, 6, stride=8), :] = (after[i] + TIME_STEP * past)[0:6]

    def strip_of(rows_of, indices):
        made = flat
        for i in indices:
            g = i % GROUPS
            piece = jnp.where(place_in < 4, roll(rows_of[i], GROUP * g + 3), roll(rows_of[i], GROUP * g + 5))
            made = jnp.where(group == g, piece, made)
        return made

    known = strip_of(after, range(-1, 9))
    known_fast, known_gain, known_facet = (strip_of(x, range(ROWS)) for x in (fast, gain, later))
    known_point = strip_of({i: of_row(base, i) for i in range(ROWS)}, range(ROWS))
    shifts = (1, -1)
    own_pushes = [roll(own_push, shift) for shift in shifts]

    has_direct = from_last | from_above

    @pl.when(jnp.logical_not(has_direct))
    def _():
        landed(2 * 2 * 8, 6).wait()

    @pl.when(has_direct)
    def _():
        landed(2 * 8, 6).wait()
        landed(3 * 8, 7).wait()

    far = column(edges[2], edges[1], edges[3])
    left, right = jnp.where(from_last, far, noted[0, 0]), jnp.where(from_above, far, noted[1, 0])
    from_before = (place_in == 0) | (place_in == 2) | (place_in == 3) | (place_in == 6)
    strips = [jnp.where(from_before, left, centre), jnp.where(from_before, centre, right)]
    moved = [
        [roll(x, shift - (GROUP * di + dj)) for di in (-1, 0, 1) for dj in (-1, 0, 1)]
        for x, shift in zip(strips, shifts)
    ]
    strip_force = side_forces(moved)
    strip_speed = [roll(x, shift - 3) for x, shift in zip(strips, shifts)]
    far_point = jnp.where(from_last, roll(far, 3 + shifts[0]), roll(far, 3 + shifts[1]))
    far_wanted = wanted_by(far_point)
    noted_push = [roll(noted[k, 1], shifts[k]) for k in range(2)]

    @pl.when(has_direct)
    def _():
        landed(n_mesh * size, 8).wait()

    far_push = push_of(facet_by(far_wanted, of_side), far_point)
    strip_after = []
    for k, by_far in enumerate((from_last, from_above)):
        push = jnp.where(by_far, far_push, noted_push[k])
        push = jnp.where(place_in == (4, 3)[k], push, own_pushes[k])
        strip_after.append(ring_step(moved[k][4], strip_speed[k], push - strip_force[k]))

    low, high = (place_in == 4) | (place_in == 5), (place_in == 2) | (place_in == 3)
    edge_now = jnp.where(low, strip_after[0][0], jnp.where(high, strip_after[1][0], known))
    edge_fast = jnp.where(place_in == 5, strip_after[0][1], jnp.where(place_in == 2, strip_after[1][1], known_fast))
    (edge_force,) = side_forces([[roll(edge_now, -(GROUP * di + dj)) for di in (-1, 0, 1) for dj in (-1, 0, 1)]])
    at_point = jnp.where(surface, known_point + edge_now, known_point)
    past = edge_fast + known_gain * (push_of(known_facet, at_point) - edge_force)
    moved_to = edge_now + TIME_STEP * past
    side = (lane < 2) | (lane >= LANES - 2)
    for i in range(ROWS):
        for ref, x in ((out_vel, past), (out_disp, moved_to)):
            fixed = jnp.where(lane < 2, roll(x, -(GROUP * i + 5)), roll(x, LANES - 3 - GROUP * i))
            at_row = pl.ds(i, 6, stride=8)
            ref[at_row, :] = jnp.where(side[0:6], fixed[0:6], ref[at_row, :])

    landed(planar, 0).wait()

    @pl.when(to_below | last)
    def _():
        landed(direct, 1).wait()

    @pl.when(jnp.logical_not(last))
    def _():
        landed(2 * 8, 2).wait()

    @pl.when(odd | first)
    def _():
        landed(2 * 8, 3).wait()


def flush(moved, speed, out_moved, out_speed, sem):
    copies = [
        pltpu.make_async_copy(src, dst, sem.at[i])
        for i, (src, dst) in enumerate(((moved, out_moved), (speed, out_speed)))
    ]
    for copy in copies:
        copy.start()
    for copy in copies:
        copy.wait()


def shards(
    displacement,
    velocity,
    node_mass,
    moduli,
    stiffness,
    surface_ref,
    facets,
    penalty,
    owners,
    facet_pairs,
):
    steps = owners.shape[0]
    width = facets.shape[3]
    n_mesh, n_sub = lax.axis_size("mesh"), lax.axis_size("sub")
    assert displacement.shape == (3, 2, ROWS, LANES) and steps == 2 and n_sub % 2 == 0
    assert width == 1 << (width.bit_length() - 1) and width >= 2 * LANES
    out = pltpu.VMEM((6 * ROWS, LANES), F32)
    anywhere = pl.BlockSpec(memory_space=pl.ANY)
    vmem = pl.BlockSpec(memory_space=pltpu.VMEM)
    dma = pltpu.SemaphoreType.DMA
    moved, speed = pl.pallas_call(
        functools.partial(kernel, n_mesh, n_sub, width),
        out_shape=(out, out),
        in_specs=[anywhere] * 10,
        out_specs=(vmem, vmem),
        scratch_shapes=[
            pltpu.VMEM((24, 24), F32),
            pltpu.SMEM((steps, ROWS), jnp.int32),
            pltpu.VMEM((24 * ROWS, LANES), F32),
            pltpu.VMEM((8 * ROWS, LANES), F32),
            pltpu.VMEM((steps * ROWS, LANES), jnp.int32),
            pltpu.VMEM((7 * width // LANES, LANES), F32),
            pltpu.VMEM((n_mesh, 4 * width // LANES, LANES), F32),
            pltpu.VMEM((n_mesh * 4 * width // LANES + 128, LANES), F32),
            pltpu.VMEM((8, LANES), F32),
            pltpu.VMEM((2, 32, LANES), F32),
            pltpu.VMEM((5, 8, LANES), F32),
            pltpu.VMEM((2, 32, LANES), F32),
            pltpu.VMEM((2, 8, LANES), F32),
            pltpu.VMEM((2, 2, 8, LANES), F32),
            pltpu.VMEM((8 * len(SPREAD), LANES), F32),
            pltpu.VMEM((2 * 9 * 8, LANES), F32),
            dma((9,)),
            pltpu.SemaphoreType.REGULAR,
        ],
        compiler_params=pltpu.CompilerParams(collective_id=0, has_side_effects=True),
    )(
        stiffness,
        owners.reshape(steps, ROWS),
        displacement.reshape(6 * ROWS, LANES),
        velocity.reshape(6 * ROWS, LANES),
        node_mass.reshape(2 * ROWS, LANES),
        moduli.reshape(2 * ROWS, LANES),
        surface_ref.reshape(3 * ROWS, LANES),
        facets.transpose(0, 2, 1, 3).reshape(6 * width // LANES, LANES),
        penalty.reshape(width // LANES, LANES),
        facet_pairs.reshape(steps * ROWS, LANES),
    )
    moved, speed = pl.pallas_call(
        flush,
        out_shape=[jax.ShapeDtypeStruct((6 * ROWS, LANES), F32)] * 2,
        in_specs=[anywhere, anywhere],
        out_specs=[anywhere, anywhere],
        scratch_shapes=[dma((2,))],
        compiler_params=pltpu.CompilerParams(vmem_limit_bytes=1 << 20),
    )(pltpu.with_memory_space_constraint(moved, pltpu.VMEM), pltpu.with_memory_space_constraint(speed, pltpu.VMEM))
    return moved.reshape(displacement.shape), speed.reshape(velocity.shape)


def solution(mesh):
    in_specs = (
        P(None, None, "mesh", "sub"),
        P(None, None, "mesh", "sub"),
        P(None, "mesh", "sub"),
        P(None, "mesh", "sub"),
        P(),
        P(None, "mesh", "sub"),
        P("mesh", "sub", None, None),
        P("mesh", "sub", None),
        P(None, "mesh", "sub", None, None),
        P(None, "mesh", "sub"),
    )
    out_specs = (P(None, None, "mesh", "sub"), P(None, None, "mesh", "sub"))
    return jax.shard_map(shards, mesh=mesh, in_specs=in_specs, out_specs=out_specs, check_vma=False)
```

```python
import functools

import jax
import jax.numpy as jnp
from jax import lax
from jax.experimental import pallas as pl
from jax.experimental.pallas import tpu as pltpu
from jax.sharding import PartitionSpec as P

TIME_STEP = 0.1
MESH = pl.DeviceIdType.MESH
ROWS = 8
LANES = 128
GROUP = 8
GROUPS = LANES // GROUP
F32 = jnp.float32
BF16 = jnp.bfloat16
BLOCKS = 9 * 8
DEPTH = BLOCKS + 8


def roll(x, shift):
    shift %= LANES
    return pltpu.roll(x, shift, 1) if shift else x


def iota(shape, axis):
    return lax.broadcasted_iota(jnp.int32, shape, axis)


def one_hot(condition):
    return jnp.where(condition, 1.0, 0.0).astype(BF16)


def coefficients(stiff):
    high = stiff.astype(BF16)
    low = (stiff - high.astype(F32)).astype(BF16)
    row = iota((32, 24), 0)
    o, b, e = row & 7, row >> 4, (row >> 3) & 1
    wanted = 3 * (4 * (o & 1) + 2 * b + e) + (o >> 1)
    pick = one_hot((wanted == iota((32, 24), 1)) & (o < 6))
    high = jnp.dot(pick, high, preferred_element_type=F32).astype(BF16)
    low = jnp.dot(pick, low, preferred_element_type=F32).astype(BF16)

    def columns(shape):
        col = iota(shape, 1)
        third = jnp.where(col >= DEPTH, 1, 0) + jnp.where(col >= 2 * DEPTH, 1, 0) + jnp.where(col >= 3 * DEPTH, 1, 0)
        rest = col - DEPTH * third
        off, p = rest >> 3, rest & 7
        di = jnp.where(off >= 3, 1, 0) + jnp.where(off >= 6, 1, 0) - 1
        dj = off - 3 * (di + 1) - 1
        return third, di, dj, p, off < 9

    def inside(b2, e2):
        return (b2 >= 0) & (b2 <= 1) & (e2 >= 0) & (e2 <= 1)

    third, di, dj, p, used = columns((24, 256))
    force = None
    for group in range(4):
        b2, e2 = di + (group >> 1), dj + (group & 1)
        wanted = 3 * (4 * (p & 1) + 2 * b2 + e2) + (p >> 1)
        place = used & inside(b2, e2) & (p < 6) & (wanted == iota((24, 256), 0))
        term = jnp.dot(high, one_hot(place & (third < 2)), preferred_element_type=F32)
        term = term + jnp.dot(low, one_hot(place & (third == 2)), preferred_element_type=F32)
        force = term if force is None else jnp.where((iota((32, 256), 0) >> 3) == group, term, force)
    third, di, dj, p, used = columns((24, LANES))
    single = None
    for group in range(4):
        b2, e2 = di + (group >> 1), dj + (group & 1)
        wanted = 3 * (4 * (p & 1) + 2 * b2 + e2) + (p >> 1)
        place = used & inside(b2, e2) & (p < 6) & (wanted == iota((24, LANES), 0)) & (third == 0)
        term = jnp.dot(high, one_hot(place), preferred_element_type=F32)
        term = term + jnp.dot(low, one_hot(place), preferred_element_type=F32)
        single = term if single is None else jnp.where((iota((32, LANES), 0) >> 3) == group, term, single)
    third, di, dj, p, used = columns((32, 256))
    row = iota((32, 256), 0)
    counted = used & inside(di + (row >> 4), dj + ((row >> 3) & 1)) & (p >= 6) & (third < 2)
    return jnp.concatenate([force, jnp.where(counted, 0.125, 0.0)], axis=0).astype(BF16), single


TOUCHED = [
    [2 * b + e for b in (0, 1) for e in (0, 1) if 0 <= di + b <= 1 and 0 <= dj + e <= 1]
    for di in (-1, 0, 1)
    for dj in (-1, 0, 1)
]
SPREAD = [(off, p, g) for off in range(9) for p in range(6) for g in TOUCHED[off]]


def stacked(blocks):
    x = jnp.concatenate(blocks + [jnp.zeros_like(blocks[0])], axis=0)
    high = x.astype(BF16)
    low = (x - high.astype(F32)).astype(BF16)
    return jnp.concatenate([high, low, high, jnp.zeros((256 - 3 * DEPTH, x.shape[1]), BF16)], axis=0)


def kernel(
    n_mesh,
    n_sub,
    width,
    stiff_hbm,
    owners_hbm,
    disp_hbm,
    vel_hbm,
    mass_hbm,
    moduli_hbm,
    surf_hbm,
    facets_hbm,
    penalty_hbm,
    pairs_hbm,
    out_disp,
    out_vel,
    stiff,
    owners,
    inbox,
    inverse,
    pairs,
    raw,
    tables,
    distant,
    edge,
    border,
    edges,
    borders,
    note,
    noted,
    spread,
    turns,
    sems,
    ready,
):
    q, s = lax.axis_index("mesh"), lax.axis_index("sub")
    own, vel = inbox.at[pl.ds(0, 64)], inbox.at[pl.ds(64, 64)]
    mass, base = inbox.at[pl.ds(112, 16)], inbox.at[pl.ds(128, 64)]
    chunks = width // LANES
    half = chunks // 2
    bits = width.bit_length() - 1

    def at(dq, ds):
        return (lax.rem(q + dq + n_mesh, n_mesh), lax.rem(s + ds + n_sub, n_sub))

    size = 4 * chunks
    planar = 2 * 8 + 2 * 32 + (n_mesh - 1) * size
    direct = 3 * 8 + n_mesh * size

    def landed(rows, i):
        ref = distant.at[pl.ds(0, rows)]
        return pltpu.make_async_copy(ref, ref, sems.at[i])

    copies = [
        pltpu.make_async_copy(src, dst, sems.at[i])
        for src, dst, i in [
            (facets_hbm, raw.at[pl.ds(0, 6 * chunks)], 2),
            (penalty_hbm, raw.at[pl.ds(6 * chunks, chunks)], 2),
            (disp_hbm, own.at[pl.ds(0, 48)], 0),
            (moduli_hbm, own.at[pl.ds(48, 16)], 0),
            (owners_hbm, owners, 1),
            (pairs_hbm, pairs, 0),
            (vel_hbm, vel.at[pl.ds(0, 48)], 0),
            (mass_hbm, mass, 0),
        ]
        + [(surf_hbm.at[pl.ds(8 * m, 8)], base.at[pl.ds(16 * m, 8)], 0) for m in range(3)]
    ]
    for copy in copies:
        copy.start()
    first, last, odd = s == 0, s == n_sub - 1, lax.rem(s, 2) == 1
    from_last, from_above = first, odd & (s != n_sub - 1)
    to_below = jnp.logical_not(odd | first)
    barrier = pltpu.get_barrier_semaphore()

    def hello(dq, ds):
        pl.semaphore_signal(barrier, inc=1, device_id=at(dq, ds), device_id_type=MESH)

    for dq in range(1, n_mesh):
        hello(dq, 0)

    @pl.when(first)
    def _():
        hello(0, 1)
        for dq in range(n_mesh):
            hello(dq, -1)

    @pl.when(jnp.logical_not(first))
    def _():
        hello(0, -1)

    @pl.when(from_above)
    def _():
        for dq in range(n_mesh):
            hello(dq, 1)

    @pl.when(to_below)
    def _():
        hello(0, 1)

    lane = iota((8, LANES), 1)
    plane = iota((8, LANES), 0)
    group = lane >> 3
    place_in = lane & 7
    entry = plane < 6
    surface = entry & ((plane & 1) == 0)
    flat = jnp.zeros((8, LANES), F32)
    for p in (1, 3, 5):
        base[pl.ds(8 * p, 8), :] = flat
    base[pl.ds(48, 8), :] = flat - 1.0

    landed(7 * chunks, 2).wait()
    parts = [raw[pl.ds(chunks * c, chunks), :] for c in range(7)]
    root = jnp.sqrt(parts[6])
    normal = [root * parts[3 + m] for m in range(3)]
    offset = normal[0] * parts[0] + normal[1] * parts[1] + normal[2] * parts[2]
    for c, values in enumerate(normal + [offset]):
        for h in range(2):
            tables[q, pl.ds(2 * c + h, half, stride=8), :] = values[half * h : half * (h + 1)]

    expected = n_mesh - 1 + jnp.where(first, 1, jnp.where(odd, jnp.where(last, n_mesh + 1, 2), n_mesh + 1))
    def send(source, target, device, going, coming):
        return pltpu.make_async_remote_copy(
            src_ref=source,
            dst_ref=target,
            send_sem=sems.at[going],
            recv_sem=sems.at[coming],
            device_id=device,
            device_id_type=MESH,
        )

    def send_table(ds, t):
        place = pl.ds(pl.multiple_of(q * size, size), size)
        send(tables.at[q], distant.at[place], (t, lax.rem(s + ds + n_sub, n_sub)), 2, 4).start()

    @pl.when(last)
    def _():
        pl.semaphore_wait(barrier, expected)
        send_table(1, 0)

    landed(152 + 16, 0).wait()
    copies[4].wait()
    stiff_copy = pltpu.make_async_copy(stiff_hbm, stiff, sems.at[1])
    stiff_copy.start()

    holder = jnp.zeros((8, LANES), jnp.int32)
    for b in range(ROWS):
        holder = jnp.where(plane == b, owners[0, b], holder)
    base[pl.ds(56, 8), :] = ((holder << bits) + pairs[pl.ds(0, 8), :]).astype(F32)

    def of_row(ref, i):
        return ref[pl.ds(i, 8, stride=8), :]

    here = {i: of_row(own, i) for i in range(ROWS)}
    speed = {i: of_row(vel, i) for i in range(ROWS)}
    point = {i: of_row(base, i) for i in range(ROWS)}
    point = {i: jnp.where(surface, point[i] + here[i], point[i]) for i in range(ROWS)}

    sent = flat
    for g, i in [(i, i) for i in range(ROWS)] + [(8, 0), (9, 1), (14, 6), (15, 7)]:
        deep = roll(here[i], GROUP * g + 4)
        deep = jnp.where(place_in == 0, roll(point[i], GROUP * g + 1), deep)
        deep = jnp.where(place_in == 7, roll(point[i], GROUP * g + 7), deep)
        deep = jnp.where(place_in == 1, roll(speed[i], GROUP * g + 2), deep)
        deep = jnp.where(place_in == 6, roll(speed[i], GROUP * g + 6), deep)
        sent = jnp.where(group == g, deep, sent)
    edge[...] = sent
    for k, ids in enumerate(((6, 7, 7, 7), (0, 1, 0, 0))):
        for j, (what, i) in enumerate(zip((here, here, speed, point), ids)):
            border[k, pl.ds(8 * j, 8), :] = what[i]

    @pl.when(jnp.logical_not(last))
    def _():
        pl.semaphore_wait(barrier, expected)

    def send_direct(ds):
        def edge_to(dq):
            send(edge, edges.at[2 - dq], at(dq, ds), 2, 4).start()

        for dq in (0, 1, -1):

            @pl.when(at(dq, 0)[0] == 0)
            def _():
                edge_to(dq)

        if ds == -1:
            send_table(ds, 0)
        for dq in (0, 1, -1):

            @pl.when(at(dq, 0)[0] != 0)
            def _():
                edge_to(dq)

        for t in range(1, n_mesh):
            send_table(ds, t)

    @pl.when(last)
    def _():
        send_direct(1)
        pl.semaphore_signal(ready, inc=1, device_id=at(0, 1), device_id_type=MESH)

    for t in range(n_mesh):
        for k, dq in enumerate((1, -1)):

            @pl.when(lax.rem(q + dq + n_mesh, n_mesh) == t)
            def _():
                send(border.at[k], borders.at[k], (t, s), 0, 3).start()
                send(edge, edges.at[4 * k], (t, s), 0, 3).start()

        @pl.when(q != t)
        def _():
            send(tables.at[q], tables.at[q], (t, s), 0, 3).start()

    @pl.when(to_below)
    def _():
        send_direct(-1)

    for a in range(2):
        slowness = TIME_STEP / mass[pl.ds(8 * a, 8), :]
        for p in range(a, 8, 2):
            inverse[pl.ds(8 * p, 8), :] = slowness
    gain = {i: of_row(inverse, i) for i in range(ROWS)}
    stiff_copy.wait()
    weights, single = coefficients(stiff[...])
    for n, (off, p, g) in enumerate(SPREAD):
        column_of = single[8 * g : 8 * g + 8, 8 * off + p : 8 * off + p + 1]
        spread[pl.ds(8 * n, 8), :] = jnp.broadcast_to(column_of, (8, LANES))

    def elastic(first, second):
        blocks = [jnp.concatenate([a, b], axis=1) for a, b in zip(first, second)]
        got = jnp.dot(weights, stacked(blocks), preferred_element_type=F32)
        terms = [got[8 * g : 8 * g + 8] * got[32 + 8 * g : 40 + 8 * g] for g in range(4)]
        force = (terms[0] + terms[1]) + (terms[2] + terms[3])
        return force[:, :LANES], force[:, LANES:]

    def side_forces(moved):
        for k, blocks in enumerate(moved):
            for off, x in enumerate(blocks):
                turns[pl.ds(72 * k + 8 * off, 8), :] = x

        def plane_of(k, off, p):
            return jnp.broadcast_to(turns[pl.ds(72 * k + 8 * off + p, 1), :], (8, LANES))

        def plus(table, key, term):
            table[key] = table[key] + term if key in table else term

        sums, scales, n = {}, {}, 0
        for off in range(9):
            for k in range(len(moved)):
                both = plane_of(k, off, 6) + plane_of(k, off, 7)
                for g in TOUCHED[off]:
                    plus(scales, (k, g), both)
            for p in range(6):
                values = [plane_of(k, off, p) for k in range(len(moved))]
                for g in TOUCHED[off]:
                    factor = spread[pl.ds(8 * n, 8), :]
                    n += 1
                    for k, value in enumerate(values):
                        plus(sums, (k, g), factor * value)
        terms = {key: sums[key] * (0.125 * scales[key]) for key in sums}
        return [(terms[k, 0] + terms[k, 1]) + (terms[k, 2] + terms[k, 3]) for k in range(len(moved))]

    def around(rows, i):
        return [x for di in (-1, 0, 1) for x in rows[i + di]]

    def turned(x):
        return (roll(x, 1), x, roll(x, -1))

    def narrowed(total, second):
        return jnp.where(second, pltpu.roll(total, 7, 0), total)

    def facet_of(step, i):
        index = jnp.broadcast_to(pairs[pl.ds(step * ROWS + i, 1), :], (8, LANES))
        chunk, place = index >> 7, index & (LANES - 1)
        second = chunk >= half
        chunk = jnp.where(second, chunk - half, chunk)
        owner = owners[step, i]
        total = flat
        for k in range(half):
            picked = jnp.take_along_axis(tables[owner, pl.ds(8 * k, 8), :], place, axis=1, mode="promise_in_bounds")
            total = jnp.where(chunk == k, picked, total)
        return narrowed(total, second)

    def wanted_by(at_point):
        code = jnp.broadcast_to(at_point[7:8], (8, LANES)).astype(jnp.int32)
        owner, index = code >> bits, code & (width - 1)
        chunk, place = index >> 7, index & (LANES - 1)
        second = chunk >= half
        return jnp.where(second, chunk - half, chunk) + half * owner, place, second

    def facet_by(wanted, ref):
        chunk, place, second = wanted
        total = flat
        for k in range(half * n_mesh):
            rows = ref(k)
            picked = jnp.take_along_axis(rows, place, axis=1, mode="promise_in_bounds")
            total = jnp.where(chunk == k, picked, total)
        return narrowed(total, second)

    def of_plane(k):
        return tables[k // half, pl.ds(8 * (k % half), 8), :]

    def of_side(k):
        return distant[pl.ds(8 * k, 8), :]

    def push_of(facet, at_point):
        product = jnp.where(surface | (plane == 6), facet * at_point, 0.0)
        product = product + pltpu.roll(product, 4, 0)
        product = product + pltpu.roll(product, 2, 0)
        return jnp.where(surface, facet * jnp.maximum(-product, 0.0), 0.0)

    def ring_step(values, moving, net):
        weight = jnp.where(
            (plane & 1) == 0, jnp.broadcast_to(moving[6:7], (8, LANES)), jnp.broadcast_to(moving[7:8], (8, LANES))
        )
        slow = TIME_STEP / weight
        faster = moving + slow * net
        return jnp.where(entry, values + TIME_STEP * faster, values), faster

    rows = {i: turned(here[i]) for i in range(ROWS)}
    force = {}
    for i in (1, 3, 5):
        force[i], force[i + 1] = elastic(around(rows, i), around(rows, i + 1))
    landed(planar, 3).wait()
    for i, (k, j) in {-2: (0, 0), -1: (0, 1), 8: (1, 0), 9: (1, 1)}.items():
        here[i] = borders[k, pl.ds(8 * j, 8), :]
        rows[i] = turned(here[i])
    force[0], force[7] = elastic(around(rows, 0), around(rows, 7))
    force[-1], force[8] = elastic(around(rows, -1), around(rows, 8))

    def column(middle, before, behind):
        return jnp.where(group < 8, middle, jnp.where(group < 12, behind, before))

    centre = column(sent, edges[0], edges[4])
    own_push = push_of(facet_by(wanted_by(centre), of_plane), centre)

    note[0] = centre
    note[1] = own_push

    @pl.when(jnp.logical_not(last))
    def _():
        send(note, noted.at[0], at(0, 1), 1, 4).start()

    @pl.when(odd)
    def _():
        send(note, noted.at[1], at(0, -1), 1, 4).start()

    @pl.when(first)
    def _():
        pl.semaphore_wait(ready, 1)
        send(note, noted.at[1], at(0, -1), 1, 4).start()

    later = {}
    after, fast = {}, {}
    for i in range(ROWS):
        net = push_of(facet_of(0, i), point[i]) - force[i]
        later[i] = facet_of(1, i)
        fast[i] = speed[i] + gain[i] * net
        after[i] = jnp.where(entry, here[i] + TIME_STEP * fast[i], here[i])
    for i, k in ((-1, 0), (8, 1)):
        moving, at_point = borders[k, pl.ds(16, 8), :], borders[k, pl.ds(24, 8), :]
        facet = facet_by(wanted_by(at_point), of_plane)
        after[i], _ = ring_step(here[i], moving, push_of(facet, at_point) - force[i])

    rows = {i: turned(after[i]) for i in range(-1, 9)}
    for i in range(0, ROWS, 2):
        force[i], force[i + 1] = elastic(around(rows, i), around(rows, i + 1))
    for i in range(ROWS):
        at_point = of_row(base, i)
        at_point = jnp.where(surface, at_point + after[i], at_point)
        past = fast[i] + gain[i] * (push_of(later[i], at_point) - force[i])
        out_vel[pl.ds(i, 6, stride=8), :] = past[0:6]
        out_disp[pl.ds(i, 6, stride=8), :] = (after[i] + TIME_STEP * past)[0:6]

    def strip_of(rows_of, indices):
        made = flat
        for i in indices:
            g = i % GROUPS
            piece = jnp.where(place_in < 4, roll(rows_of[i], GROUP * g + 1), roll(rows_of[i], GROUP * g + 7))
            made = jnp.where(group == g, piece, made)
        return made

    known = strip_of(after, range(-1, 9))
    known_fast, known_gain, known_facet = (strip_of(x, range(ROWS)) for x in (fast, gain, later))
    known_point = strip_of({i: of_row(base, i) for i in range(ROWS)}, range(ROWS))
    shifts = (-3, 3)
    own_pushes = [roll(own_push, -6), roll(own_push, 6)]

    has_direct = from_last | from_above

    @pl.when(jnp.logical_not(has_direct))
    def _():
        landed(2 * 2 * 8, 4).wait()

    @pl.when(has_direct)
    def _():
        landed(2 * 8 + direct, 4).wait()

    far = column(edges[2], edges[1], edges[3])
    left, right = jnp.where(from_last, far, noted[0, 0]), jnp.where(from_above, far, noted[1, 0])
    from_before = place_in < 4
    strips = [jnp.where(from_before, left, centre), jnp.where(from_before, centre, right)]
    moved = [
        [roll(x, shift - (GROUP * di + dj)) for di in (-1, 0, 1) for dj in (-1, 0, 1)]
        for x, shift in zip(strips, shifts)
    ]
    strip_force = side_forces(moved)
    strip_speed = [
        jnp.where(place_in == 0, roll(strips[0], -1), roll(strips[0], -5)),
        jnp.where(place_in == 7, roll(strips[1], 1), roll(strips[1], 5)),
    ]
    far_wanted = wanted_by(far)

    far_push = push_of(facet_by(far_wanted, of_side), far)
    strip_after = []
    for k, by_far in enumerate((from_last, from_above)):
        push = jnp.where(by_far, far_push, noted[k, 1])
        push = jnp.where(place_in == (0, 7)[k], push, own_pushes[k])
        strip_after.append(ring_step(moved[k][4], strip_speed[k], push - strip_force[k]))

    low, high = place_in < 2, place_in > 5
    edge_now = jnp.where(low, strip_after[0][0], jnp.where(high, strip_after[1][0], known))
    edge_fast = jnp.where(place_in == 1, strip_after[0][1], jnp.where(place_in == 6, strip_after[1][1], known_fast))
    (edge_force,) = side_forces([[roll(edge_now, -(GROUP * di + dj)) for di in (-1, 0, 1) for dj in (-1, 0, 1)]])
    at_point = jnp.where(surface, known_point + edge_now, known_point)
    past = edge_fast + known_gain * (push_of(known_facet, at_point) - edge_force)
    moved_to = edge_now + TIME_STEP * past
    side = (lane < 2) | (lane >= LANES - 2)
    for i in range(ROWS):
        for ref, x in ((out_vel, past), (out_disp, moved_to)):
            fixed = jnp.where(lane < 2, roll(x, -(GROUP * i + 1)), roll(x, LANES - 7 - GROUP * i))
            at_row = pl.ds(i, 6, stride=8)
            ref[at_row, :] = jnp.where(side[0:6], fixed[0:6], ref[at_row, :])

    landed(planar, 0).wait()

    @pl.when(to_below | last)
    def _():
        landed(direct, 2).wait()

    two_notes = first | (odd & jnp.logical_not(last))

    @pl.when(two_notes)
    def _():
        landed(2 * 2 * 8, 1).wait()

    @pl.when(jnp.logical_not(two_notes))
    def _():
        landed(2 * 8, 1).wait()


def flush(moved, speed, out_moved, out_speed, sem):
    copies = [
        pltpu.make_async_copy(src, dst, sem.at[i])
        for i, (src, dst) in enumerate(((moved, out_moved), (speed, out_speed)))
    ]
    for copy in copies:
        copy.start()
    for copy in copies:
        copy.wait()


def shards(
    displacement,
    velocity,
    node_mass,
    moduli,
    stiffness,
    surface_ref,
    facets,
    penalty,
    owners,
    facet_pairs,
):
    steps = owners.shape[0]
    width = facets.shape[3]
    n_mesh, n_sub = lax.axis_size("mesh"), lax.axis_size("sub")
    assert displacement.shape == (3, 2, ROWS, LANES) and steps == 2 and n_sub % 2 == 0
    assert width == 1 << (width.bit_length() - 1) and width >= 2 * LANES
    out = pltpu.VMEM((6 * ROWS, LANES), F32)
    anywhere = pl.BlockSpec(memory_space=pl.ANY)
    vmem = pl.BlockSpec(memory_space=pltpu.VMEM)
    dma = pltpu.SemaphoreType.DMA
    moved, speed = pl.pallas_call(
        functools.partial(kernel, n_mesh, n_sub, width),
        out_shape=(out, out),
        in_specs=[anywhere] * 10,
        out_specs=(vmem, vmem),
        scratch_shapes=[
            pltpu.VMEM((24, 24), F32),
            pltpu.SMEM((steps, ROWS), jnp.int32),
            pltpu.VMEM((24 * ROWS, LANES), F32),
            pltpu.VMEM((8 * ROWS, LANES), F32),
            pltpu.VMEM((steps * ROWS, LANES), jnp.int32),
            pltpu.VMEM((7 * width // LANES, LANES), F32),
            pltpu.VMEM((n_mesh, 4 * width // LANES, LANES), F32),
            pltpu.VMEM((n_mesh * 4 * width // LANES + 128, LANES), F32),
            pltpu.VMEM((8, LANES), F32),
            pltpu.VMEM((2, 32, LANES), F32),
            pltpu.VMEM((5, 8, LANES), F32),
            pltpu.VMEM((2, 32, LANES), F32),
            pltpu.VMEM((2, 8, LANES), F32),
            pltpu.VMEM((2, 2, 8, LANES), F32),
            pltpu.VMEM((8 * len(SPREAD), LANES), F32),
            pltpu.VMEM((2 * 9 * 8, LANES), F32),
            dma((5,)),
            pltpu.SemaphoreType.REGULAR,
        ],
        compiler_params=pltpu.CompilerParams(collective_id=0, has_side_effects=True),
    )(
        stiffness,
        owners.reshape(steps, ROWS),
        displacement.reshape(6 * ROWS, LANES),
        velocity.reshape(6 * ROWS, LANES),
        node_mass.reshape(2 * ROWS, LANES),
        moduli.reshape(2 * ROWS, LANES),
        surface_ref.reshape(3 * ROWS, LANES),
        facets.transpose(0, 2, 1, 3).reshape(6 * width // LANES, LANES),
        penalty.reshape(width // LANES, LANES),
        facet_pairs.reshape(steps * ROWS, LANES),
    )
    moved, speed = pl.pallas_call(
        flush,
        out_shape=[jax.ShapeDtypeStruct((6 * ROWS, LANES), F32)] * 2,
        in_specs=[anywhere, anywhere],
        out_specs=[anywhere, anywhere],
        scratch_shapes=[dma((2,))],
        compiler_params=pltpu.CompilerParams(vmem_limit_bytes=1 << 20),
    )(pltpu.with_memory_space_constraint(moved, pltpu.VMEM), pltpu.with_memory_space_constraint(speed, pltpu.VMEM))
    return moved.reshape(displacement.shape), speed.reshape(velocity.shape)


def solution(mesh):
    in_specs = (
        P(None, None, "mesh", "sub"),
        P(None, None, "mesh", "sub"),
        P(None, "mesh", "sub"),
        P(None, "mesh", "sub"),
        P(),
        P(None, "mesh", "sub"),
        P("mesh", "sub", None, None),
        P("mesh", "sub", None),
        P(None, "mesh", "sub", None, None),
        P(None, "mesh", "sub"),
    )
    out_specs = (P(None, None, "mesh", "sub"), P(None, None, "mesh", "sub"))
    return jax.shard_map(shards, mesh=mesh, in_specs=in_specs, out_specs=out_specs, check_vma=False)
```

```python
import functools

import jax
import jax.numpy as jnp
from jax import lax
from jax.experimental import pallas as pl
from jax.experimental.pallas import tpu as pltpu
from jax.sharding import PartitionSpec as P

TIME_STEP = 0.1
MESH = pl.DeviceIdType.MESH
ROWS = 8
LANES = 128
GROUP = 8
GROUPS = LANES // GROUP
F32 = jnp.float32
BF16 = jnp.bfloat16
BLOCKS = 9 * 8
DEPTH = BLOCKS + 8


def roll(x, shift):
    shift %= LANES
    return pltpu.roll(x, shift, 1) if shift else x


def iota(shape, axis):
    return lax.broadcasted_iota(jnp.int32, shape, axis)


def one_hot(condition):
    return jnp.where(condition, 1.0, 0.0).astype(BF16)


def coefficients(stiff):
    high = stiff.astype(BF16)
    low = (stiff - high.astype(F32)).astype(BF16)
    row = iota((32, 24), 0)
    o, b, e = row & 7, row >> 4, (row >> 3) & 1
    wanted = 3 * (4 * (o & 1) + 2 * b + e) + (o >> 1)
    pick = one_hot((wanted == iota((32, 24), 1)) & (o < 6))
    high = jnp.dot(pick, high, preferred_element_type=F32).astype(BF16)
    low = jnp.dot(pick, low, preferred_element_type=F32).astype(BF16)

    def columns(shape):
        col = iota(shape, 1)
        third = jnp.where(col >= DEPTH, 1, 0) + jnp.where(col >= 2 * DEPTH, 1, 0) + jnp.where(col >= 3 * DEPTH, 1, 0)
        rest = col - DEPTH * third
        off, p = rest >> 3, rest & 7
        di = jnp.where(off >= 3, 1, 0) + jnp.where(off >= 6, 1, 0) - 1
        dj = off - 3 * (di + 1) - 1
        return third, di, dj, p, off < 9

    def inside(b2, e2):
        return (b2 >= 0) & (b2 <= 1) & (e2 >= 0) & (e2 <= 1)

    third, di, dj, p, used = columns((24, 256))
    force = None
    for group in range(4):
        b2, e2 = di + (group >> 1), dj + (group & 1)
        wanted = 3 * (4 * (p & 1) + 2 * b2 + e2) + (p >> 1)
        place = used & inside(b2, e2) & (p < 6) & (wanted == iota((24, 256), 0))
        term = jnp.dot(high, one_hot(place & (third < 2)), preferred_element_type=F32)
        term = term + jnp.dot(low, one_hot(place & (third == 2)), preferred_element_type=F32)
        force = term if force is None else jnp.where((iota((32, 256), 0) >> 3) == group, term, force)
    third, di, dj, p, used = columns((24, LANES))
    single = None
    for group in range(4):
        b2, e2 = di + (group >> 1), dj + (group & 1)
        wanted = 3 * (4 * (p & 1) + 2 * b2 + e2) + (p >> 1)
        place = used & inside(b2, e2) & (p < 6) & (wanted == iota((24, LANES), 0)) & (third == 0)
        term = jnp.dot(high, one_hot(place), preferred_element_type=F32)
        term = term + jnp.dot(low, one_hot(place), preferred_element_type=F32)
        single = term if single is None else jnp.where((iota((32, LANES), 0) >> 3) == group, term, single)
    third, di, dj, p, used = columns((32, 256))
    row = iota((32, 256), 0)
    counted = used & inside(di + (row >> 4), dj + ((row >> 3) & 1)) & (p >= 6) & (third < 2)
    return jnp.concatenate([force, jnp.where(counted, 0.125, 0.0)], axis=0).astype(BF16), single


TOUCHED = [
    [2 * b + e for b in (0, 1) for e in (0, 1) if 0 <= di + b <= 1 and 0 <= dj + e <= 1]
    for di in (-1, 0, 1)
    for dj in (-1, 0, 1)
]
SPREAD = [(off, p, g) for off in range(9) for p in range(6) for g in TOUCHED[off]]


def stacked(blocks):
    x = jnp.concatenate(blocks + [jnp.zeros_like(blocks[0])], axis=0)
    high = x.astype(BF16)
    low = (x - high.astype(F32)).astype(BF16)
    return jnp.concatenate([high, low, high, jnp.zeros((256 - 3 * DEPTH, x.shape[1]), BF16)], axis=0)


def kernel(
    n_mesh,
    n_sub,
    width,
    stiff_hbm,
    owners_hbm,
    disp_hbm,
    vel_hbm,
    mass_hbm,
    moduli_hbm,
    surf_hbm,
    facets_hbm,
    penalty_hbm,
    pairs_hbm,
    out_disp,
    out_vel,
    stiff,
    owners,
    inbox,
    inverse,
    pairs,
    raw,
    tables,
    distant,
    edge,
    border,
    edges,
    borders,
    note,
    noted,
    spread,
    turns,
    sems,
    ready,
):
    q, s = lax.axis_index("mesh"), lax.axis_index("sub")
    own, vel = inbox.at[pl.ds(0, 64)], inbox.at[pl.ds(64, 64)]
    mass, base = inbox.at[pl.ds(112, 16)], inbox.at[pl.ds(128, 64)]
    chunks = width // LANES
    half = chunks // 2
    bits = width.bit_length() - 1

    def at(dq, ds):
        return (lax.rem(q + dq + n_mesh, n_mesh), lax.rem(s + ds + n_sub, n_sub))

    size = 4 * chunks
    planar = 2 * 8 + 2 * 32 + (n_mesh - 1) * size
    direct = 3 * 8 + n_mesh * size

    def landed(rows, i):
        ref = distant.at[pl.ds(0, rows)]
        return pltpu.make_async_copy(ref, ref, sems.at[i])

    copies = [
        pltpu.make_async_copy(src, dst, sems.at[i])
        for src, dst, i in [
            (facets_hbm, raw.at[pl.ds(0, 6 * chunks)], 2),
            (penalty_hbm, raw.at[pl.ds(6 * chunks, chunks)], 2),
            (disp_hbm, own.at[pl.ds(0, 48)], 0),
            (moduli_hbm, own.at[pl.ds(48, 16)], 0),
            (owners_hbm, owners, 1),
            (pairs_hbm, pairs, 0),
            (vel_hbm, vel.at[pl.ds(0, 48)], 0),
            (mass_hbm, mass, 0),
        ]
        + [(surf_hbm.at[pl.ds(8 * m, 8)], base.at[pl.ds(16 * m, 8)], 0) for m in range(3)]
    ]
    for copy in copies:
        copy.start()
    first, last, odd = s == 0, s == n_sub - 1, lax.rem(s, 2) == 1
    from_last, from_above = first, odd & (s != n_sub - 1)
    to_below = jnp.logical_not(odd | first)
    barrier = pltpu.get_barrier_semaphore()

    def hello(dq, ds):
        pl.semaphore_signal(barrier, inc=1, device_id=at(dq, ds), device_id_type=MESH)

    for dq in range(1, n_mesh):
        hello(dq, 0)

    @pl.when(first)
    def _():
        hello(0, 1)
        for dq in range(n_mesh):
            hello(dq, -1)

    @pl.when(jnp.logical_not(first))
    def _():
        hello(0, -1)

    @pl.when(from_above)
    def _():
        for dq in range(n_mesh):
            hello(dq, 1)

    @pl.when(to_below)
    def _():
        hello(0, 1)

    lane = iota((8, LANES), 1)
    plane = iota((8, LANES), 0)
    group = lane >> 3
    place_in = lane & 7
    entry = plane < 6
    surface = entry & ((plane & 1) == 0)
    flat = jnp.zeros((8, LANES), F32)
    for p in (1, 3, 5):
        base[pl.ds(8 * p, 8), :] = flat
    base[pl.ds(48, 8), :] = flat - 1.0

    landed(7 * chunks, 2).wait()
    parts = [raw[pl.ds(chunks * c, chunks), :] for c in range(7)]
    root = jnp.sqrt(parts[6])
    normal = [root * parts[3 + m] for m in range(3)]
    offset = normal[0] * parts[0] + normal[1] * parts[1] + normal[2] * parts[2]
    for c, values in enumerate(normal + [offset]):
        for h in range(2):
            tables[q, pl.ds(2 * c + h, half, stride=8), :] = values[half * h : half * (h + 1)]

    expected = n_mesh - 1 + jnp.where(first, 1, jnp.where(odd, jnp.where(last, n_mesh + 1, 2), n_mesh + 1))
    def send(source, target, device, going, coming):
        return pltpu.make_async_remote_copy(
            src_ref=source,
            dst_ref=target,
            send_sem=sems.at[going],
            recv_sem=sems.at[coming],
            device_id=device,
            device_id_type=MESH,
        )

    def send_table(ds, t):
        place = pl.ds(pl.multiple_of(q * size, size), size)
        send(tables.at[q], distant.at[place], (t, lax.rem(s + ds + n_sub, n_sub)), 2, 5 if ds == 1 else 4).start()

    @pl.when(last)
    def _():
        pl.semaphore_wait(barrier, expected)
        send_table(1, 0)

    landed(152 + 16, 0).wait()
    copies[4].wait()
    stiff_copy = pltpu.make_async_copy(stiff_hbm, stiff, sems.at[1])
    stiff_copy.start()

    def of_row(ref, i):
        return ref[pl.ds(i, 8, stride=8), :]

    here = {i: of_row(own, i) for i in range(ROWS)}
    speed = {i: of_row(vel, i) for i in range(ROWS)}
    point = {i: of_row(base, i) for i in range(ROWS)}
    for i in range(ROWS):
        code = jnp.broadcast_to(pairs[pl.ds(i, 1), :] + (owners[0, i] << bits), (8, LANES)).astype(F32)
        point[i] = jnp.where(surface, point[i] + here[i], jnp.where(plane == 7, code, point[i]))

    sent = flat
    for g, i in [(i, i) for i in range(ROWS)] + [(8, 0), (9, 1), (14, 6), (15, 7)]:
        deep = roll(here[i], GROUP * g + 4)
        deep = jnp.where(place_in == 0, roll(point[i], GROUP * g + 1), deep)
        deep = jnp.where(place_in == 7, roll(point[i], GROUP * g + 7), deep)
        deep = jnp.where(place_in == 1, roll(speed[i], GROUP * g + 2), deep)
        deep = jnp.where(place_in == 6, roll(speed[i], GROUP * g + 6), deep)
        sent = jnp.where(group == g, deep, sent)
    edge[...] = sent
    for k, ids in enumerate(((6, 7, 7, 7), (0, 1, 0, 0))):
        for j, (what, i) in enumerate(zip((here, here, speed, point), ids)):
            border[k, pl.ds(8 * j, 8), :] = what[i]

    @pl.when(jnp.logical_not(last))
    def _():
        pl.semaphore_wait(barrier, expected)

    def send_direct(ds):
        def edge_to(dq):
            send(edge, edges.at[2 - dq + (4 if ds == 1 else 0)], at(dq, ds), 2, 5 if ds == 1 else 4).start()

        for dq in (0, 1, -1):

            @pl.when(at(dq, 0)[0] == 0)
            def _():
                edge_to(dq)

        if ds == -1:
            send_table(ds, 0)
        for dq in (0, 1, -1):

            @pl.when(at(dq, 0)[0] != 0)
            def _():
                edge_to(dq)

        for t in range(1, n_mesh):
            send_table(ds, t)

    @pl.when(last)
    def _():
        send_direct(1)
        pl.semaphore_signal(ready, inc=1, device_id=at(0, 1), device_id_type=MESH)

    for t in range(n_mesh):
        for k, dq in enumerate((1, -1)):

            @pl.when(lax.rem(q + dq + n_mesh, n_mesh) == t)
            def _():
                send(border.at[k], borders.at[k], (t, s), 0, 3).start()
                send(edge, edges.at[4 * k], (t, s), 0, 3).start()

        @pl.when(q != t)
        def _():
            send(tables.at[q], tables.at[q], (t, s), 0, 3).start()

    @pl.when(to_below)
    def _():
        send_direct(-1)

    for a in range(2):
        slowness = TIME_STEP / mass[pl.ds(8 * a, 8), :]
        for p in range(a, 8, 2):
            inverse[pl.ds(8 * p, 8), :] = slowness
    gain = {i: of_row(inverse, i) for i in range(ROWS)}
    stiff_copy.wait()
    weights, single = coefficients(stiff[...])
    for n, (off, p, g) in enumerate(SPREAD):
        column_of = single[8 * g : 8 * g + 8, 8 * off + p : 8 * off + p + 1]
        spread[pl.ds(8 * n, 8), :] = jnp.broadcast_to(column_of, (8, LANES))

    def elastic(first, second):
        blocks = [jnp.concatenate([a, b], axis=1) for a, b in zip(first, second)]
        got = jnp.dot(weights, stacked(blocks), preferred_element_type=F32)
        terms = [got[8 * g : 8 * g + 8] * got[32 + 8 * g : 40 + 8 * g] for g in range(4)]
        force = (terms[0] + terms[1]) + (terms[2] + terms[3])
        return force[:, :LANES], force[:, LANES:]

    def side_forces(moved):
        for k, blocks in enumerate(moved):
            for off, x in enumerate(blocks):
                turns[pl.ds(72 * k + 8 * off, 8), :] = x

        def plane_of(k, off, p):
            return jnp.broadcast_to(turns[pl.ds(72 * k + 8 * off + p, 1), :], (8, LANES))

        def plus(table, key, term):
            table[key] = table[key] + term if key in table else term

        sums, scales, n = {}, {}, 0
        for off in range(9):
            for k in range(len(moved)):
                both = plane_of(k, off, 6) + plane_of(k, off, 7)
                for g in TOUCHED[off]:
                    plus(scales, (k, g), both)
            for p in range(6):
                values = [plane_of(k, off, p) for k in range(len(moved))]
                for g in TOUCHED[off]:
                    factor = spread[pl.ds(8 * n, 8), :]
                    n += 1
                    for k, value in enumerate(values):
                        plus(sums, (k, g), factor * value)
        terms = {key: sums[key] * (0.125 * scales[key]) for key in sums}
        return [(terms[k, 0] + terms[k, 1]) + (terms[k, 2] + terms[k, 3]) for k in range(len(moved))]

    def around(rows, i):
        return [x for di in (-1, 0, 1) for x in rows[i + di]]

    def turned(x):
        return (roll(x, 1), x, roll(x, -1))

    def narrowed(total, second):
        return jnp.where(second, pltpu.roll(total, 7, 0), total)

    def facet_of(step, i):
        index = jnp.broadcast_to(pairs[pl.ds(step * ROWS + i, 1), :], (8, LANES))
        chunk, place = index >> 7, index & (LANES - 1)
        second = chunk >= half
        chunk = jnp.where(second, chunk - half, chunk)
        owner = owners[step, i]
        total = flat
        for k in range(half):
            picked = jnp.take_along_axis(tables[owner, pl.ds(8 * k, 8), :], place, axis=1, mode="promise_in_bounds")
            total = jnp.where(chunk == k, picked, total)
        return narrowed(total, second)

    def wanted_by(at_point):
        code = jnp.broadcast_to(at_point[7:8], (8, LANES)).astype(jnp.int32)
        owner, index = code >> bits, code & (width - 1)
        chunk, place = index >> 7, index & (LANES - 1)
        second = chunk >= half
        return jnp.where(second, chunk - half, chunk) + half * owner, place, second

    def facet_by(wanted, ref):
        chunk, place, second = wanted
        total = flat
        for k in range(half * n_mesh):
            rows = ref(k)
            picked = jnp.take_along_axis(rows, place, axis=1, mode="promise_in_bounds")
            total = jnp.where(chunk == k, picked, total)
        return narrowed(total, second)

    def of_plane(k):
        return tables[k // half, pl.ds(8 * (k % half), 8), :]

    def of_side(k):
        return distant[pl.ds(8 * k, 8), :]

    def push_of(facet, at_point):
        product = jnp.where(surface | (plane == 6), facet * at_point, 0.0)
        product = product + pltpu.roll(product, 4, 0)
        product = product + pltpu.roll(product, 2, 0)
        return jnp.where(surface, facet * jnp.maximum(-product, 0.0), 0.0)

    def ring_step(values, moving, net):
        weight = jnp.where(
            (plane & 1) == 0, jnp.broadcast_to(moving[6:7], (8, LANES)), jnp.broadcast_to(moving[7:8], (8, LANES))
        )
        slow = TIME_STEP / weight
        faster = moving + slow * net
        return jnp.where(entry, values + TIME_STEP * faster, values), faster

    rows = {i: turned(here[i]) for i in range(ROWS)}
    force = {}
    for i in (1, 3, 5):
        force[i], force[i + 1] = elastic(around(rows, i), around(rows, i + 1))
    landed(planar, 3).wait()
    for i, (k, j) in {-2: (0, 0), -1: (0, 1), 8: (1, 0), 9: (1, 1)}.items():
        here[i] = borders[k, pl.ds(8 * j, 8), :]
        rows[i] = turned(here[i])
    force[0], force[7] = elastic(around(rows, 0), around(rows, 7))
    force[-1], force[8] = elastic(around(rows, -1), around(rows, 8))

    def column(middle, before, behind):
        return jnp.where(group < 8, middle, jnp.where(group < 12, behind, before))

    centre = column(sent, edges[0], edges[4])
    own_push = push_of(facet_by(wanted_by(centre), of_plane), centre)

    note[0] = centre
    note[1] = own_push

    @pl.when(jnp.logical_not(last))
    def _():
        send(note, noted.at[0], at(0, 1), 1, 4).start()

    @pl.when(odd)
    def _():
        send(note, noted.at[1], at(0, -1), 1, 4).start()

    @pl.when(first)
    def _():
        pl.semaphore_wait(ready, 1)
        send(note, noted.at[1], at(0, -1), 1, 4).start()

    later = {}
    after, fast = {}, {}
    for i in range(ROWS):
        net = push_of(facet_of(0, i), point[i]) - force[i]
        later[i] = facet_of(1, i)
        fast[i] = speed[i] + gain[i] * net
        after[i] = jnp.where(entry, here[i] + TIME_STEP * fast[i], here[i])
    for i, k in ((-1, 0), (8, 1)):
        moving, at_point = borders[k, pl.ds(16, 8), :], borders[k, pl.ds(24, 8), :]
        facet = facet_by(wanted_by(at_point), of_plane)
        after[i], _ = ring_step(here[i], moving, push_of(facet, at_point) - force[i])

    rows = {i: turned(after[i]) for i in range(-1, 9)}
    for i in range(0, ROWS, 2):
        force[i], force[i + 1] = elastic(around(rows, i), around(rows, i + 1))
    for i in range(ROWS):
        at_point = of_row(base, i)
        at_point = jnp.where(surface, at_point + after[i], at_point)
        past = fast[i] + gain[i] * (push_of(later[i], at_point) - force[i])
        out_vel[pl.ds(i, 6, stride=8), :] = past[0:6]
        out_disp[pl.ds(i, 6, stride=8), :] = (after[i] + TIME_STEP * past)[0:6]

    def strip_of(rows_of, indices):
        made = flat
        for i in indices:
            g = i % GROUPS
            piece = jnp.where(place_in < 4, roll(rows_of[i], GROUP * g + 1), roll(rows_of[i], GROUP * g + 7))
            made = jnp.where(group == g, piece, made)
        return made

    known = strip_of(after, range(-1, 9))
    known_fast, known_gain, known_facet = (strip_of(x, range(ROWS)) for x in (fast, gain, later))
    known_point = strip_of({i: of_row(base, i) for i in range(ROWS)}, range(ROWS))
    shifts = (-3, 3)
    own_pushes = [roll(own_push, -6), roll(own_push, 6)]

    @pl.when(from_above)
    def _():
        landed(2 * 8 + direct, 4).wait()

    @pl.when(first)
    def _():
        landed(2 * 8, 4).wait()

    @pl.when(jnp.logical_not(first | from_above))
    def _():
        landed(2 * 2 * 8, 4).wait()

    above = column(edges[2], edges[1], edges[3])

    def turned_strip(x, shift):
        return [roll(x, shift - (GROUP * di + dj)) for di in (-1, 0, 1) for dj in (-1, 0, 1)]

    from_before = place_in < 4
    right = jnp.where(from_before, centre, jnp.where(from_above, above, noted[1, 0]))
    moved_right = turned_strip(right, shifts[1])
    (force_right,) = side_forces([moved_right])

    @pl.when(first)
    def _():
        landed(direct, 5).wait()

    far = jnp.where(first, column(edges[6], edges[5], edges[7]), above)
    left = jnp.where(from_before, jnp.where(from_last, far, noted[0, 0]), centre)
    moved_left = turned_strip(left, shifts[0])
    (force_left,) = side_forces([moved_left])
    strips, moved, strip_force = (left, right), (moved_left, moved_right), (force_left, force_right)
    strip_speed = [
        jnp.where(place_in == 0, roll(strips[0], -1), roll(strips[0], -5)),
        jnp.where(place_in == 7, roll(strips[1], 1), roll(strips[1], 5)),
    ]
    far_wanted = wanted_by(far)

    far_push = push_of(facet_by(far_wanted, of_side), far)
    strip_after = []
    for k, by_far in enumerate((from_last, from_above)):
        push = jnp.where(by_far, far_push, noted[k, 1])
        push = jnp.where(place_in == (0, 7)[k], push, own_pushes[k])
        strip_after.append(ring_step(moved[k][4], strip_speed[k], push - strip_force[k]))

    low, high = place_in < 2, place_in > 5
    edge_now = jnp.where(low, strip_after[0][0], jnp.where(high, strip_after[1][0], known))
    edge_fast = jnp.where(place_in == 1, strip_after[0][1], jnp.where(place_in == 6, strip_after[1][1], known_fast))
    (edge_force,) = side_forces([[roll(edge_now, -(GROUP * di + dj)) for di in (-1, 0, 1) for dj in (-1, 0, 1)]])
    at_point = jnp.where(surface, known_point + edge_now, known_point)
    past = edge_fast + known_gain * (push_of(known_facet, at_point) - edge_force)
    moved_to = edge_now + TIME_STEP * past
    side = (lane < 2) | (lane >= LANES - 2)
    for i in range(ROWS):
        for ref, x in ((out_vel, past), (out_disp, moved_to)):
            fixed = jnp.where(lane < 2, roll(x, -(GROUP * i + 1)), roll(x, LANES - 7 - GROUP * i))
            at_row = pl.ds(i, 6, stride=8)
            ref[at_row, :] = jnp.where(side[0:6], fixed[0:6], ref[at_row, :])

    landed(planar, 0).wait()

    @pl.when(to_below | last)
    def _():
        landed(direct, 2).wait()

    two_notes = first | (odd & jnp.logical_not(last))

    @pl.when(two_notes)
    def _():
        landed(2 * 2 * 8, 1).wait()

    @pl.when(jnp.logical_not(two_notes))
    def _():
        landed(2 * 8, 1).wait()


def flush(moved, speed, out_moved, out_speed, sem):
    copies = [
        pltpu.make_async_copy(src, dst, sem.at[i])
        for i, (src, dst) in enumerate(((moved, out_moved), (speed, out_speed)))
    ]
    for copy in copies:
        copy.start()
    for copy in copies:
        copy.wait()


def shards(
    displacement,
    velocity,
    node_mass,
    moduli,
    stiffness,
    surface_ref,
    facets,
    penalty,
    owners,
    facet_pairs,
):
    steps = owners.shape[0]
    width = facets.shape[3]
    n_mesh, n_sub = lax.axis_size("mesh"), lax.axis_size("sub")
    assert displacement.shape == (3, 2, ROWS, LANES) and steps == 2 and n_sub % 2 == 0
    assert width == 1 << (width.bit_length() - 1) and width >= 2 * LANES
    out = pltpu.VMEM((6 * ROWS, LANES), F32)
    anywhere = pl.BlockSpec(memory_space=pl.ANY)
    vmem = pl.BlockSpec(memory_space=pltpu.VMEM)
    dma = pltpu.SemaphoreType.DMA
    moved, speed = pl.pallas_call(
        functools.partial(kernel, n_mesh, n_sub, width),
        out_shape=(out, out),
        in_specs=[anywhere] * 10,
        out_specs=(vmem, vmem),
        scratch_shapes=[
            pltpu.VMEM((24, 24), F32),
            pltpu.SMEM((steps, ROWS), jnp.int32),
            pltpu.VMEM((24 * ROWS, LANES), F32),
            pltpu.VMEM((8 * ROWS, LANES), F32),
            pltpu.VMEM((steps * ROWS, LANES), jnp.int32),
            pltpu.VMEM((7 * width // LANES, LANES), F32),
            pltpu.VMEM((n_mesh, 4 * width // LANES, LANES), F32),
            pltpu.VMEM((n_mesh * 4 * width // LANES + 128, LANES), F32),
            pltpu.VMEM((8, LANES), F32),
            pltpu.VMEM((2, 32, LANES), F32),
            pltpu.VMEM((8, 8, LANES), F32),
            pltpu.VMEM((2, 32, LANES), F32),
            pltpu.VMEM((2, 8, LANES), F32),
            pltpu.VMEM((2, 2, 8, LANES), F32),
            pltpu.VMEM((8 * len(SPREAD), LANES), F32),
            pltpu.VMEM((2 * 9 * 8, LANES), F32),
            dma((6,)),
            pltpu.SemaphoreType.REGULAR,
        ],
        compiler_params=pltpu.CompilerParams(collective_id=0, has_side_effects=True),
    )(
        stiffness,
        owners.reshape(steps, ROWS),
        displacement.reshape(6 * ROWS, LANES),
        velocity.reshape(6 * ROWS, LANES),
        node_mass.reshape(2 * ROWS, LANES),
        moduli.reshape(2 * ROWS, LANES),
        surface_ref.reshape(3 * ROWS, LANES),
        facets.transpose(0, 2, 1, 3).reshape(6 * width // LANES, LANES),
        penalty.reshape(width // LANES, LANES),
        facet_pairs.reshape(steps * ROWS, LANES),
    )
    moved, speed = pl.pallas_call(
        flush,
        out_shape=[jax.ShapeDtypeStruct((6 * ROWS, LANES), F32)] * 2,
        in_specs=[anywhere, anywhere],
        out_specs=[anywhere, anywhere],
        scratch_shapes=[dma((2,))],
        compiler_params=pltpu.CompilerParams(vmem_limit_bytes=1 << 20),
    )(pltpu.with_memory_space_constraint(moved, pltpu.VMEM), pltpu.with_memory_space_constraint(speed, pltpu.VMEM))
    return moved.reshape(displacement.shape), speed.reshape(velocity.shape)


def solution(mesh):
    in_specs = (
        P(None, None, "mesh", "sub"),
        P(None, None, "mesh", "sub"),
        P(None, "mesh", "sub"),
        P(None, "mesh", "sub"),
        P(),
        P(None, "mesh", "sub"),
        P("mesh", "sub", None, None),
        P("mesh", "sub", None),
        P(None, "mesh", "sub", None, None),
        P(None, "mesh", "sub"),
    )
    out_specs = (P(None, None, "mesh", "sub"), P(None, None, "mesh", "sub"))
    return jax.shard_map(shards, mesh=mesh, in_specs=in_specs, out_specs=out_specs, check_vma=False)
```

```python
import functools

import jax
import jax.numpy as jnp
from jax import lax
from jax.experimental import pallas as pl
from jax.experimental.pallas import tpu as pltpu
from jax.sharding import PartitionSpec as P

TIME_STEP = 0.1
MESH = pl.DeviceIdType.MESH
ROWS = 8
LANES = 128
GROUP = 8
GROUPS = LANES // GROUP
F32 = jnp.float32
BF16 = jnp.bfloat16
BLOCKS = 9 * 8
DEPTH = BLOCKS + 8


def roll(x, shift):
    shift %= LANES
    return pltpu.roll(x, shift, 1) if shift else x


def iota(shape, axis):
    return lax.broadcasted_iota(jnp.int32, shape, axis)


def one_hot(condition):
    return jnp.where(condition, 1.0, 0.0).astype(BF16)


def coefficients(stiff):
    high = stiff.astype(BF16)
    low = (stiff - high.astype(F32)).astype(BF16)
    row = iota((32, 24), 0)
    o, b, e = row & 7, row >> 4, (row >> 3) & 1
    wanted = 3 * (4 * (o & 1) + 2 * b + e) + (o >> 1)
    pick = one_hot((wanted == iota((32, 24), 1)) & (o < 6))
    high = jnp.dot(pick, high, preferred_element_type=F32).astype(BF16)
    low = jnp.dot(pick, low, preferred_element_type=F32).astype(BF16)

    def columns(shape):
        col = iota(shape, 1)
        third = jnp.where(col >= DEPTH, 1, 0) + jnp.where(col >= 2 * DEPTH, 1, 0) + jnp.where(col >= 3 * DEPTH, 1, 0)
        rest = col - DEPTH * third
        off, p = rest >> 3, rest & 7
        di = jnp.where(off >= 3, 1, 0) + jnp.where(off >= 6, 1, 0) - 1
        dj = off - 3 * (di + 1) - 1
        return third, di, dj, p, off < 9

    def inside(b2, e2):
        return (b2 >= 0) & (b2 <= 1) & (e2 >= 0) & (e2 <= 1)

    third, di, dj, p, used = columns((24, 256))
    force = None
    for group in range(4):
        b2, e2 = di + (group >> 1), dj + (group & 1)
        wanted = 3 * (4 * (p & 1) + 2 * b2 + e2) + (p >> 1)
        place = used & inside(b2, e2) & (p < 6) & (wanted == iota((24, 256), 0))
        term = jnp.dot(high, one_hot(place & (third < 2)), preferred_element_type=F32)
        term = term + jnp.dot(low, one_hot(place & (third == 2)), preferred_element_type=F32)
        force = term if force is None else jnp.where((iota((32, 256), 0) >> 3) == group, term, force)
    third, di, dj, p, used = columns((24, LANES))
    single = None
    for group in range(4):
        b2, e2 = di + (group >> 1), dj + (group & 1)
        wanted = 3 * (4 * (p & 1) + 2 * b2 + e2) + (p >> 1)
        place = used & inside(b2, e2) & (p < 6) & (wanted == iota((24, LANES), 0)) & (third == 0)
        term = jnp.dot(high, one_hot(place), preferred_element_type=F32)
        term = term + jnp.dot(low, one_hot(place), preferred_element_type=F32)
        single = term if single is None else jnp.where((iota((32, LANES), 0) >> 3) == group, term, single)
    third, di, dj, p, used = columns((32, 256))
    row = iota((32, 256), 0)
    counted = used & inside(di + (row >> 4), dj + ((row >> 3) & 1)) & (p >= 6) & (third < 2)
    return jnp.concatenate([force, jnp.where(counted, 0.125, 0.0)], axis=0).astype(BF16), single


TOUCHED = [
    [2 * b + e for b in (0, 1) for e in (0, 1) if 0 <= di + b <= 1 and 0 <= dj + e <= 1]
    for di in (-1, 0, 1)
    for dj in (-1, 0, 1)
]
SPREAD = [(off, p, g) for off in range(9) for p in range(6) for g in TOUCHED[off]]


def stacked(blocks):
    x = jnp.concatenate(blocks + [jnp.zeros_like(blocks[0])], axis=0)
    high = x.astype(BF16)
    low = (x - high.astype(F32)).astype(BF16)
    return jnp.concatenate([high, low, high, jnp.zeros((256 - 3 * DEPTH, x.shape[1]), BF16)], axis=0)


def kernel(
    n_mesh,
    n_sub,
    width,
    stiff_hbm,
    owners_hbm,
    disp_hbm,
    vel_hbm,
    mass_hbm,
    moduli_hbm,
    surf_hbm,
    facets_hbm,
    penalty_hbm,
    pairs_hbm,
    out_disp,
    out_vel,
    stiff,
    owners,
    inbox,
    inverse,
    pairs,
    raw,
    tables,
    distant,
    edge,
    border,
    edges,
    borders,
    note,
    noted,
    spread,
    turns,
    sems,
    ready,
):
    q, s = lax.axis_index("mesh"), lax.axis_index("sub")
    own, vel = inbox.at[pl.ds(0, 64)], inbox.at[pl.ds(64, 64)]
    mass, base = inbox.at[pl.ds(112, 16)], inbox.at[pl.ds(128, 64)]
    chunks = width // LANES
    half = chunks // 2
    bits = width.bit_length() - 1

    def at(dq, ds):
        return (lax.rem(q + dq + n_mesh, n_mesh), lax.rem(s + ds + n_sub, n_sub))

    size = 4 * chunks
    planar = 2 * 8 + 2 * 32 + (n_mesh - 1) * size
    direct = 3 * 8 + n_mesh * size

    def landed(rows, i):
        ref = distant.at[pl.ds(0, rows)]
        return pltpu.make_async_copy(ref, ref, sems.at[i])

    copies = [
        pltpu.make_async_copy(src, dst, sems.at[i])
        for src, dst, i in [
            (facets_hbm, raw.at[pl.ds(0, 6 * chunks)], 2),
            (penalty_hbm, raw.at[pl.ds(6 * chunks, chunks)], 2),
            (disp_hbm, own.at[pl.ds(0, 48)], 0),
            (moduli_hbm, own.at[pl.ds(48, 16)], 0),
            (owners_hbm, owners, 1),
            (pairs_hbm, pairs, 0),
            (vel_hbm, vel.at[pl.ds(0, 48)], 0),
            (mass_hbm, mass, 0),
        ]
        + [(surf_hbm.at[pl.ds(8 * m, 8)], base.at[pl.ds(16 * m, 8)], 0) for m in range(3)]
    ]
    for copy in copies:
        copy.start()
    first, last, odd = s == 0, s == n_sub - 1, lax.rem(s, 2) == 1
    from_last, from_above = first, odd & (s != n_sub - 1)
    to_below = jnp.logical_not(odd | first)
    barrier = pltpu.get_barrier_semaphore()

    def hello(dq, ds):
        pl.semaphore_signal(barrier, inc=1, device_id=at(dq, ds), device_id_type=MESH)

    for dq in range(1, n_mesh):
        hello(dq, 0)

    @pl.when(first)
    def _():
        hello(0, 1)
        for dq in range(n_mesh):
            hello(dq, -1)

    @pl.when(jnp.logical_not(first))
    def _():
        hello(0, -1)

    @pl.when(from_above)
    def _():
        for dq in range(n_mesh):
            hello(dq, 1)

    @pl.when(to_below)
    def _():
        hello(0, 1)

    lane = iota((8, LANES), 1)
    plane = iota((8, LANES), 0)
    group = lane >> 3
    place_in = lane & 7
    entry = plane < 6
    surface = entry & ((plane & 1) == 0)
    flat = jnp.zeros((8, LANES), F32)
    for p in (1, 3, 5):
        base[pl.ds(8 * p, 8), :] = flat
    base[pl.ds(48, 8), :] = flat - 1.0

    landed(7 * chunks, 2).wait()
    parts = [raw[pl.ds(chunks * c, chunks), :] for c in range(7)]
    root = jnp.sqrt(parts[6])
    normal = [root * parts[3 + m] for m in range(3)]
    offset = normal[0] * parts[0] + normal[1] * parts[1] + normal[2] * parts[2]
    for c, values in enumerate(normal + [offset]):
        for h in range(2):
            tables[q, pl.ds(2 * c + h, half, stride=8), :] = values[half * h : half * (h + 1)]

    expected = n_mesh - 1 + jnp.where(first, 1, jnp.where(odd, jnp.where(last, n_mesh + 1, 2), n_mesh + 1))
    def send(source, target, device, going, coming):
        return pltpu.make_async_remote_copy(
            src_ref=source,
            dst_ref=target,
            send_sem=sems.at[going],
            recv_sem=sems.at[coming],
            device_id=device,
            device_id_type=MESH,
        )

    def send_table(ds, t):
        place = pl.ds(pl.multiple_of(q * size, size), size)
        send(tables.at[q], distant.at[place], (t, lax.rem(s + ds + n_sub, n_sub)), 2, 4).start()

    @pl.when(last)
    def _():
        pl.semaphore_wait(barrier, expected)
        send_table(1, 0)

    landed(152 + 16, 0).wait()
    copies[4].wait()
    stiff_copy = pltpu.make_async_copy(stiff_hbm, stiff, sems.at[1])
    stiff_copy.start()

    def of_row(ref, i):
        return ref[pl.ds(i, 8, stride=8), :]

    here = {i: of_row(own, i) for i in range(ROWS)}
    speed = {i: of_row(vel, i) for i in range(ROWS)}
    point = {i: of_row(base, i) for i in range(ROWS)}
    for i in range(ROWS):
        code = jnp.broadcast_to(pairs[pl.ds(i, 1), :] + (owners[0, i] << bits), (8, LANES)).astype(F32)
        point[i] = jnp.where(surface, point[i] + here[i], jnp.where(plane == 7, code, point[i]))

    sent = flat
    for g, i in [(i, i) for i in range(ROWS)] + [(8, 0), (9, 1), (14, 6), (15, 7)]:
        deep = roll(here[i], GROUP * g + 4)
        deep = jnp.where(place_in == 0, roll(point[i], GROUP * g + 1), deep)
        deep = jnp.where(place_in == 7, roll(point[i], GROUP * g + 7), deep)
        deep = jnp.where(place_in == 1, roll(speed[i], GROUP * g + 2), deep)
        deep = jnp.where(place_in == 6, roll(speed[i], GROUP * g + 6), deep)
        sent = jnp.where(group == g, deep, sent)
    edge[...] = sent
    for k, ids in enumerate(((6, 7, 7, 7), (0, 1, 0, 0))):
        for j, (what, i) in enumerate(zip((here, here, speed, point), ids)):
            border[k, pl.ds(8 * j, 8), :] = what[i]

    @pl.when(jnp.logical_not(last))
    def _():
        pl.semaphore_wait(barrier, expected)

    def send_direct(ds):
        def edge_to(dq):
            send(edge, edges.at[2 - dq], at(dq, ds), 2, 4).start()

        for dq in (0, 1, -1):

            @pl.when(at(dq, 0)[0] == 0)
            def _():
                edge_to(dq)

        if ds == -1:
            send_table(ds, 0)
        for dq in (0, 1, -1):

            @pl.when(at(dq, 0)[0] != 0)
            def _():
                edge_to(dq)

        for t in range(1, n_mesh):
            send_table(ds, t)

    @pl.when(last)
    def _():
        send_direct(1)
        pl.semaphore_signal(ready, inc=1, device_id=at(0, 1), device_id_type=MESH)

    for t in range(n_mesh):
        for k, dq in enumerate((1, -1)):

            @pl.when(lax.rem(q + dq + n_mesh, n_mesh) == t)
            def _():
                send(border.at[k], borders.at[k], (t, s), 0, 3).start()
                send(edge, edges.at[4 * k], (t, s), 0, 3).start()

        @pl.when(q != t)
        def _():
            send(tables.at[q], tables.at[q], (t, s), 0, 3).start()

    @pl.when(to_below)
    def _():
        send_direct(-1)

    for a in range(2):
        slowness = TIME_STEP / mass[pl.ds(8 * a, 8), :]
        for p in range(a, 8, 2):
            inverse[pl.ds(8 * p, 8), :] = slowness
    gain = {i: of_row(inverse, i) for i in range(ROWS)}
    stiff_copy.wait()
    weights, single = coefficients(stiff[...])
    for n, (off, p, g) in enumerate(SPREAD):
        column_of = single[8 * g : 8 * g + 8, 8 * off + p : 8 * off + p + 1]
        spread[pl.ds(8 * n, 8), :] = jnp.broadcast_to(column_of, (8, LANES))

    def elastic(first, second):
        blocks = [jnp.concatenate([a, b], axis=1) for a, b in zip(first, second)]
        got = jnp.dot(weights, stacked(blocks), preferred_element_type=F32)
        terms = [got[8 * g : 8 * g + 8] * got[32 + 8 * g : 40 + 8 * g] for g in range(4)]
        force = (terms[0] + terms[1]) + (terms[2] + terms[3])
        return force[:, :LANES], force[:, LANES:]

    def side_forces(moved):
        for k, blocks in enumerate(moved):
            for off, x in enumerate(blocks):
                turns[pl.ds(72 * k + 8 * off, 8), :] = x

        def plane_of(k, off, p):
            return jnp.broadcast_to(turns[pl.ds(72 * k + 8 * off + p, 1), :], (8, LANES))

        def plus(table, key, term):
            table[key] = table[key] + term if key in table else term

        sums, scales, n = {}, {}, 0
        for off in range(9):
            for k in range(len(moved)):
                both = plane_of(k, off, 6) + plane_of(k, off, 7)
                for g in TOUCHED[off]:
                    plus(scales, (k, g), both)
            for p in range(6):
                values = [plane_of(k, off, p) for k in range(len(moved))]
                for g in TOUCHED[off]:
                    factor = spread[pl.ds(8 * n, 8), :]
                    n += 1
                    for k, value in enumerate(values):
                        plus(sums, (k, g), factor * value)
        terms = {key: sums[key] * (0.125 * scales[key]) for key in sums}
        return [(terms[k, 0] + terms[k, 1]) + (terms[k, 2] + terms[k, 3]) for k in range(len(moved))]

    def around(rows, i):
        return [x for di in (-1, 0, 1) for x in rows[i + di]]

    def turned(x):
        return (roll(x, 1), x, roll(x, -1))

    def narrowed(total, second):
        return jnp.where(second, pltpu.roll(total, 7, 0), total)

    def facet_of(step, i):
        index = jnp.broadcast_to(pairs[pl.ds(step * ROWS + i, 1), :], (8, LANES))
        chunk, place = index >> 7, index & (LANES - 1)
        second = chunk >= half
        chunk = jnp.where(second, chunk - half, chunk)
        owner = owners[step, i]
        total = flat
        for k in range(half):
            picked = jnp.take_along_axis(tables[owner, pl.ds(8 * k, 8), :], place, axis=1, mode="promise_in_bounds")
            total = jnp.where(chunk == k, picked, total)
        return narrowed(total, second)

    def wanted_by(at_point):
        code = jnp.broadcast_to(at_point[7:8], (8, LANES)).astype(jnp.int32)
        owner, index = code >> bits, code & (width - 1)
        chunk, place = index >> 7, index & (LANES - 1)
        second = chunk >= half
        return jnp.where(second, chunk - half, chunk) + half * owner, place, second

    def facet_by(wanted, ref):
        chunk, place, second = wanted
        total = flat
        for k in range(half * n_mesh):
            rows = ref(k)
            picked = jnp.take_along_axis(rows, place, axis=1, mode="promise_in_bounds")
            total = jnp.where(chunk == k, picked, total)
        return narrowed(total, second)

    def of_plane(k):
        return tables[k // half, pl.ds(8 * (k % half), 8), :]

    def of_side(k):
        return distant[pl.ds(8 * k, 8), :]

    def push_of(facet, at_point):
        product = jnp.where(surface | (plane == 6), facet * at_point, 0.0)
        product = product + pltpu.roll(product, 4, 0)
        product = product + pltpu.roll(product, 2, 0)
        return jnp.where(surface, facet * jnp.maximum(-product, 0.0), 0.0)

    def ring_step(values, moving, net):
        weight = jnp.where(
            (plane & 1) == 0, jnp.broadcast_to(moving[6:7], (8, LANES)), jnp.broadcast_to(moving[7:8], (8, LANES))
        )
        slow = TIME_STEP / weight
        faster = moving + slow * net
        return jnp.where(entry, values + TIME_STEP * faster, values), faster

    rows = {i: turned(here[i]) for i in range(ROWS)}
    force = {}
    for i in (1, 3, 5):
        force[i], force[i + 1] = elastic(around(rows, i), around(rows, i + 1))
    landed(planar, 3).wait()
    for i, (k, j) in {-2: (0, 0), -1: (0, 1), 8: (1, 0), 9: (1, 1)}.items():
        here[i] = borders[k, pl.ds(8 * j, 8), :]
        rows[i] = turned(here[i])
    force[0], force[7] = elastic(around(rows, 0), around(rows, 7))
    force[-1], force[8] = elastic(around(rows, -1), around(rows, 8))

    def column(middle, before, behind):
        return jnp.where(group < 8, middle, jnp.where(group < 12, behind, before))

    centre = column(sent, edges[0], edges[4])
    own_push = push_of(facet_by(wanted_by(centre), of_plane), centre)

    note[0] = centre
    note[1] = own_push

    @pl.when(jnp.logical_not(last))
    def _():
        send(note, noted.at[0], at(0, 1), 1, 4).start()

    @pl.when(odd)
    def _():
        send(note, noted.at[1], at(0, -1), 1, 4).start()

    @pl.when(first)
    def _():
        pl.semaphore_wait(ready, 1)
        send(note, noted.at[1], at(0, -1), 1, 4).start()

    later = {}
    after, fast = {}, {}
    for i in range(ROWS):
        net = push_of(facet_of(0, i), point[i]) - force[i]
        later[i] = facet_of(1, i)
        fast[i] = speed[i] + gain[i] * net
        after[i] = jnp.where(entry, here[i] + TIME_STEP * fast[i], here[i])
    for i, k in ((-1, 0), (8, 1)):
        moving, at_point = borders[k, pl.ds(16, 8), :], borders[k, pl.ds(24, 8), :]
        facet = facet_by(wanted_by(at_point), of_plane)
        after[i], _ = ring_step(here[i], moving, push_of(facet, at_point) - force[i])

    rows = {i: turned(after[i]) for i in range(-1, 9)}
    for i in range(0, ROWS, 2):
        force[i], force[i + 1] = elastic(around(rows, i), around(rows, i + 1))
    for i in range(ROWS):
        at_point = of_row(base, i)
        at_point = jnp.where(surface, at_point + after[i], at_point)
        past = fast[i] + gain[i] * (push_of(later[i], at_point) - force[i])
        out_vel[pl.ds(i, 6, stride=8), :] = past[0:6]
        out_disp[pl.ds(i, 6, stride=8), :] = (after[i] + TIME_STEP * past)[0:6]

    def strip_of(rows_of, indices):
        made = flat
        for i in indices:
            g = i % GROUPS
            piece = jnp.where(place_in < 4, roll(rows_of[i], GROUP * g + 1), roll(rows_of[i], GROUP * g + 7))
            made = jnp.where(group == g, piece, made)
        return made

    known = strip_of(after, range(-1, 9))
    known_fast, known_gain, known_facet = (strip_of(x, range(ROWS)) for x in (fast, gain, later))
    known_point = strip_of({i: of_row(base, i) for i in range(ROWS)}, range(ROWS))
    shifts = (-3, 3)
    own_pushes = [roll(own_push, -6), roll(own_push, 6)]

    has_direct = from_last | from_above

    @pl.when(jnp.logical_not(has_direct))
    def _():
        landed(2 * 2 * 8, 4).wait()

    @pl.when(has_direct)
    def _():
        landed(2 * 8 + direct, 4).wait()

    far = column(edges[2], edges[1], edges[3])
    left, right = jnp.where(from_last, far, noted[0, 0]), jnp.where(from_above, far, noted[1, 0])
    from_before = place_in < 4
    strips = [jnp.where(from_before, left, centre), jnp.where(from_before, centre, right)]
    moved = [
        [roll(x, shift - (GROUP * di + dj)) for di in (-1, 0, 1) for dj in (-1, 0, 1)]
        for x, shift in zip(strips, shifts)
    ]
    strip_force = side_forces(moved)
    strip_speed = [
        jnp.where(place_in == 0, roll(strips[0], -1), roll(strips[0], -5)),
        jnp.where(place_in == 7, roll(strips[1], 1), roll(strips[1], 5)),
    ]
    far_wanted = wanted_by(far)

    far_push = push_of(facet_by(far_wanted, of_side), far)
    strip_after = []
    for k, by_far in enumerate((from_last, from_above)):
        push = jnp.where(by_far, far_push, noted[k, 1])
        push = jnp.where(place_in == (0, 7)[k], push, own_pushes[k])
        strip_after.append(ring_step(moved[k][4], strip_speed[k], push - strip_force[k]))

    low, high = place_in < 2, place_in > 5
    edge_now = jnp.where(low, strip_after[0][0], jnp.where(high, strip_after[1][0], known))
    edge_fast = jnp.where(place_in == 1, strip_after[0][1], jnp.where(place_in == 6, strip_after[1][1], known_fast))
    (edge_force,) = side_forces([[roll(edge_now, -(GROUP * di + dj)) for di in (-1, 0, 1) for dj in (-1, 0, 1)]])
    at_point = jnp.where(surface, known_point + edge_now, known_point)
    past = edge_fast + known_gain * (push_of(known_facet, at_point) - edge_force)
    moved_to = edge_now + TIME_STEP * past
    side = (lane < 2) | (lane >= LANES - 2)
    for i in range(ROWS):
        for ref, x in ((out_vel, past), (out_disp, moved_to)):
            fixed = jnp.where(lane < 2, roll(x, -(GROUP * i + 1)), roll(x, LANES - 7 - GROUP * i))
            at_row = pl.ds(i, 6, stride=8)
            ref[at_row, :] = jnp.where(side[0:6], fixed[0:6], ref[at_row, :])

    landed(planar, 0).wait()

    @pl.when(to_below | last)
    def _():
        landed(direct, 2).wait()

    two_notes = first | (odd & jnp.logical_not(last))

    @pl.when(two_notes)
    def _():
        landed(2 * 2 * 8, 1).wait()

    @pl.when(jnp.logical_not(two_notes))
    def _():
        landed(2 * 8, 1).wait()


def flush(moved, speed, out_moved, out_speed, sem):
    copies = [
        pltpu.make_async_copy(src, dst, sem.at[i])
        for i, (src, dst) in enumerate(((moved, out_moved), (speed, out_speed)))
    ]
    for copy in copies:
        copy.start()
    for copy in copies:
        copy.wait()


def shards(
    displacement,
    velocity,
    node_mass,
    moduli,
    stiffness,
    surface_ref,
    facets,
    penalty,
    owners,
    facet_pairs,
):
    steps = owners.shape[0]
    width = facets.shape[3]
    n_mesh, n_sub = lax.axis_size("mesh"), lax.axis_size("sub")
    assert displacement.shape == (3, 2, ROWS, LANES) and steps == 2 and n_sub % 2 == 0
    assert width == 1 << (width.bit_length() - 1) and width >= 2 * LANES
    out = pltpu.VMEM((6 * ROWS, LANES), F32)
    anywhere = pl.BlockSpec(memory_space=pl.ANY)
    vmem = pl.BlockSpec(memory_space=pltpu.VMEM)
    dma = pltpu.SemaphoreType.DMA
    moved, speed = pl.pallas_call(
        functools.partial(kernel, n_mesh, n_sub, width),
        out_shape=(out, out),
        in_specs=[anywhere] * 10,
        out_specs=(vmem, vmem),
        scratch_shapes=[
            pltpu.VMEM((24, 24), F32),
            pltpu.SMEM((steps, ROWS), jnp.int32),
            pltpu.VMEM((24 * ROWS, LANES), F32),
            pltpu.VMEM((8 * ROWS, LANES), F32),
            pltpu.VMEM((steps * ROWS, LANES), jnp.int32),
            pltpu.VMEM((7 * width // LANES, LANES), F32),
            pltpu.VMEM((n_mesh, 4 * width // LANES, LANES), F32),
            pltpu.VMEM((n_mesh * 4 * width // LANES + 128, LANES), F32),
            pltpu.VMEM((8, LANES), F32),
            pltpu.VMEM((2, 32, LANES), F32),
            pltpu.VMEM((5, 8, LANES), F32),
            pltpu.VMEM((2, 32, LANES), F32),
            pltpu.VMEM((2, 8, LANES), F32),
            pltpu.VMEM((2, 2, 8, LANES), F32),
            pltpu.VMEM((8 * len(SPREAD), LANES), F32),
            pltpu.VMEM((2 * 9 * 8, LANES), F32),
            dma((5,)),
            pltpu.SemaphoreType.REGULAR,
        ],
        compiler_params=pltpu.CompilerParams(collective_id=0, has_side_effects=True),
    )(
        stiffness,
        owners.reshape(steps, ROWS),
        displacement.reshape(6 * ROWS, LANES),
        velocity.reshape(6 * ROWS, LANES),
        node_mass.reshape(2 * ROWS, LANES),
        moduli.reshape(2 * ROWS, LANES),
        surface_ref.reshape(3 * ROWS, LANES),
        facets.transpose(0, 2, 1, 3).reshape(6 * width // LANES, LANES),
        penalty.reshape(width // LANES, LANES),
        facet_pairs.reshape(steps * ROWS, LANES),
    )
    moved, speed = pl.pallas_call(
        flush,
        out_shape=[jax.ShapeDtypeStruct((6 * ROWS, LANES), F32)] * 2,
        in_specs=[anywhere, anywhere],
        out_specs=[anywhere, anywhere],
        scratch_shapes=[dma((2,))],
        compiler_params=pltpu.CompilerParams(vmem_limit_bytes=1 << 20),
    )(pltpu.with_memory_space_constraint(moved, pltpu.VMEM), pltpu.with_memory_space_constraint(speed, pltpu.VMEM))
    return moved.reshape(displacement.shape), speed.reshape(velocity.shape)


def solution(mesh):
    in_specs = (
        P(None, None, "mesh", "sub"),
        P(None, None, "mesh", "sub"),
        P(None, "mesh", "sub"),
        P(None, "mesh", "sub"),
        P(),
        P(None, "mesh", "sub"),
        P("mesh", "sub", None, None),
        P("mesh", "sub", None),
        P(None, "mesh", "sub", None, None),
        P(None, "mesh", "sub"),
    )
    out_specs = (P(None, None, "mesh", "sub"), P(None, None, "mesh", "sub"))
    return jax.shard_map(shards, mesh=mesh, in_specs=in_specs, out_specs=out_specs, check_vma=False)
```
